32 devices in a mesh: dp: 1 (over z), ep: 4 (over y), tp: 8 (over x, core).
Axes of the slice: x: 4, y: 4, z: 1, core: 2. Of those that a mesh axis runs over, the one named last changes fastest.
The devices are a block of a 4x4x8 slice.
Arguments:
- tokens: bfloat16 [32768, 768], P(('dp', 'ep', 'tp'))
- expert_ids: int32 [32768, 1], P(('dp', 'ep', 'tp'))
- gate_vals: float32 [32768, 1], P(('dp', 'ep', 'tp'))
- w_gate: bfloat16 [64, 768, 3072], P('ep', None, 'tp')
- w_up: bfloat16 [64, 768, 3072], P('ep', None, 'tp')
- w_down: bfloat16 [64, 3072, 768], P('ep', 'tp')
Outputs:
- output: bfloat16 [32768, 768], P(('dp', 'ep', 'tp'))
All inputs are finite; a program needn't handle non-finite values.
Results may differ from the reference program's by a relative error of at most 0.00844203.
Values are sent between devices in bfloat16 or wider.
A program may use at most 768 MiB of HBM per device.

```python
import jax
import jax.numpy as jnp
from jax import lax

DMODEL = 768
FFN = 3072
EXPERTS = 64
TOP = 1
TOK_LOC = 1024
CAP_FACTOR = 2
EXPERT_RANKS = 4
TENSOR_RANKS = 8

NUM_DEV = EXPERT_RANKS * TENSOR_RANKS
CAPACITY = CAP_FACTOR * TOP * TOK_LOC // EXPERTS
HOT_ROWS = CAPACITY + 1


def routing_draw(key_route, key_hot):
    scores = jax.random.randint(key_route, (NUM_DEV, TOK_LOC, EXPERTS), 0, 65536)
    scores = scores * EXPERTS + jnp.arange(EXPERTS, dtype=jnp.int32)
    hot_ids = jax.random.randint(key_hot, (NUM_DEV, 1, 1), 0, EXPERTS)
    forced = (jnp.arange(TOK_LOC)[None, :, None] < HOT_ROWS) & (jnp.arange(EXPERTS)[None, None, :] == hot_ids)
    scores = scores + jnp.where(forced, 16777216, 0)
    chosen = lax.top_k(scores, TOP)[1]
    return chosen.reshape(NUM_DEV * TOK_LOC, TOP).astype(jnp.int32)


def setup_inputs(seed: int = 0, part: int = 0) -> dict:
    subkeys = jax.random.split(jax.random.key(seed), 8)
    key_tok = jax.random.fold_in(subkeys[0], part)
    key_route = jax.random.fold_in(subkeys[1], part)
    key_hot = jax.random.fold_in(subkeys[2], part)
    key_gate = jax.random.fold_in(subkeys[3], part)
    row_count = NUM_DEV * TOK_LOC
    tokens = jax.random.normal(key_tok, (row_count, DMODEL), jnp.float32).astype(jnp.bfloat16)
    expert_ids = routing_draw(key_route, key_hot)
    gate_vals = (0.5 + jax.random.uniform(key_gate, (row_count, TOP), jnp.float32)) * TOP ** -0.5
    w_gate = (jax.random.normal(subkeys[4], (EXPERTS, DMODEL, FFN), jnp.float32) * DMODEL ** -0.5).astype(jnp.bfloat16)
    w_up = (jax.random.normal(subkeys[5], (EXPERTS, DMODEL, FFN), jnp.float32) * DMODEL ** -0.5).astype(jnp.bfloat16)
    w_down = (jax.random.normal(subkeys[6], (EXPERTS, FFN, DMODEL), jnp.float32) * FFN ** -0.5).astype(jnp.bfloat16)
    return {"tokens": tokens, "expert_ids": expert_ids, "gate_vals": gate_vals, "w_gate": w_gate, "w_up": w_up, "w_down": w_down}


def slot_table(ids_one):
    flat_ids = ids_one.reshape(TOK_LOC * TOP)
    one_hot = (flat_ids[:, None] == jnp.arange(EXPERTS, dtype=jnp.int32)[None, :]).astype(jnp.int32)
    preceding = jnp.cumsum(one_hot, axis=0) - one_hot
    return jnp.sum(preceding * one_hot, axis=1).reshape(TOK_LOC, TOP)


def reference(tokens, expert_ids, gate_vals, w_gate, w_up, w_down):
    ids_dev = expert_ids.reshape(NUM_DEV, TOK_LOC, TOP)
    slot_ids = jax.vmap(slot_table)(ids_dev)
    kept_mask = slot_ids < CAPACITY
    dev_index = jnp.arange(NUM_DEV, dtype=jnp.int32)[:, None, None]
    tok_index = dev_index * TOK_LOC + jnp.arange(TOK_LOC, dtype=jnp.int32)[None, :, None] + jnp.zeros_like(slot_ids)
    total_slots = EXPERTS * NUM_DEV * CAPACITY
    dest_slot = jnp.where(kept_mask, (ids_dev * NUM_DEV + dev_index) * CAPACITY + slot_ids, total_slots)
    src_rows = jnp.zeros((total_slots,), jnp.int32).at[dest_slot.reshape(-1)].set(tok_index.reshape(-1), mode="drop")
    src_gate = jnp.zeros((total_slots,), jnp.float32).at[dest_slot.reshape(-1)].set(gate_vals.reshape(-1), mode="drop")

    def expert_step(acc_sum, per_expert):
        rows_idx, row_gate, wg_one, wu_one, wd_one = per_expert
        x_rows = jnp.take(tokens, rows_idx, axis=0)
        gate_pre = jnp.dot(x_rows, wg_one, preferred_element_type=jnp.float32)
        up_pre = jnp.dot(x_rows, wu_one, preferred_element_type=jnp.float32)
        hidden = (jax.nn.silu(gate_pre) * up_pre).astype(jnp.bfloat16)
        y_rows = jnp.dot(hidden, wd_one, preferred_element_type=jnp.float32).astype(jnp.bfloat16)
        acc_sum = acc_sum.at[rows_idx].add(y_rows.astype(jnp.float32) * row_gate[:, None])
        return acc_sum, None

    acc_init = jnp.zeros((NUM_DEV * TOK_LOC, DMODEL), jnp.float32)
    per_rows = src_rows.reshape(EXPERTS, NUM_DEV * CAPACITY)
    per_gate = src_gate.reshape(EXPERTS, NUM_DEV * CAPACITY)
    acc_final, _ = lax.scan(expert_step, acc_init, (per_rows, per_gate, w_gate, w_up, w_down))
    return acc_final.astype(jnp.bfloat16)
```

```python
import functools

import jax
import jax.numpy as jnp
from jax import lax
from jax.experimental import pallas as pl
from jax.experimental.pallas import tpu as pltpu
from jax.sharding import PartitionSpec as P

CAP_FACTOR = 2
GROUP = 2
MESH = pl.DeviceIdType.MESH
BF16 = jnp.bfloat16
F32 = jnp.float32


def dispatch_kernel(capacity, n_exp, ids_ref, x_ref, rows_ref, pos_ref):
    tok = ids_ref.shape[1]
    n_slots = rows_ref.shape[0]
    ids = ids_ref[...]
    one_hot = lax.broadcasted_iota(jnp.int32, (n_exp, tok), 0) == ids
    before = lax.broadcasted_iota(jnp.int32, (tok, tok), 0) < lax.broadcasted_iota(jnp.int32, (tok, tok), 1)
    preceding = jnp.dot(one_hot.astype(F32).astype(BF16), before.astype(F32).astype(BF16), preferred_element_type=F32)
    slot = jnp.sum(jnp.where(one_hot, preceding, 0.0), axis=0, keepdims=True).astype(jnp.int32)
    pos = jnp.where(slot < capacity, ids * capacity + slot, -1)
    pos_ref[...] = pos
    tile = 256

    @pl.loop(0, n_slots // tile)
    def _(i):
        want = lax.broadcasted_iota(jnp.int32, (tile, tok), 0) + i * tile
        pick = (want == pos).astype(F32).astype(BF16)
        start = pl.multiple_of(i * tile, tile)
        rows_ref[pl.ds(start, tile), :] = jnp.dot(pick, x_ref[...], preferred_element_type=F32).astype(BF16)


def dispatch(x_loc, ids_loc, n_exp, capacity):
    tok, d_model = x_loc.shape
    return pl.pallas_call(
        functools.partial(dispatch_kernel, capacity, n_exp),
        out_shape=(
            jax.ShapeDtypeStruct((n_exp * capacity, d_model), BF16),
            jax.ShapeDtypeStruct((1, tok), jnp.int32),
        ),
        name="dispatch",
    )(ids_loc.reshape(1, tok), x_loc)


def combine_kernel(pos_ref, gate_ref, y_ref, out_ref):
    n_slots = y_ref.shape[0]
    tok = out_ref.shape[0]
    tile = 256

    @pl.loop(0, tok // tile)
    def _(i):
        rows = pl.ds(pl.multiple_of(i * tile, tile), tile)
        pos = pos_ref[rows, :]
        pick = (lax.broadcasted_iota(jnp.int32, (tile, n_slots), 1) == pos).astype(F32).astype(BF16)
        y = jnp.dot(pick, y_ref[...], preferred_element_type=F32)
        weight = jnp.where(pos >= 0, gate_ref[rows, :], 0.0)
        out_ref[rows, :] = (y * weight).astype(BF16)


def combine(pos, gate_loc, y_slots):
    tok = gate_loc.shape[0]
    return pl.pallas_call(
        combine_kernel,
        out_shape=jax.ShapeDtypeStruct((tok, y_slots.shape[1]), BF16),
        name="combine",
    )(pos.reshape(tok, 1), gate_loc, y_slots)


def expert_kernel(
    n_y, n_x, rows_hbm, wg_hbm, wu_hbm, wd_hbm, out_hbm,
    x_buf, pair_buf, opp_buf, nbr_buf, w_in, w_out,
    ys_send, ys_recv, ys_loc, a_send, a_recv, b_send, b_recv, d_send, d_recv,
    p_send, p_recv, e_send, e_recv, f_send, f_recv, h_send, h_recv, h_loc, w_sem,
):
    n_loc, _, _, cap, d_model = x_buf.shape
    hidden = w_out.shape[2]
    n_grp = n_loc // GROUP
    half = n_y // 2
    yy = lax.axis_index("ep")
    tt = lax.axis_index("tp")
    xx, cc = tt // 2, tt % 2
    xr, xl, xo = (xx + 1) % n_x, (xx + n_x - 1) % n_x, (xx + 2) % n_x
    right, left, mate = {"tp": xr * 2 + cc}, {"tp": xl * 2 + cc}, {"tp": xx * 2 + 1 - cc}
    peers = [(yy + d) % n_y for d in range(1, n_y)]
    mine = cc * n_x

    def remote(src, dst, send, recv, device):
        return pltpu.make_async_remote_copy(
            src_ref=src, dst_ref=dst, send_sem=send, recv_sem=recv, device_id=device, device_id_type=MESH
        )

    def grp(g):
        return pl.ds(g * GROUP, GROUP)

    def y_copy(g, k, peer):
        return remote(
            rows_hbm.at[pl.ds(peer * n_loc + g * GROUP, GROUP)], x_buf.at[grp(g), mine + xx, yy],
            ys_send.at[g, k], ys_recv.at[g, k], {"ep": peer},
        )

    def y_local(g):
        return pltpu.make_async_copy(
            rows_hbm.at[pl.ds(yy * n_loc + g * GROUP, GROUP)], x_buf.at[grp(g), mine + xx, yy], ys_loc.at[g]
        )

    def block_copy(g, blk, send, recv, device):
        view = x_buf.at[grp(g), mine + blk]
        return remote(view, view, send, recv, device)

    def a_copy(g, k):
        return block_copy(g, xx, a_send.at[g, k], a_recv.at[g, k], (right, left)[k])

    def b_copy(g, k):
        view = x_buf.at[grp(g), mine + (xl, xr)[k], pl.ds(k * half, half)]
        return remote(view, view, b_send.at[g, k], b_recv.at[g, k], (right, left)[k])

    def d_copy(g, k):
        return block_copy(g, (xx, xl, xr, xo)[k], d_send.at[g, k], d_recv.at[g, k], mate)

    def p_copy(g):
        other = (1 - cc) * n_x
        return remote(x_buf.at[grp(g), pl.ds(other, n_x)], pair_buf.at[grp(g)], p_send.at[g], p_recv.at[g], mate)

    def e_copy(g, k):
        view = x_buf.at[grp(g), mine + xo, pl.ds(k * half, half)]
        return remote(view, opp_buf.at[k, grp(g)], e_send.at[g, k], e_recv.at[g, k], (right, left)[k])

    def f_copy(g, k):
        view = x_buf.at[grp(g), mine + (xr, xl)[k]]
        return remote(view, nbr_buf.at[k, grp(g)], f_send.at[g, k], f_recv.at[g, k], (right, left)[k])

    def h_copy(g, k, peer):
        return remote(
            x_buf.at[grp(g), mine + xx, peer], out_hbm.at[pl.ds(yy * n_loc + g * GROUP, GROUP)],
            h_send.at[g, k], h_recv.at[g, k], {"ep": peer},
        )

    def h_local(g):
        return pltpu.make_async_copy(
            x_buf.at[grp(g), mine + xx, yy], out_hbm.at[pl.ds(yy * n_loc + g * GROUP, GROUP)], h_loc.at[g]
        )

    def w_copies(g):
        s = g % 2
        return (
            pltpu.make_async_copy(wg_hbm.at[grp(g)], w_in.at[s, :, :, pl.ds(0, hidden)], w_sem.at[s, 0]),
            pltpu.make_async_copy(wu_hbm.at[grp(g)], w_in.at[s, :, :, pl.ds(hidden, hidden)], w_sem.at[s, 1]),
            pltpu.make_async_copy(wd_hbm.at[grp(g)], w_out.at[s], w_sem.at[s, 2]),
        )

    for g in range(2):
        for c in w_copies(g):
            c.start()

    barrier = pltpu.get_barrier_semaphore()
    for device in [right, left, mate] + [{"ep": p} for p in peers]:
        pl.semaphore_signal(barrier, inc=1, device_id=device, device_id_type=MESH)
    pl.semaphore_wait(barrier, 3 + len(peers))

    @pl.loop(0, n_grp)
    def _(g):
        for k, peer in enumerate(peers):
            y_copy(g, k, peer).start()
        y_local(g).start()

    def stage_a(g):
        for k, peer in enumerate(peers):
            y_copy(g, k, peer).wait_recv()
        y_local(g).wait()
        for k in range(2):
            a_copy(g, k).start()
        d_copy(g, 0).start()

    def stage_b(g):
        for k in range(2):
            a_copy(g, k).wait_recv()
            b_copy(g, k).start()
        for k in range(2):
            d_copy(g, 1 + k).start()

    def stage_c(g):
        for k in range(2):
            b_copy(g, k).wait_recv()
        d_copy(g, 3).start()

    def stage_d(g):
        for k in range(4):
            d_copy(g, k).wait()
        for k in range(2):
            a_copy(g, k).wait_send()
            b_copy(g, k).wait_send()
        for c in w_copies(g):
            c.wait()
        s = g % 2
        blocks = 2
        per = 2 * n_x // blocks

        @pl.loop(0, GROUP * per)
        def _(j):
            el = j // per
            at = (g * GROUP + el, pl.ds((j % per) * blocks, blocks))
            tile = x_buf[at].reshape(blocks * n_y * cap, d_model)
            both = jnp.dot(tile, w_in[s, el], preferred_element_type=F32)
            pre = both[:, :hidden]
            act = (jax.nn.silu(pre) * both[:, hidden:]).astype(BF16)
            part = jnp.dot(act, w_out[s, el], preferred_element_type=F32)
            x_buf[at] = part.astype(BF16).reshape(blocks, n_y, cap, d_model)

        p_copy(g).start()

        @pl.when(g + 2 < n_grp)
        def _():
            for c in w_copies(g + 2):
                c.start()

    def stage_e(g):
        p_copy(g).wait_recv()

        @pl.loop(0, GROUP * n_y)
        def _(j):
            e, q = g * GROUP + j // n_y, j % n_y
            total = x_buf[e, mine + xo, q].astype(F32) + pair_buf[e, xo, q].astype(F32)
            x_buf[e, mine + xo, q] = total.astype(BF16)

        for k in range(2):
            e_copy(g, k).start()

    def stage_f(g):
        for k in range(2):
            e_copy(g, k).wait_recv()
            blk = (xr, xl)[k]

            @pl.loop(0, GROUP * half)
            def _(j):
                e, q = g * GROUP + j // half, j % half
                a = q + k * half
                total = x_buf[e, mine + blk, a].astype(F32) + pair_buf[e, blk, a].astype(F32)
                total = total + opp_buf[k, e, q].astype(F32)
                x_buf[e, mine + blk, a] = total.astype(BF16)
                b = q + (1 - k) * half
                rest = x_buf[e, mine + blk, b].astype(F32) + pair_buf[e, blk, b].astype(F32)
                x_buf[e, mine + blk, b] = rest.astype(BF16)

            f_copy(g, k).start()

    def stage_h(g):
        for k in range(2):
            f_copy(g, k).wait_recv()

        @pl.loop(0, GROUP * n_y)
        def _(j):
            e, q = g * GROUP + j // n_y, j % n_y
            total = x_buf[e, mine + xx, q].astype(F32) + pair_buf[e, xx, q].astype(F32)
            total = total + (nbr_buf[0, e, q].astype(F32) + nbr_buf[1, e, q].astype(F32))
            x_buf[e, mine + xx, q] = total.astype(BF16)

        for k, peer in enumerate(peers):
            h_copy(g, k, peer).start()
        h_local(g).start()

    stages = (stage_a, stage_b, stage_c, stage_d, stage_e, stage_f, stage_h)

    @pl.loop(0, n_grp + len(stages) - 1)
    def _(t):
        for lag, stage in enumerate(stages):
            g = t - lag

            @pl.when((g >= 0) & (g < n_grp))
            def _():
                stage(g)

    @pl.loop(0, n_grp)
    def _(g):
        p_copy(g).wait_send()
        for k in range(2):
            e_copy(g, k).wait_send()
            f_copy(g, k).wait_send()
        for k, peer in enumerate(peers):
            y_copy(g, k, peer).wait_send()
            h_copy(g, k, peer).wait()
        h_local(g).wait()


def experts(rows, wg, wu, wd, n_y, n_tp):
    n_exp, cap, d_model = rows.shape
    n_loc, _, hidden = wg.shape
    n_x = n_tp // 2
    half = n_y // 2
    n_grp = n_loc // GROUP
    dma = pltpu.SemaphoreType.DMA
    hbm = pl.BlockSpec(memory_space=pltpu.HBM)
    return pl.pallas_call(
        functools.partial(expert_kernel, n_y, n_x),
        out_shape=jax.ShapeDtypeStruct(rows.shape, BF16),
        in_specs=[hbm] * 4,
        out_specs=hbm,
        scratch_shapes=[
            pltpu.VMEM((n_loc, 2 * n_x, n_y, cap, d_model), BF16),
            pltpu.VMEM((n_loc, n_x, n_y, cap, d_model), BF16),
            pltpu.VMEM((2, n_loc, half, cap, d_model), BF16),
            pltpu.VMEM((2, n_loc, n_y, cap, d_model), BF16),
            pltpu.VMEM((2, GROUP, d_model, 2 * hidden), BF16),
            pltpu.VMEM((2, GROUP, hidden, d_model), BF16),
            dma((n_grp, n_y - 1)), dma((n_grp, n_y - 1)), dma((n_grp,)),
            dma((n_grp, 2)), dma((n_grp, 2)),
            dma((n_grp, 2)), dma((n_grp, 2)),
            dma((n_grp, 4)), dma((n_grp, 4)),
            dma((n_grp,)), dma((n_grp,)),
            dma((n_grp, 2)), dma((n_grp, 2)),
            dma((n_grp, 2)), dma((n_grp, 2)),
            dma((n_grp, n_y - 1)), dma((n_grp, n_y - 1)), dma((n_grp,)),
            dma((2, 3)),
        ],
        compiler_params=pltpu.CompilerParams(
            collective_id=0, has_side_effects=True, vmem_limit_bytes=67043328
        ),
        name="experts",
    )(rows, wg, wu, wd)


def solution(mesh):
    n_y, n_tp = mesh.shape["ep"], mesh.shape["tp"]
    row_spec = P(("dp", "ep", "tp"), None)

    def local_layer(x_loc, ids_loc, gate_loc, wg_loc, wu_loc, wd_loc):
        tok, d_model = x_loc.shape
        n_exp = wg_loc.shape[0] * n_y
        capacity = CAP_FACTOR * tok // n_exp
        rows, pos = dispatch(x_loc, ids_loc, n_exp, capacity)
        y = experts(rows.reshape(n_exp, capacity, d_model), wg_loc, wu_loc, wd_loc, n_y, n_tp)
        return combine(pos, gate_loc, y.reshape(n_exp * capacity, d_model))

    return jax.shard_map(local_layer, mesh=mesh, in_specs=(row_spec, row_spec, row_spec, P("ep", None, "tp"), P("ep", None, "tp"), P("ep", "tp", None)), out_specs=row_spec, check_vma=False)
```

```python
import functools

import jax
import jax.numpy as jnp
from jax import lax
from jax.experimental import pallas as pl
from jax.experimental.pallas import tpu as pltpu
from jax.sharding import PartitionSpec as P

CAP_FACTOR = 2
GROUP = 2
W_SLOTS = 4
MESH = pl.DeviceIdType.MESH
BF16 = jnp.bfloat16
F32 = jnp.float32


def dispatch_kernel(capacity, n_exp, ids_ref, x_ref, rows_ref, pos_ref):
    tok = ids_ref.shape[1]
    n_slots = rows_ref.shape[0]
    ids = ids_ref[...]
    one_hot = lax.broadcasted_iota(jnp.int32, (n_exp, tok), 0) == ids
    before = lax.broadcasted_iota(jnp.int32, (tok, tok), 0) < lax.broadcasted_iota(jnp.int32, (tok, tok), 1)
    preceding = jnp.dot(one_hot.astype(F32).astype(BF16), before.astype(F32).astype(BF16), preferred_element_type=F32)
    slot = jnp.sum(jnp.where(one_hot, preceding, 0.0), axis=0, keepdims=True).astype(jnp.int32)
    pos = jnp.where(slot < capacity, ids * capacity + slot, -1)
    pos_ref[...] = pos
    tile = 256

    @pl.loop(0, n_slots // tile)
    def _(i):
        want = lax.broadcasted_iota(jnp.int32, (tile, tok), 0) + i * tile
        pick = (want == pos).astype(F32).astype(BF16)
        start = pl.multiple_of(i * tile, tile)
        rows_ref[pl.ds(start, tile), :] = jnp.dot(pick, x_ref[...], preferred_element_type=F32).astype(BF16)


def dispatch(x_loc, ids_loc, n_exp, capacity):
    tok, d_model = x_loc.shape
    return pl.pallas_call(
        functools.partial(dispatch_kernel, capacity, n_exp),
        out_shape=(
            jax.ShapeDtypeStruct((n_exp * capacity, d_model), BF16),
            jax.ShapeDtypeStruct((1, tok), jnp.int32),
        ),
        name="dispatch",
    )(ids_loc.reshape(1, tok), x_loc)


def combine_kernel(pos_ref, gate_ref, y_ref, out_ref):
    n_slots = y_ref.shape[0]
    tok = out_ref.shape[0]
    tile = 256

    @pl.loop(0, tok // tile)
    def _(i):
        rows = pl.ds(pl.multiple_of(i * tile, tile), tile)
        pos = pos_ref[rows, :]
        pick = (lax.broadcasted_iota(jnp.int32, (tile, n_slots), 1) == pos).astype(F32).astype(BF16)
        y = jnp.dot(pick, y_ref[...], preferred_element_type=F32)
        weight = jnp.where(pos >= 0, gate_ref[rows, :], 0.0)
        out_ref[rows, :] = (y * weight).astype(BF16)


def combine(pos, gate_loc, y_slots):
    tok = gate_loc.shape[0]
    return pl.pallas_call(
        combine_kernel,
        out_shape=jax.ShapeDtypeStruct((tok, y_slots.shape[1]), BF16),
        name="combine",
    )(pos.reshape(tok, 1), gate_loc, y_slots)


def expert_kernel(
    n_y, n_x, rows_hbm, wg_hbm, wu_hbm, wd_hbm, out_hbm,
    x_buf, pair_buf, opp_buf, nbr_buf, w_in, w_out,
    ys_send, ys_recv, ys_loc, a_send, a_recv, b_send, b_recv, d_send, d_recv,
    p_send, p_recv, e_send, e_recv, f_send, f_recv, h_send, h_recv, h_loc, w_sem,
):
    n_loc, _, _, cap, d_model = x_buf.shape
    hidden = w_out.shape[2]
    n_grp = n_loc // GROUP
    half = n_y // 2
    yy = lax.axis_index("ep")
    tt = lax.axis_index("tp")
    xx, cc = tt // 2, tt % 2
    xr, xl, xo = (xx + 1) % n_x, (xx + n_x - 1) % n_x, (xx + 2) % n_x
    right, left, mate = {"tp": xr * 2 + cc}, {"tp": xl * 2 + cc}, {"tp": xx * 2 + 1 - cc}
    peers = [(yy + d) % n_y for d in range(1, n_y)]
    mine = cc * n_x

    def remote(src, dst, send, recv, device):
        return pltpu.make_async_remote_copy(
            src_ref=src, dst_ref=dst, send_sem=send, recv_sem=recv, device_id=device, device_id_type=MESH
        )

    def grp(g):
        return pl.ds(g * GROUP, GROUP)

    def y_copy(g, k, peer):
        return remote(
            rows_hbm.at[pl.ds(peer * n_loc + g * GROUP, GROUP)], x_buf.at[grp(g), mine + xx, yy],
            ys_send.at[g, k], ys_recv.at[g, k], {"ep": peer},
        )

    def y_local(g):
        return pltpu.make_async_copy(
            rows_hbm.at[pl.ds(yy * n_loc + g * GROUP, GROUP)], x_buf.at[grp(g), mine + xx, yy], ys_loc.at[g]
        )

    def block_copy(g, blk, send, recv, device):
        view = x_buf.at[grp(g), mine + blk]
        return remote(view, view, send, recv, device)

    def a_copy(g, k):
        return block_copy(g, xx, a_send.at[g, k], a_recv.at[g, k], (right, left)[k])

    def b_copy(g, k):
        view = x_buf.at[grp(g), mine + (xl, xr)[k], pl.ds(k * half, half)]
        return remote(view, view, b_send.at[g, k], b_recv.at[g, k], (right, left)[k])

    def d_copy(g, k):
        return block_copy(g, (xx, xl, xr, xo)[k], d_send.at[g, k], d_recv.at[g, k], mate)

    def p_copy(g):
        other = (1 - cc) * n_x
        return remote(x_buf.at[grp(g), pl.ds(other, n_x)], pair_buf.at[grp(g)], p_send.at[g], p_recv.at[g], mate)

    def e_copy(g, k):
        view = x_buf.at[grp(g), mine + xo, pl.ds(k * half, half)]
        return remote(view, opp_buf.at[k, grp(g)], e_send.at[g, k], e_recv.at[g, k], (right, left)[k])

    def f_copy(g, k):
        view = x_buf.at[grp(g), mine + (xr, xl)[k]]
        return remote(view, nbr_buf.at[k, grp(g)], f_send.at[g, k], f_recv.at[g, k], (right, left)[k])

    def h_copy(g, k, peer):
        return remote(
            x_buf.at[grp(g), mine + xx, peer], out_hbm.at[pl.ds(yy * n_loc + g * GROUP, GROUP)],
            h_send.at[g, k], h_recv.at[g, k], {"ep": peer},
        )

    def h_local(g):
        return pltpu.make_async_copy(
            x_buf.at[grp(g), mine + xx, yy], out_hbm.at[pl.ds(yy * n_loc + g * GROUP, GROUP)], h_loc.at[g]
        )

    def w_copies(g):
        s = g % 2
        return (
            pltpu.make_async_copy(wg_hbm.at[grp(g)], w_in.at[s, :, :, pl.ds(0, hidden)], w_sem.at[s, 0]),
            pltpu.make_async_copy(wu_hbm.at[grp(g)], w_in.at[s, :, :, pl.ds(hidden, hidden)], w_sem.at[s, 1]),
            pltpu.make_async_copy(wd_hbm.at[grp(g)], w_out.at[s], w_sem.at[s, 2]),
        )

    for g in range(2):
        for c in w_copies(g):
            c.start()

    barrier = pltpu.get_barrier_semaphore()
    for device in [right, left, mate] + [{"ep": p} for p in peers]:
        pl.semaphore_signal(barrier, inc=1, device_id=device, device_id_type=MESH)
    pl.semaphore_wait(barrier, 3 + len(peers))

    @pl.loop(0, n_grp)
    def _(g):
        for k, peer in enumerate(peers):
            y_copy(g, k, peer).start()
        y_local(g).start()

    def stage_a(g):
        for k, peer in enumerate(peers):
            y_copy(g, k, peer).wait_recv()
        y_local(g).wait()
        for k in range(2):
            a_copy(g, k).start()
        d_copy(g, 0).start()

    def stage_b(g):
        for k in range(2):
            a_copy(g, k).wait_recv()
            b_copy(g, k).start()
        for k in range(2):
            d_copy(g, 1 + k).start()

    def stage_c(g):
        for k in range(2):
            b_copy(g, k).wait_recv()
        d_copy(g, 3).start()

    def stage_d(g):
        for k in range(4):
            d_copy(g, k).wait()
        for k in range(2):
            a_copy(g, k).wait_send()
            b_copy(g, k).wait_send()
        for c in w_copies(g):
            c.wait()
        s = g % 2
        blocks = 2
        per = 2 * n_x // blocks

        @pl.loop(0, GROUP * per)
        def _(j):
            el = j // per
            at = (g * GROUP + el, pl.ds((j % per) * blocks, blocks))
            tile = x_buf[at].reshape(blocks * n_y * cap, d_model)
            both = jnp.dot(tile, w_in[s, el], preferred_element_type=F32)
            pre = both[:, :hidden]
            act = (jax.nn.silu(pre) * both[:, hidden:]).astype(BF16)
            part = jnp.dot(act, w_out[s, el], preferred_element_type=F32)
            x_buf[at] = part.astype(BF16).reshape(blocks, n_y, cap, d_model)

        p_copy(g).start()

        @pl.when(g + 2 < n_grp)
        def _():
            for c in w_copies(g + 2):
                c.start()

    def stage_e(g):
        p_copy(g).wait_recv()

        @pl.loop(0, GROUP * n_y)
        def _(j):
            e, q = g * GROUP + j // n_y, j % n_y
            total = x_buf[e, mine + xo, q].astype(F32) + pair_buf[e, xo, q].astype(F32)
            x_buf[e, mine + xo, q] = total.astype(BF16)

        for k in range(2):
            e_copy(g, k).start()

    def stage_f(g):
        for k in range(2):
            e_copy(g, k).wait_recv()
            blk = (xr, xl)[k]

            @pl.loop(0, GROUP * half)
            def _(j):
                e, q = g * GROUP + j // half, j % half
                a = q + k * half
                total = x_buf[e, mine + blk, a].astype(F32) + pair_buf[e, blk, a].astype(F32)
                total = total + opp_buf[k, e, q].astype(F32)
                x_buf[e, mine + blk, a] = total.astype(BF16)
                b = q + (1 - k) * half
                rest = x_buf[e, mine + blk, b].astype(F32) + pair_buf[e, blk, b].astype(F32)
                x_buf[e, mine + blk, b] = rest.astype(BF16)

            f_copy(g, k).start()

    def stage_h(g):
        for k in range(2):
            f_copy(g, k).wait_recv()

        @pl.loop(0, GROUP * n_y)
        def _(j):
            e, q = g * GROUP + j // n_y, j % n_y
            total = x_buf[e, mine + xx, q].astype(F32) + pair_buf[e, xx, q].astype(F32)
            total = total + (nbr_buf[0, e, q].astype(F32) + nbr_buf[1, e, q].astype(F32))
            x_buf[e, mine + xx, q] = total.astype(BF16)

        for k, peer in enumerate(peers):
            h_copy(g, k, peer).start()
        h_local(g).start()

    stages = (stage_a, stage_b, stage_c, stage_d, stage_e, stage_f, stage_h)

    @pl.loop(0, n_grp + len(stages) - 1)
    def _(t):
        for lag, stage in enumerate(stages):
            g = t - lag

            @pl.when((g >= 0) & (g < n_grp))
            def _():
                stage(g)

    @pl.loop(0, n_grp)
    def _(g):
        p_copy(g).wait_send()
        for k in range(2):
            e_copy(g, k).wait_send()
            f_copy(g, k).wait_send()
        for k, peer in enumerate(peers):
            y_copy(g, k, peer).wait_send()
            h_copy(g, k, peer).wait()
        h_local(g).wait()


def experts(rows, wg, wu, wd, n_y, n_tp):
    n_exp, cap, d_model = rows.shape
    n_loc, _, hidden = wg.shape
    n_x = n_tp // 2
    half = n_y // 2
    n_grp = n_loc // GROUP
    dma = pltpu.SemaphoreType.DMA
    hbm = pl.BlockSpec(memory_space=pltpu.HBM)
    return pl.pallas_call(
        functools.partial(expert_kernel, n_y, n_x),
        out_shape=jax.ShapeDtypeStruct(rows.shape, BF16),
        in_specs=[hbm] * 4,
        out_specs=hbm,
        scratch_shapes=[
            pltpu.VMEM((n_loc, 2 * n_x, n_y, cap, d_model), BF16),
            pltpu.VMEM((n_loc, n_x, n_y, cap, d_model), BF16),
            pltpu.VMEM((2, n_loc, half, cap, d_model), BF16),
            pltpu.VMEM((2, n_loc, n_y, cap, d_model), BF16),
            pltpu.VMEM((2, GROUP, d_model, 2 * hidden), BF16),
            pltpu.VMEM((2, GROUP, hidden, d_model), BF16),
            dma((n_grp, n_y - 1)), dma((n_grp, n_y - 1)), dma((n_grp,)),
            dma((n_grp, 2)), dma((n_grp, 2)),
            dma((n_grp, 2)), dma((n_grp, 2)),
            dma((n_grp, 4)), dma((n_grp, 4)),
            dma((n_grp,)), dma((n_grp,)),
            dma((n_grp, 2)), dma((n_grp, 2)),
            dma((n_grp, 2)), dma((n_grp, 2)),
            dma((n_grp, n_y - 1)), dma((n_grp, n_y - 1)), dma((n_grp,)),
            dma((2, 3)),
        ],
        compiler_params=pltpu.CompilerParams(
            collective_id=0, has_side_effects=True, vmem_limit_bytes=67043328
        ),
        name="experts",
    )(rows, wg, wu, wd)


def route_kernel(
    n_y, n_tp, n_exp, capacity, ids_ref, x_ref, rows_ref, pos_ref, table_ref, most_ref,
    meta, col_send, col_recv, row_send, row_recv,
):
    tok = ids_ref.shape[1]
    packed = rows_ref.shape[1]
    width = table_ref.shape[2]
    n_loc = n_exp // n_y
    yy = lax.axis_index("ep")
    tt = lax.axis_index("tp")
    y_peers = [(yy + d) % n_y for d in range(1, n_y)]
    t_peers = [(tt + d) % n_tp for d in range(1, n_tp)]

    barrier = pltpu.get_barrier_semaphore()
    for device in [{"ep": p} for p in y_peers] + [{"tp": p} for p in t_peers]:
        pl.semaphore_signal(barrier, inc=1, device_id=device, device_id_type=MESH)

    ids = ids_ref[...]
    one_hot = lax.broadcasted_iota(jnp.int32, (n_exp, tok), 0) == ids
    before = lax.broadcasted_iota(jnp.int32, (tok, tok), 0) < lax.broadcasted_iota(jnp.int32, (tok, tok), 1)
    before = before.astype(F32).astype(BF16)
    preceding = jnp.dot(one_hot.astype(F32).astype(BF16), before, preferred_element_type=F32)
    slot = jnp.sum(jnp.where(one_hot, preceding, 0.0), axis=0, keepdims=True)
    kept = slot < capacity
    rank = ids // n_loc
    pad = 8
    to_rank = (lax.broadcasted_iota(jnp.int32, (pad, tok), 0) == rank) & kept
    ahead = jnp.dot(to_rank.astype(F32).astype(BF16), before, preferred_element_type=F32)
    place = jnp.sum(jnp.where(to_rank, ahead, 0.0), axis=0, keepdims=True).astype(jnp.int32)
    counts = jnp.sum(to_rank.astype(F32), axis=1, keepdims=True)
    most = jnp.max(counts, axis=0, keepdims=True).astype(jnp.int32)
    fits = kept & (place < packed)
    pos_ref[...] = jnp.where(fits, rank * packed + place, -1)
    key = jnp.where(fits, rank * tok + place, -1)
    row_id = lax.broadcasted_iota(jnp.int32, (pad, tok), 0)
    parts = jnp.where(row_id == 0, (ids % n_loc).astype(F32), jnp.where(row_id == 1, slot, 1.0))
    parts = jnp.where(kept, parts, 0.0).astype(BF16)

    def pick(r):
        return ((lax.broadcasted_iota(jnp.int32, (packed, tok), 0) + r * tok) == key).astype(F32).astype(BF16)

    @pl.loop(0, n_y)
    def _(r):
        got = lax.dot_general(parts, pick(r), (((1,), (1,)), ((), ())), preferred_element_type=F32)
        where = jnp.where(got[2:3] > 0.5, got[0:1] * capacity + got[1:2], -1.0)
        meta[r, :, 0:packed] = where.astype(jnp.int32)
        meta[r, :, packed:width] = jnp.broadcast_to(most, (1, width - packed))

    pl.semaphore_wait(barrier, len(y_peers) + len(t_peers))
    table_ref[pl.ds(tt * n_y + yy, 1)] = meta[pl.ds(yy, 1)]

    def col_copy(k):
        return pltpu.make_async_remote_copy(
            src_ref=meta.at[y_peers[k]], dst_ref=table_ref.at[tt * n_y + yy],
            send_sem=col_send.at[k], recv_sem=col_recv.at[k], device_id={"ep": y_peers[k]}, device_id_type=MESH,
        )

    def col_arrival(k):
        src = (yy + n_y - 1 - k) % n_y
        return pltpu.make_async_remote_copy(
            src_ref=meta.at[src], dst_ref=table_ref.at[tt * n_y + src],
            send_sem=col_send.at[k], recv_sem=col_recv.at[k], device_id={"ep": src}, device_id_type=MESH,
        )

    def row_copy(k):
        view = table_ref.at[pl.ds(tt * n_y, n_y)]
        return pltpu.make_async_remote_copy(
            src_ref=view, dst_ref=view,
            send_sem=row_send.at[k], recv_sem=row_recv.at[k], device_id={"tp": t_peers[k]}, device_id_type=MESH,
        )

    def row_arrival(k):
        src = (tt + n_tp - 1 - k) % n_tp
        view = table_ref.at[pl.ds(src * n_y, n_y)]
        return pltpu.make_async_remote_copy(
            src_ref=view, dst_ref=view,
            send_sem=row_send.at[k], recv_sem=row_recv.at[k], device_id={"tp": src}, device_id_type=MESH,
        )

    for k in range(len(y_peers)):
        col_copy(k).start()

    @pl.loop(0, n_y)
    def _(r):
        rows_ref[r] = jnp.dot(pick(r), x_ref[...], preferred_element_type=F32).astype(BF16)

    for k in range(len(y_peers)):
        col_arrival(k).wait_recv()
    for k in range(len(t_peers)):
        row_copy(k).start()
    for k in range(len(t_peers)):
        row_arrival(k).wait_recv()
    most_ref[...] = jnp.max(table_ref[:, :, packed:width], axis=0)
    for k in range(len(y_peers)):
        col_copy(k).wait_send()
    for k in range(len(t_peers)):
        row_copy(k).wait_send()


def route(x_loc, ids_loc, n_exp, capacity, packed, n_y, n_tp):
    tok, d_model = x_loc.shape
    width = -(-(packed + 1) // 128) * 128
    dma = pltpu.SemaphoreType.DMA
    return pl.pallas_call(
        functools.partial(route_kernel, n_y, n_tp, n_exp, capacity),
        out_shape=(
            jax.ShapeDtypeStruct((n_y, packed, d_model), BF16),
            jax.ShapeDtypeStruct((1, tok), jnp.int32),
            jax.ShapeDtypeStruct((n_y * n_tp, 1, width), jnp.int32),
            jax.ShapeDtypeStruct((1, width - packed), jnp.int32),
        ),
        scratch_shapes=[
            pltpu.VMEM((n_y, 1, width), jnp.int32),
            dma((n_y - 1,)), dma((n_y - 1,)), dma((n_tp - 1,)), dma((n_tp - 1,)),
        ],
        compiler_params=pltpu.CompilerParams(collective_id=1, has_side_effects=True),
        name="route",
    )(ids_loc.reshape(1, tok), x_loc)


def packed_kernel(
    n_y, n_x, cap, table_ref, rows_hbm, wg_hbm, wu_hbm, wd_hbm, out_hbm,
    x_buf, slot_buf, pair_buf, opp_buf, nbr_buf, w_in, w_out,
    ys_send, ys_recv, ys_loc, a_send, a_recv, b_send, b_recv, d_send, d_recv,
    p_send, p_recv, e_send, e_recv, n_send, n_recv, f_send, f_recv, h_send, h_recv, h_loc, w_sem,
):
    _, _, packed, d_model = x_buf.shape
    n_loc = slot_buf.shape[0]
    n_slots = n_loc * cap
    hidden = w_out.shape[2]
    half = packed // 2
    n_src = 2 * n_x
    n_grp = n_loc // GROUP
    n_w = n_y * n_grp
    yy = lax.axis_index("ep")
    tt = lax.axis_index("tp")
    xx, cc = tt // 2, tt % 2
    xr, xl, xo = (xx + 1) % n_x, (xx + n_x - 1) % n_x, (xx + 2) % n_x
    right, left, mate = {"tp": xr * 2 + cc}, {"tp": xl * 2 + cc}, {"tp": xx * 2 + 1 - cc}
    sides = (right, left)
    ahead, behind = (xr, xl), (xl, xr)
    mine, other = cc * n_x, (1 - cc) * n_x

    def remote(src, dst, send, recv, device):
        return pltpu.make_async_remote_copy(
            src_ref=src, dst_ref=dst, send_sem=send, recv_sem=recv, device_id=device, device_id_type=MESH
        )

    def part(h):
        return pl.ds(h * half, half)

    def y_copy(k):
        q = n_y - k
        peer = (yy + k) % n_y
        return remote(rows_hbm.at[peer], x_buf.at[q, mine + xx], ys_send.at[q], ys_recv.at[q], {"ep": peer})

    def y_local():
        return pltpu.make_async_copy(rows_hbm.at[yy], x_buf.at[0, mine + xx], ys_loc)

    def a_copy(t, k, h):
        view = x_buf.at[t, mine + xx, part(h)]
        return remote(view, view, a_send.at[t, k, h], a_recv.at[t, k, h], sides[k])

    def a_arrival(t, k, h):
        view = x_buf.at[t, mine + behind[k], part(h)]
        return remote(view, view, a_send.at[t, k, h], a_recv.at[t, k, h], sides[k])

    def b_copy(t, k):
        view = x_buf.at[t, mine + behind[k], part(k)]
        return remote(view, view, b_send.at[t, k], b_recv.at[t, k], sides[k])

    def b_arrival(t, k):
        view = x_buf.at[t, mine + xo, part(k)]
        return remote(view, view, b_send.at[t, k], b_recv.at[t, k], sides[k])

    def d_copy(t, k):
        view = x_buf.at[t, mine + (xx, xl, xr, xo)[k]]
        return remote(view, view, d_send.at[t, k], d_recv.at[t, k], mate)

    def d_arrival(t, k):
        view = x_buf.at[t, other + (xx, xl, xr, xo)[k]]
        return remote(view, view, d_send.at[t, k], d_recv.at[t, k], mate)

    def p_copy(t):
        return remote(x_buf.at[t, pl.ds(other, n_x)], pair_buf.at[t], p_send.at[t], p_recv.at[t], mate)

    def e_copy(t, k):
        return remote(
            x_buf.at[t, mine + xo, part(k)], opp_buf.at[k, t], e_send.at[t, k], e_recv.at[t, k], sides[k]
        )

    def n_copy(t, k):
        h = 1 - k
        return remote(
            x_buf.at[t, mine + ahead[k], part(h)], nbr_buf.at[k, t, part(h)],
            n_send.at[t, k], n_recv.at[t, k], sides[k],
        )

    def f_copy(t, k):
        return remote(
            x_buf.at[t, mine + ahead[k], part(k)], nbr_buf.at[k, t, part(k)],
            f_send.at[t, k], f_recv.at[t, k], sides[k],
        )

    def h_copy(t):
        return remote(x_buf.at[t, mine + xx], out_hbm.at[yy], h_send.at[t], h_recv.at[t], {"ep": (yy + t) % n_y})

    def h_arrival(t):
        return remote(
            x_buf.at[t, mine + xx], out_hbm.at[(yy + n_y - t) % n_y], h_send.at[t], h_recv.at[t],
            {"ep": (yy + t) % n_y},
        )

    def h_local():
        return pltpu.make_async_copy(x_buf.at[0, mine + xx], out_hbm.at[yy], h_loc)

    def w_copies(w):
        s = w % W_SLOTS
        at = pl.ds((w % n_grp) * GROUP, GROUP)
        return (
            pltpu.make_async_copy(wg_hbm.at[at], w_in.at[s, :, :, pl.ds(0, hidden)], w_sem.at[s, 0]),
            pltpu.make_async_copy(wu_hbm.at[at], w_in.at[s, :, :, pl.ds(hidden, hidden)], w_sem.at[s, 1]),
            pltpu.make_async_copy(wd_hbm.at[at], w_out.at[s], w_sem.at[s, 2]),
        )

    y_local().start()
    for w in range(W_SLOTS):
        for c in w_copies(w):
            c.start()

    barrier = pltpu.get_barrier_semaphore()
    for device in [right, left, mate] + [{"ep": (yy + d) % n_y} for d in range(1, n_y)]:
        pl.semaphore_signal(barrier, inc=1, device_id=device, device_id_type=MESH)
    pl.semaphore_wait(barrier, 2 + n_y)

    for k in range(n_y - 1, 0, -1):
        y_copy(k).start()

    def send_own(t):
        for h in range(2):
            for k in range(2):
                a_copy(t, k, h if k == 0 else 1 - h).start()
        d_copy(t, 0).start()

    def pass_on(t):
        for k in range(2):
            a_arrival(t, k, k).wait_recv()
            b_copy(t, k).start()

    def share(t):
        for k in range(2):
            a_arrival(t, k, 1 - k).wait_recv()
            d_copy(t, 1 + k).start()

    def source_row(t, b):
        row = table_ref[(b % n_x * 2 + b // n_x) * n_y + (yy + t) % n_y]
        return row[:, :packed]

    def spread(t):
        @pl.loop(0, n_src)
        def _(b):
            to = source_row(t, b)
            pick = (lax.broadcasted_iota(jnp.int32, (n_slots, packed), 0) == to).astype(F32).astype(BF16)
            slots = jnp.dot(pick, x_buf[t, b], preferred_element_type=F32).astype(BF16)
            slot_buf[:, b] = slots.reshape(n_loc, cap, d_model)

    def multiply(t):
        @pl.loop(0, n_grp)
        def _(i):
            w = t * n_grp + i
            s = w % W_SLOTS
            for c in w_copies(w):
                c.wait()

            @pl.loop(0, GROUP)
            def _(el):
                e = i * GROUP + el
                tile = slot_buf[e].reshape(n_src * cap, d_model)
                both = jnp.dot(tile, w_in[s, el], preferred_element_type=F32)
                act = (jax.nn.silu(both[:, :hidden]) * both[:, hidden:]).astype(BF16)
                out = jnp.dot(act, w_out[s, el], preferred_element_type=F32)
                slot_buf[e] = out.astype(BF16).reshape(n_src, cap, d_model)

            @pl.when(w + W_SLOTS < n_w)
            def _():
                for c in w_copies(w + W_SLOTS):
                    c.start()

    def gather_back(t, base):
        @pl.loop(0, n_x)
        def _(j):
            b = base + j
            to = source_row(t, b).astype(F32)
            col = jnp.transpose(jnp.broadcast_to(to, (128, packed)))
            lane = lax.broadcasted_iota(jnp.int32, (packed, 128), 1).astype(F32)
            pick = jnp.concatenate(
                [(col == lane + float(128 * m)).astype(F32).astype(BF16) for m in range(n_slots // 128)], axis=1
            )
            slots = slot_buf[:, b].reshape(n_slots, d_model)
            x_buf[t, b] = jnp.dot(pick, slots, preferred_element_type=F32).astype(BF16)

    def pair_sum(t, blk, h, extra=None):
        total = x_buf[t, mine + blk, h * half:(h + 1) * half].astype(F32)
        total = total + pair_buf[t, blk, h * half:(h + 1) * half].astype(F32)
        if extra is not None:
            total = total + extra.astype(F32)
        x_buf[t, mine + blk, h * half:(h + 1) * half] = total.astype(BF16)

    def first_sums(t):
        p_copy(t).wait_recv()
        for k in range(2):
            pair_sum(t, xo, k)
            e_copy(t, k).start()
        for k in range(2):
            pair_sum(t, ahead[k], 1 - k)
            n_copy(t, k).start()

    def last_sums(t):
        for k in range(2):
            e_copy(t, k).wait_recv()
            pair_sum(t, ahead[k], k, opp_buf[k, t])
            f_copy(t, k).start()

    def give_back(t):
        for k in range(2):
            n_copy(t, k).wait_recv()
            f_copy(t, k).wait_recv()
        for h in range(2):
            at = slice(h * half, (h + 1) * half)
            pair_sum(t, xx, h, nbr_buf[0, t, at].astype(F32) + nbr_buf[1, t, at].astype(F32))

        @pl.when(t == 0)
        def _():
            h_local().start()

        @pl.when(t > 0)
        def _():
            h_copy(t).start()

    def own_rows(t):
        y_copy(n_y - t).wait_recv()

    y_local().wait()
    send_own(0)
    pass_on(0)
    own_rows(1)
    send_own(1)
    share(0)

    @pl.loop(0, n_y)
    def _(t):
        for k in range(2):
            b_arrival(t, k).wait_recv()
        d_copy(t, 3).start()
        for k in range(4):
            d_arrival(t, k).wait_recv()
        spread(t)

        @pl.when(t + 1 < n_y)
        def _():
            pass_on(t + 1)

        @pl.when(t + 2 < n_y)
        def _():
            own_rows(t + 2)
            send_own(t + 2)

        multiply(t)

        @pl.when(t + 1 < n_y)
        def _():
            share(t + 1)

        @pl.when(t > 0)
        def _():
            last_sums(t - 1)

        for k in range(2):
            for h in range(2):
                a_copy(t, k, h).wait_send()
            b_copy(t, k).wait_send()
        for k in range(4):
            d_copy(t, k).wait_send()
        gather_back(t, other)
        p_copy(t).start()
        gather_back(t, mine)
        first_sums(t)

        @pl.when(t > 1)
        def _():
            give_back(t - 2)

    last_sums(n_y - 1)
    give_back(n_y - 2)
    give_back(n_y - 1)

    for k in range(1, n_y):
        y_copy(k).wait_send()
        h_copy(k).wait_send()
        h_arrival(k).wait_recv()
    h_local().wait()

    @pl.loop(0, n_y)
    def _(t):
        p_copy(t).wait_send()
        for k in range(2):
            e_copy(t, k).wait_send()
            n_copy(t, k).wait_send()
            f_copy(t, k).wait_send()


def packed_experts(table, rows, wg, wu, wd, n_tp, cap):
    n_y, packed, d_model = rows.shape
    n_loc, _, hidden = wg.shape
    n_x = n_tp // 2
    half = packed // 2
    dma = pltpu.SemaphoreType.DMA
    hbm = pl.BlockSpec(memory_space=pltpu.HBM)
    return pl.pallas_call(
        functools.partial(packed_kernel, n_y, n_x, cap),
        out_shape=jax.ShapeDtypeStruct(rows.shape, BF16),
        in_specs=[pl.BlockSpec(memory_space=pltpu.VMEM)] + [hbm] * 4,
        out_specs=hbm,
        scratch_shapes=[
            pltpu.VMEM((n_y, 2 * n_x, packed, d_model), BF16),
            pltpu.VMEM((n_loc, 2 * n_x, cap, d_model), BF16),
            pltpu.VMEM((n_y, n_x, packed, d_model), BF16),
            pltpu.VMEM((2, n_y, half, d_model), BF16),
            pltpu.VMEM((2, n_y, packed, d_model), BF16),
            pltpu.VMEM((W_SLOTS, GROUP, d_model, 2 * hidden), BF16),
            pltpu.VMEM((W_SLOTS, GROUP, hidden, d_model), BF16),
            dma((n_y,)), dma((n_y,)), dma,
            dma((n_y, 2, 2)), dma((n_y, 2, 2)),
            dma((n_y, 2)), dma((n_y, 2)),
            dma((n_y, 4)), dma((n_y, 4)),
            dma((n_y,)), dma((n_y,)),
            dma((n_y, 2)), dma((n_y, 2)),
            dma((n_y, 2)), dma((n_y, 2)),
            dma((n_y, 2)), dma((n_y, 2)),
            dma((n_y,)), dma((n_y,)), dma,
            dma((W_SLOTS, 3)),
        ],
        compiler_params=pltpu.CompilerParams(
            collective_id=2, has_side_effects=True, vmem_limit_bytes=67043328
        ),
        name="packed_experts",
    )(table, rows, wg, wu, wd)


def solution(mesh):
    n_y, n_tp = mesh.shape["ep"], mesh.shape["tp"]
    row_spec = P(("dp", "ep", "tp"), None)

    def local_layer(x_loc, ids_loc, gate_loc, wg_loc, wu_loc, wd_loc):
        tok, d_model = x_loc.shape
        n_loc = wg_loc.shape[0]
        n_exp = n_loc * n_y
        capacity = CAP_FACTOR * tok // n_exp
        packed = n_loc * capacity * 5 // 8
        rows, pos, table, most = route(x_loc, ids_loc, n_exp, capacity, packed, n_y, n_tp)

        def by_rows():
            y = packed_experts(table, rows, wg_loc, wu_loc, wd_loc, n_tp, capacity)
            return combine(pos, gate_loc, y.reshape(n_y * packed, d_model))

        def by_slots():
            rows, pos = dispatch(x_loc, ids_loc, n_exp, capacity)
            y = experts(rows.reshape(n_exp, capacity, d_model), wg_loc, wu_loc, wd_loc, n_y, n_tp)
            return combine(pos, gate_loc, y.reshape(n_exp * capacity, d_model))

        return lax.cond(most[0, 0] <= packed, by_rows, by_slots)

    return jax.shard_map(local_layer, mesh=mesh, in_specs=(row_spec, row_spec, row_spec, P("ep", None, "tp"), P("ep", None, "tp"), P("ep", "tp", None)), out_specs=row_spec, check_vma=False)
```

```python
import functools

import jax
import jax.numpy as jnp
from jax import lax
from jax.experimental import pallas as pl
from jax.experimental.pallas import tpu as pltpu
from jax.sharding import PartitionSpec as P

CAP_FACTOR = 2
GROUP = 2
W_SLOTS = 4
MESH = pl.DeviceIdType.MESH
BF16 = jnp.bfloat16
F32 = jnp.float32


def dispatch_kernel(capacity, n_exp, ids_ref, x_ref, rows_ref, pos_ref):
    tok = ids_ref.shape[1]
    n_slots = rows_ref.shape[0]
    ids = ids_ref[...]
    one_hot = lax.broadcasted_iota(jnp.int32, (n_exp, tok), 0) == ids
    before = lax.broadcasted_iota(jnp.int32, (tok, tok), 0) < lax.broadcasted_iota(jnp.int32, (tok, tok), 1)
    preceding = jnp.dot(one_hot.astype(F32).astype(BF16), before.astype(F32).astype(BF16), preferred_element_type=F32)
    slot = jnp.sum(jnp.where(one_hot, preceding, 0.0), axis=0, keepdims=True).astype(jnp.int32)
    pos = jnp.where(slot < capacity, ids * capacity + slot, -1)
    pos_ref[...] = pos
    tile = 256

    @pl.loop(0, n_slots // tile)
    def _(i):
        want = lax.broadcasted_iota(jnp.int32, (tile, tok), 0) + i * tile
        pick = (want == pos).astype(F32).astype(BF16)
        start = pl.multiple_of(i * tile, tile)
        rows_ref[pl.ds(start, tile), :] = jnp.dot(pick, x_ref[...], preferred_element_type=F32).astype(BF16)


def dispatch(x_loc, ids_loc, n_exp, capacity):
    tok, d_model = x_loc.shape
    return pl.pallas_call(
        functools.partial(dispatch_kernel, capacity, n_exp),
        out_shape=(
            jax.ShapeDtypeStruct((n_exp * capacity, d_model), BF16),
            jax.ShapeDtypeStruct((1, tok), jnp.int32),
        ),
        name="dispatch",
    )(ids_loc.reshape(1, tok), x_loc)


def combine_kernel(pos_ref, gate_ref, y_ref, out_ref):
    n_slots = y_ref.shape[0]
    tok = out_ref.shape[0]
    tile = 256

    @pl.loop(0, tok // tile)
    def _(i):
        rows = pl.ds(pl.multiple_of(i * tile, tile), tile)
        pos = pos_ref[rows, :]
        pick = (lax.broadcasted_iota(jnp.int32, (tile, n_slots), 1) == pos).astype(F32).astype(BF16)
        y = jnp.dot(pick, y_ref[...], preferred_element_type=F32)
        weight = jnp.where(pos >= 0, gate_ref[rows, :], 0.0)
        out_ref[rows, :] = (y * weight).astype(BF16)


def combine(pos, gate_loc, y_slots):
    tok = gate_loc.shape[0]
    return pl.pallas_call(
        combine_kernel,
        out_shape=jax.ShapeDtypeStruct((tok, y_slots.shape[1]), BF16),
        name="combine",
    )(pos.reshape(tok, 1), gate_loc, y_slots)


def expert_kernel(
    n_y, n_x, rows_hbm, wg_hbm, wu_hbm, wd_hbm, out_hbm,
    x_buf, pair_buf, opp_buf, nbr_buf, w_in, w_out,
    ys_send, ys_recv, ys_loc, a_send, a_recv, b_send, b_recv, d_send, d_recv,
    p_send, p_recv, e_send, e_recv, f_send, f_recv, h_send, h_recv, h_loc, w_sem,
):
    n_loc, _, _, cap, d_model = x_buf.shape
    hidden = w_out.shape[2]
    n_grp = n_loc // GROUP
    half = n_y // 2
    yy = lax.axis_index("ep")
    tt = lax.axis_index("tp")
    xx, cc = tt // 2, tt % 2
    xr, xl, xo = (xx + 1) % n_x, (xx + n_x - 1) % n_x, (xx + 2) % n_x
    right, left, mate = {"tp": xr * 2 + cc}, {"tp": xl * 2 + cc}, {"tp": xx * 2 + 1 - cc}
    peers = [(yy + d) % n_y for d in range(1, n_y)]
    mine = cc * n_x

    def remote(src, dst, send, recv, device):
        return pltpu.make_async_remote_copy(
            src_ref=src, dst_ref=dst, send_sem=send, recv_sem=recv, device_id=device, device_id_type=MESH
        )

    def grp(g):
        return pl.ds(g * GROUP, GROUP)

    def y_copy(g, k, peer):
        return remote(
            rows_hbm.at[pl.ds(peer * n_loc + g * GROUP, GROUP)], x_buf.at[grp(g), mine + xx, yy],
            ys_send.at[g, k], ys_recv.at[g, k], {"ep": peer},
        )

    def y_local(g):
        return pltpu.make_async_copy(
            rows_hbm.at[pl.ds(yy * n_loc + g * GROUP, GROUP)], x_buf.at[grp(g), mine + xx, yy], ys_loc.at[g]
        )

    def block_copy(g, blk, send, recv, device):
        view = x_buf.at[grp(g), mine + blk]
        return remote(view, view, send, recv, device)

    def a_copy(g, k):
        return block_copy(g, xx, a_send.at[g, k], a_recv.at[g, k], (right, left)[k])

    def b_copy(g, k):
        view = x_buf.at[grp(g), mine + (xl, xr)[k], pl.ds(k * half, half)]
        return remote(view, view, b_send.at[g, k], b_recv.at[g, k], (right, left)[k])

    def d_copy(g, k):
        return block_copy(g, (xx, xl, xr, xo)[k], d_send.at[g, k], d_recv.at[g, k], mate)

    def p_copy(g):
        other = (1 - cc) * n_x
        return remote(x_buf.at[grp(g), pl.ds(other, n_x)], pair_buf.at[grp(g)], p_send.at[g], p_recv.at[g], mate)

    def e_copy(g, k):
        view = x_buf.at[grp(g), mine + xo, pl.ds(k * half, half)]
        return remote(view, opp_buf.at[k, grp(g)], e_send.at[g, k], e_recv.at[g, k], (right, left)[k])

    def f_copy(g, k):
        view = x_buf.at[grp(g), mine + (xr, xl)[k]]
        return remote(view, nbr_buf.at[k, grp(g)], f_send.at[g, k], f_recv.at[g, k], (right, left)[k])

    def h_copy(g, k, peer):
        return remote(
            x_buf.at[grp(g), mine + xx, peer], out_hbm.at[pl.ds(yy * n_loc + g * GROUP, GROUP)],
            h_send.at[g, k], h_recv.at[g, k], {"ep": peer},
        )

    def h_local(g):
        return pltpu.make_async_copy(
            x_buf.at[grp(g), mine + xx, yy], out_hbm.at[pl.ds(yy * n_loc + g * GROUP, GROUP)], h_loc.at[g]
        )

    def w_copies(g):
        s = g % 2
        return (
            pltpu.make_async_copy(wg_hbm.at[grp(g)], w_in.at[s, :, :, pl.ds(0, hidden)], w_sem.at[s, 0]),
            pltpu.make_async_copy(wu_hbm.at[grp(g)], w_in.at[s, :, :, pl.ds(hidden, hidden)], w_sem.at[s, 1]),
            pltpu.make_async_copy(wd_hbm.at[grp(g)], w_out.at[s], w_sem.at[s, 2]),
        )

    for g in range(2):
        for c in w_copies(g):
            c.start()

    barrier = pltpu.get_barrier_semaphore()
    for device in [right, left, mate] + [{"ep": p} for p in peers]:
        pl.semaphore_signal(barrier, inc=1, device_id=device, device_id_type=MESH)
    pl.semaphore_wait(barrier, 3 + len(peers))

    @pl.loop(0, n_grp)
    def _(g):
        for k, peer in enumerate(peers):
            y_copy(g, k, peer).start()
        y_local(g).start()

    def stage_a(g):
        for k, peer in enumerate(peers):
            y_copy(g, k, peer).wait_recv()
        y_local(g).wait()
        for k in range(2):
            a_copy(g, k).start()
        d_copy(g, 0).start()

    def stage_b(g):
        for k in range(2):
            a_copy(g, k).wait_recv()
            b_copy(g, k).start()
        for k in range(2):
            d_copy(g, 1 + k).start()

    def stage_c(g):
        for k in range(2):
            b_copy(g, k).wait_recv()
        d_copy(g, 3).start()

    def stage_d(g):
        for k in range(4):
            d_copy(g, k).wait()
        for k in range(2):
            a_copy(g, k).wait_send()
            b_copy(g, k).wait_send()
        for c in w_copies(g):
            c.wait()
        s = g % 2
        blocks = 2
        per = 2 * n_x // blocks

        @pl.loop(0, GROUP * per)
        def _(j):
            el = j // per
            at = (g * GROUP + el, pl.ds((j % per) * blocks, blocks))
            tile = x_buf[at].reshape(blocks * n_y * cap, d_model)
            both = jnp.dot(tile, w_in[s, el], preferred_element_type=F32)
            pre = both[:, :hidden]
            act = (jax.nn.silu(pre) * both[:, hidden:]).astype(BF16)
            part = jnp.dot(act, w_out[s, el], preferred_element_type=F32)
            x_buf[at] = part.astype(BF16).reshape(blocks, n_y, cap, d_model)

        p_copy(g).start()

        @pl.when(g + 2 < n_grp)
        def _():
            for c in w_copies(g + 2):
                c.start()

    def stage_e(g):
        p_copy(g).wait_recv()

        @pl.loop(0, GROUP * n_y)
        def _(j):
            e, q = g * GROUP + j // n_y, j % n_y
            total = x_buf[e, mine + xo, q].astype(F32) + pair_buf[e, xo, q].astype(F32)
            x_buf[e, mine + xo, q] = total.astype(BF16)

        for k in range(2):
            e_copy(g, k).start()

    def stage_f(g):
        for k in range(2):
            e_copy(g, k).wait_recv()
            blk = (xr, xl)[k]

            @pl.loop(0, GROUP * half)
            def _(j):
                e, q = g * GROUP + j // half, j % half
                a = q + k * half
                total = x_buf[e, mine + blk, a].astype(F32) + pair_buf[e, blk, a].astype(F32)
                total = total + opp_buf[k, e, q].astype(F32)
                x_buf[e, mine + blk, a] = total.astype(BF16)
                b = q + (1 - k) * half
                rest = x_buf[e, mine + blk, b].astype(F32) + pair_buf[e, blk, b].astype(F32)
                x_buf[e, mine + blk, b] = rest.astype(BF16)

            f_copy(g, k).start()

    def stage_h(g):
        for k in range(2):
            f_copy(g, k).wait_recv()

        @pl.loop(0, GROUP * n_y)
        def _(j):
            e, q = g * GROUP + j // n_y, j % n_y
            total = x_buf[e, mine + xx, q].astype(F32) + pair_buf[e, xx, q].astype(F32)
            total = total + (nbr_buf[0, e, q].astype(F32) + nbr_buf[1, e, q].astype(F32))
            x_buf[e, mine + xx, q] = total.astype(BF16)

        for k, peer in enumerate(peers):
            h_copy(g, k, peer).start()
        h_local(g).start()

    stages = (stage_a, stage_b, stage_c, stage_d, stage_e, stage_f, stage_h)

    @pl.loop(0, n_grp + len(stages) - 1)
    def _(t):
        for lag, stage in enumerate(stages):
            g = t - lag

            @pl.when((g >= 0) & (g < n_grp))
            def _():
                stage(g)

    @pl.loop(0, n_grp)
    def _(g):
        p_copy(g).wait_send()
        for k in range(2):
            e_copy(g, k).wait_send()
            f_copy(g, k).wait_send()
        for k, peer in enumerate(peers):
            y_copy(g, k, peer).wait_send()
            h_copy(g, k, peer).wait()
        h_local(g).wait()


def experts(rows, wg, wu, wd, n_y, n_tp):
    n_exp, cap, d_model = rows.shape
    n_loc, _, hidden = wg.shape
    n_x = n_tp // 2
    half = n_y // 2
    n_grp = n_loc // GROUP
    dma = pltpu.SemaphoreType.DMA
    hbm = pl.BlockSpec(memory_space=pltpu.HBM)
    return pl.pallas_call(
        functools.partial(expert_kernel, n_y, n_x),
        out_shape=jax.ShapeDtypeStruct(rows.shape, BF16),
        in_specs=[hbm] * 4,
        out_specs=hbm,
        scratch_shapes=[
            pltpu.VMEM((n_loc, 2 * n_x, n_y, cap, d_model), BF16),
            pltpu.VMEM((n_loc, n_x, n_y, cap, d_model), BF16),
            pltpu.VMEM((2, n_loc, half, cap, d_model), BF16),
            pltpu.VMEM((2, n_loc, n_y, cap, d_model), BF16),
            pltpu.VMEM((2, GROUP, d_model, 2 * hidden), BF16),
            pltpu.VMEM((2, GROUP, hidden, d_model), BF16),
            dma((n_grp, n_y - 1)), dma((n_grp, n_y - 1)), dma((n_grp,)),
            dma((n_grp, 2)), dma((n_grp, 2)),
            dma((n_grp, 2)), dma((n_grp, 2)),
            dma((n_grp, 4)), dma((n_grp, 4)),
            dma((n_grp,)), dma((n_grp,)),
            dma((n_grp, 2)), dma((n_grp, 2)),
            dma((n_grp, 2)), dma((n_grp, 2)),
            dma((n_grp, n_y - 1)), dma((n_grp, n_y - 1)), dma((n_grp,)),
            dma((2, 3)),
        ],
        compiler_params=pltpu.CompilerParams(
            collective_id=0, has_side_effects=True, vmem_limit_bytes=67043328
        ),
        name="experts",
    )(rows, wg, wu, wd)


def route_kernel(
    n_y, n_tp, n_exp, capacity, packed, ids_ref, pos_ref, table_ref, most_ref,
    meta, col_send, col_recv, row_send, row_recv,
):
    tok = ids_ref.shape[1]
    width = table_ref.shape[2]
    n_loc = n_exp // n_y
    yy = lax.axis_index("ep")
    tt = lax.axis_index("tp")
    y_peers = [(yy + d) % n_y for d in range(1, n_y)]
    t_peers = [(tt + d) % n_tp for d in range(1, n_tp)]

    barrier = pltpu.get_barrier_semaphore()
    for device in [{"ep": p} for p in y_peers] + [{"tp": p} for p in t_peers]:
        pl.semaphore_signal(barrier, inc=1, device_id=device, device_id_type=MESH)

    ids = ids_ref[...]
    one_hot = lax.broadcasted_iota(jnp.int32, (n_exp, tok), 0) == ids
    before = lax.broadcasted_iota(jnp.int32, (tok, tok), 0) < lax.broadcasted_iota(jnp.int32, (tok, tok), 1)
    before = before.astype(F32).astype(BF16)
    preceding = jnp.dot(one_hot.astype(F32).astype(BF16), before, preferred_element_type=F32)
    slot = jnp.sum(jnp.where(one_hot, preceding, 0.0), axis=0, keepdims=True)
    kept = slot < capacity
    rank = ids // n_loc
    pad = 8
    to_rank = (lax.broadcasted_iota(jnp.int32, (pad, tok), 0) == rank) & kept
    ahead = jnp.dot(to_rank.astype(F32).astype(BF16), before, preferred_element_type=F32)
    place = jnp.sum(jnp.where(to_rank, ahead, 0.0), axis=0, keepdims=True).astype(jnp.int32)
    counts = jnp.sum(to_rank.astype(F32), axis=1, keepdims=True)
    most = jnp.max(counts, axis=0, keepdims=True).astype(jnp.int32)
    fits = kept & (place < packed)
    pos = jnp.where(fits, rank * packed + place, -1)
    pos_ref[...] = pos
    row_id = lax.broadcasted_iota(jnp.int32, (pad, tok), 0)
    parts = jnp.where(row_id == 0, (ids % n_loc).astype(F32), jnp.where(row_id == 1, slot, 1.0))
    parts = jnp.where(kept, parts, 0.0).astype(BF16)

    @pl.loop(0, n_y)
    def _(r):
        pick = (lax.broadcasted_iota(jnp.int32, (packed, tok), 0) + r * packed) == pos
        pick = pick.astype(F32).astype(BF16)
        got = lax.dot_general(parts, pick, (((1,), (1,)), ((), ())), preferred_element_type=F32)
        where = jnp.where(got[2:3] > 0.5, got[0:1] * capacity + got[1:2], -1.0)
        meta[r, :, 0:packed] = where.astype(jnp.int32)
        meta[r, :, packed:width] = jnp.broadcast_to(most, (1, width - packed))

    pl.semaphore_wait(barrier, len(y_peers) + len(t_peers))
    table_ref[pl.ds(tt * n_y + yy, 1)] = meta[pl.ds(yy, 1)]

    def col_copy(k):
        return pltpu.make_async_remote_copy(
            src_ref=meta.at[y_peers[k]], dst_ref=table_ref.at[tt * n_y + yy],
            send_sem=col_send.at[k], recv_sem=col_recv.at[k], device_id={"ep": y_peers[k]}, device_id_type=MESH,
        )

    def col_arrival(k):
        src = (yy + n_y - 1 - k) % n_y
        return pltpu.make_async_remote_copy(
            src_ref=meta.at[src], dst_ref=table_ref.at[tt * n_y + src],
            send_sem=col_send.at[k], recv_sem=col_recv.at[k], device_id={"ep": src}, device_id_type=MESH,
        )

    def row_copy(k):
        view = table_ref.at[pl.ds(tt * n_y, n_y)]
        return pltpu.make_async_remote_copy(
            src_ref=view, dst_ref=view,
            send_sem=row_send.at[k], recv_sem=row_recv.at[k], device_id={"tp": t_peers[k]}, device_id_type=MESH,
        )

    def row_arrival(k):
        src = (tt + n_tp - 1 - k) % n_tp
        view = table_ref.at[pl.ds(src * n_y, n_y)]
        return pltpu.make_async_remote_copy(
            src_ref=view, dst_ref=view,
            send_sem=row_send.at[k], recv_sem=row_recv.at[k], device_id={"tp": src}, device_id_type=MESH,
        )

    for k in range(len(y_peers)):
        col_copy(k).start()
    for k in range(len(y_peers)):
        col_arrival(k).wait_recv()
    for k in range(len(t_peers)):
        row_copy(k).start()
    for k in range(len(t_peers)):
        row_arrival(k).wait_recv()
    most_ref[...] = jnp.max(table_ref[:, :, packed:width], axis=0)
    for k in range(len(y_peers)):
        col_copy(k).wait_send()
    for k in range(len(t_peers)):
        row_copy(k).wait_send()


def route(ids_loc, n_exp, capacity, packed, n_y, n_tp):
    tok = ids_loc.shape[0]
    width = -(-(packed + 1) // 128) * 128
    dma = pltpu.SemaphoreType.DMA
    return pl.pallas_call(
        functools.partial(route_kernel, n_y, n_tp, n_exp, capacity, packed),
        out_shape=(
            jax.ShapeDtypeStruct((1, tok), jnp.int32),
            jax.ShapeDtypeStruct((n_y * n_tp, 1, width), jnp.int32),
            jax.ShapeDtypeStruct((1, width - packed), jnp.int32),
        ),
        scratch_shapes=[
            pltpu.VMEM((n_y, 1, width), jnp.int32),
            dma((n_y - 1,)), dma((n_y - 1,)), dma((n_tp - 1,)), dma((n_tp - 1,)),
        ],
        compiler_params=pltpu.CompilerParams(collective_id=1, has_side_effects=True),
        name="route",
    )(ids_loc.reshape(1, tok))


def packed_kernel(
    n_y, n_x, packed, cap, pos_ref, gate_ref, table_ref, x_ref, wg_hbm, wu_hbm, wd_hbm, out_ref,
    pack_buf, x_buf, slot_buf, pair_buf, opp_buf, nbr_buf, ret_buf, w_in, w_out, pos_col, gate_col,
    ys_send, ys_recv, a_send, a_recv, b_send, b_recv, s_send, s_recv,
    p_send, p_recv, e_send, e_recv, n_send, n_recv, f_send, f_recv, h_send, h_recv, w_sem,
):
    tok, d_model = x_ref.shape
    n_loc = slot_buf.shape[1]
    n_slots = n_loc * cap
    hidden = w_out.shape[2]
    half = packed // 2
    n_src = 2 * n_x
    n_grp = n_loc // GROUP
    n_w = n_y * n_grp
    yy = lax.axis_index("ep")
    tt = lax.axis_index("tp")
    xx, cc = tt // 2, tt % 2
    xr, xl, xo = (xx + 1) % n_x, (xx + n_x - 1) % n_x, (xx + 2) % n_x
    right, left, mate = {"tp": xr * 2 + cc}, {"tp": xl * 2 + cc}, {"tp": xx * 2 + 1 - cc}
    sides = (right, left)
    ahead, behind = (xr, xl), (xl, xr)
    mine, other = cc * n_x, (1 - cc) * n_x

    def row_of(t):
        return (yy + t + cc * (n_y - 2 * t) + n_y) % n_y

    def row_to(t):
        return (yy - t - cc * (n_y - 2 * t) + 2 * n_y) % n_y

    def remote(src, dst, send, recv, device):
        return pltpu.make_async_remote_copy(
            src_ref=src, dst_ref=dst, send_sem=send, recv_sem=recv, device_id=device, device_id_type=MESH
        )

    def part(h):
        return pl.ds(h * half, half)

    def y_copy(t):
        return remote(pack_buf.at[t], x_buf.at[t, xx], ys_send.at[t], ys_recv.at[t], {"ep": row_to(t)})

    def a_copy(t, k, h):
        view = x_buf.at[t, xx, part(h)]
        return remote(view, view, a_send.at[t, k, h], a_recv.at[t, k, h], sides[k])

    def a_arrival(t, k, h):
        view = x_buf.at[t, behind[k], part(h)]
        return remote(view, view, a_send.at[t, k, h], a_recv.at[t, k, h], sides[k])

    def b_copy(t, k):
        view = x_buf.at[t, behind[k], part(k)]
        return remote(view, view, b_send.at[t, k], b_recv.at[t, k], sides[k])

    def b_arrival(t, k):
        view = x_buf.at[t, xo, part(k)]
        return remote(view, view, b_send.at[t, k], b_recv.at[t, k], sides[k])

    def s_copy(t, b):
        view = slot_buf.at[t % 2, :, mine + b]
        return remote(view, view, s_send.at[t, b], s_recv.at[t, b], mate)

    def s_arrival(t, b):
        view = slot_buf.at[t % 2, :, other + b]
        return remote(view, view, s_send.at[t, b], s_recv.at[t, b], mate)

    def p_copy(t, i):
        at = pl.ds(i * GROUP, GROUP)
        return remote(
            slot_buf.at[t % 2, at, pl.ds(other, n_x)], pair_buf.at[t % 2, at], p_send.at[t, i], p_recv.at[t, i], mate
        )

    def e_copy(t, k):
        return remote(x_buf.at[t, xo, part(k)], opp_buf.at[k, t], e_send.at[t, k], e_recv.at[t, k], sides[k])

    def n_copy(t, k):
        h = 1 - k
        return remote(
            x_buf.at[t, ahead[k], part(h)], nbr_buf.at[k, t, part(h)], n_send.at[t, k], n_recv.at[t, k], sides[k]
        )

    def f_copy(t, k):
        return remote(
            x_buf.at[t, ahead[k], part(k)], nbr_buf.at[k, t, part(k)], f_send.at[t, k], f_recv.at[t, k], sides[k]
        )

    def h_copy(t):
        return remote(x_buf.at[t, xx], ret_buf.at[t], h_send.at[t], h_recv.at[t], {"ep": row_of(t)})

    def w_copies(w):
        s = w % W_SLOTS
        at = pl.ds((w % n_grp) * GROUP, GROUP)
        return (
            pltpu.make_async_copy(wg_hbm.at[at], w_in.at[s, :, :, pl.ds(0, hidden)], w_sem.at[s, 0]),
            pltpu.make_async_copy(wu_hbm.at[at], w_in.at[s, :, :, pl.ds(hidden, hidden)], w_sem.at[s, 1]),
            pltpu.make_async_copy(wd_hbm.at[at], w_out.at[s], w_sem.at[s, 2]),
        )

    barrier = pltpu.get_barrier_semaphore()
    for device in [right, left, mate] + [{"ep": (yy + d) % n_y} for d in range(1, n_y)]:
        pl.semaphore_signal(barrier, inc=1, device_id=device, device_id_type=MESH)

    def pack(t):
        first = row_to(t) * packed
        pick = (lax.broadcasted_iota(jnp.int32, (packed, tok), 0) + first) == pos_ref[...]
        return jnp.dot(pick.astype(F32).astype(BF16), x_ref[...], preferred_element_type=F32).astype(BF16)

    def send_own(t):
        for h in range(2):
            for k in range(2):
                a_copy(t, k, h if k == 0 else 1 - h).start()

    def pass_on(t):
        for k in range(2):
            a_arrival(t, k, k).wait_recv()
            b_copy(t, k).start()

    def source_row(t, b):
        row = table_ref[(b * 2 + cc) * n_y + row_of(t)]
        return row[:, :packed]

    def spread(t, blocks):
        @pl.loop(0, len(blocks))
        def _(j):
            b = blocks[0]
            for n, blk in enumerate(blocks[1:]):
                b = jnp.where(j == n + 1, blk, b)
            to = source_row(t, b)
            pick = (lax.broadcasted_iota(jnp.int32, (n_slots, packed), 0) == to).astype(F32).astype(BF16)
            slots = jnp.dot(pick, x_buf[t, b], preferred_element_type=F32).astype(BF16)
            slot_buf[t % 2, :, mine + b] = slots.reshape(n_loc, cap, d_model)
            s_copy(t, b).start()

    def share(t):
        for k in range(2):
            a_arrival(t, k, 1 - k).wait_recv()
        spread(t, (xl, xr))

    def multiply(t, lo, hi):
        @pl.loop(lo, hi)
        def _(i):
            w = t * n_grp + i
            s = w % W_SLOTS
            for c in w_copies(w):
                c.wait()
            both = []
            for el in range(GROUP):
                tile = slot_buf[t % 2, i * GROUP + el].reshape(n_src * cap, d_model)
                both.append(jnp.dot(tile, w_in[s, el], preferred_element_type=F32))
            for el in range(GROUP):
                act = (jax.nn.silu(both[el][:, :hidden]) * both[el][:, hidden:]).astype(BF16)
                out = jnp.dot(act, w_out[s, el], preferred_element_type=F32)
                slot_buf[t % 2, i * GROUP + el] = out.astype(BF16).reshape(n_src, cap, d_model)
            p_copy(t, i).start()

            @pl.when(w + W_SLOTS < n_w)
            def _():
                for c in w_copies(w + W_SLOTS):
                    c.start()

    def gather_back(t, blocks):
        @pl.loop(0, len(blocks))
        def _(j):
            b = blocks[0]
            for n, blk in enumerate(blocks[1:]):
                b = jnp.where(j == n + 1, blk, b)
            to = source_row(t, b).astype(F32)
            col = jnp.transpose(jnp.broadcast_to(to, (128, packed)))
            lane = lax.broadcasted_iota(jnp.int32, (packed, 128), 1).astype(F32)
            pick = jnp.concatenate(
                [(col == lane + float(128 * m)).astype(F32).astype(BF16) for m in range(n_slots // 128)], axis=1
            )
            total = slot_buf[t % 2, :, mine + b].astype(F32) + pair_buf[t % 2, :, b].astype(F32)
            slots = total.astype(BF16).reshape(n_slots, d_model)
            x_buf[t, b] = jnp.dot(pick, slots, preferred_element_type=F32).astype(BF16)

    def first_sums(t):
        @pl.loop(0, n_grp)
        def _(i):
            p_copy(t, i).wait_recv()

        gather_back(t, (xo,))
        for k in range(2):
            e_copy(t, k).start()
        gather_back(t, (xr, xl))
        for k in range(2):
            n_copy(t, k).start()

    def last_sums(t):
        for k in range(2):
            e_copy(t, k).wait_recv()
            at = (t, ahead[k], slice(k * half, (k + 1) * half))
            x_buf[at] = (x_buf[at].astype(F32) + opp_buf[k, t].astype(F32)).astype(BF16)
            f_copy(t, k).start()

    def give_back(t, local):
        for k in range(2):
            n_copy(t, k).wait_recv()
            f_copy(t, k).wait_recv()
        total = x_buf[t, xx].astype(F32) + (nbr_buf[0, t].astype(F32) + nbr_buf[1, t].astype(F32))
        if local:
            ret_buf[t] = total.astype(BF16)
        else:
            x_buf[t, xx] = total.astype(BF16)
            h_copy(t).start()

    def combine_into(t, first, last):
        if not isinstance(t, int) or t > 0:
            h_copy(t).wait_recv()
        tile = 256

        @pl.loop(0, tok // tile)
        def _(i):
            rows = pl.ds(pl.multiple_of(i * tile, tile), tile)
            want = pos_col[rows, :] - (row_to(t) * packed).astype(F32)
            lane = lax.broadcasted_iota(jnp.int32, (tile, 128), 1).astype(F32)
            pick = jnp.concatenate(
                [(want == lane + float(128 * m)).astype(F32) for m in range(-(-packed // 128))], axis=1
            )
            y = jnp.dot(pick[:, :packed].astype(BF16), ret_buf[t], preferred_element_type=F32)
            if not first:
                y = y + out_ref[rows, :].astype(F32)
            if last:
                weight = jnp.where(pos_col[rows, 0:1] >= 0, gate_col[rows, 0:1], 0.0)
                y = y * weight
            out_ref[rows, :] = y.astype(BF16)

    x_buf[0, xx] = pack(0)
    pl.semaphore_wait(barrier, 2 + n_y)
    send_own(0)

    @pl.loop(1, n_y)
    def _(t):
        pack_buf[t] = pack(t)
        y_copy(t).start()

    for w in range(W_SLOTS):
        for c in w_copies(w):
            c.start()
    spread(0, (xx,))
    pass_on(0)
    y_copy(1).wait_recv()
    send_own(1)
    tile = 256

    @pl.loop(0, tok // tile)
    def _(i):
        rows = pl.ds(pl.multiple_of(i * tile, tile), tile)
        pos_col[rows, :] = jnp.transpose(jnp.broadcast_to(pos_ref[:, rows].astype(F32), (128, tile)))
        gate_col[rows, :] = jnp.transpose(jnp.broadcast_to(gate_ref[:, rows], (128, tile)))

    share(0)

    @pl.loop(0, n_y)
    def _(t):
        for k in range(2):
            b_arrival(t, k).wait_recv()
        spread(t, (xo,))

        @pl.when(t + 1 < n_y)
        def _():
            pass_on(t + 1)

        @pl.when(t + 2 < n_y)
        def _():
            y_copy(t + 2).wait_recv()
            send_own(t + 2)

        for b in range(n_x):
            s_arrival(t, b).wait_recv()
            s_copy(t, b).wait_send()
        multiply(t, 0, n_grp // 2)

        @pl.when(t + 1 < n_y)
        def _():
            spread(t + 1, (xx,))

        multiply(t, n_grp // 2, n_grp)

        @pl.when(t > 0)
        def _():
            last_sums(t - 1)

        @pl.when(t + 1 < n_y)
        def _():
            share(t + 1)

        for k in range(2):
            for h in range(2):
                a_copy(t, k, h).wait_send()
            b_copy(t, k).wait_send()
        first_sums(t)
        gather_back(t, (xx,))

        @pl.loop(0, n_grp)
        def _(i):
            p_copy(t, i).wait_send()

        @pl.when(t == 2)
        def _():
            give_back(0, True)

        @pl.when(t > 2)
        def _():
            give_back(t - 2, False)

    last_sums(n_y - 1)
    for t in range(max(n_y - 2, 0), n_y):
        if t == n_y - 1:
            combine_into(0, True, False)
        give_back(t, t == 0)
    for t in range(1, n_y):
        combine_into(t, False, t == n_y - 1)
    for t in range(1, n_y):
        y_copy(t).wait_send()
        h_copy(t).wait_send()

    @pl.loop(0, n_y)
    def _(t):
        for k in range(2):
            e_copy(t, k).wait_send()
            n_copy(t, k).wait_send()
            f_copy(t, k).wait_send()


def packed_layer(pos, gate, table, x_loc, wg, wu, wd, n_y, n_tp, packed, cap):
    tok, d_model = x_loc.shape
    n_loc, _, hidden = wg.shape
    n_x = n_tp // 2
    n_grp = n_loc // GROUP
    half = packed // 2
    dma = pltpu.SemaphoreType.DMA
    hbm = pl.BlockSpec(memory_space=pltpu.HBM)
    vmem = pl.BlockSpec(memory_space=pltpu.VMEM)
    return pl.pallas_call(
        functools.partial(packed_kernel, n_y, n_x, packed, cap),
        out_shape=jax.ShapeDtypeStruct((tok, d_model), BF16),
        in_specs=[vmem] * 4 + [hbm] * 3,
        out_specs=vmem,
        scratch_shapes=[
            pltpu.VMEM((n_y, packed, d_model), BF16),
            pltpu.VMEM((n_y, n_x, packed, d_model), BF16),
            pltpu.VMEM((2, n_loc, 2 * n_x, cap, d_model), BF16),
            pltpu.VMEM((2, n_loc, n_x, cap, d_model), BF16),
            pltpu.VMEM((2, n_y, half, d_model), BF16),
            pltpu.VMEM((2, n_y, packed, d_model), BF16),
            pltpu.VMEM((n_y, packed, d_model), BF16),
            pltpu.VMEM((W_SLOTS, GROUP, d_model, 2 * hidden), BF16),
            pltpu.VMEM((W_SLOTS, GROUP, hidden, d_model), BF16),
            pltpu.VMEM((tok, 128), F32),
            pltpu.VMEM((tok, 128), F32),
            dma((n_y,)), dma((n_y,)),
            dma((n_y, 2, 2)), dma((n_y, 2, 2)),
            dma((n_y, 2)), dma((n_y, 2)),
            dma((n_y, n_x)), dma((n_y, n_x)),
            dma((n_y, n_grp)), dma((n_y, n_grp)),
            dma((n_y, 2)), dma((n_y, 2)),
            dma((n_y, 2)), dma((n_y, 2)),
            dma((n_y, 2)), dma((n_y, 2)),
            dma((n_y,)), dma((n_y,)),
            dma((W_SLOTS, 3)),
        ],
        compiler_params=pltpu.CompilerParams(
            collective_id=2, has_side_effects=True, vmem_limit_bytes=67043328
        ),
        name="packed_layer",
    )(pos, gate, table, x_loc, wg, wu, wd)


def solution(mesh):
    n_y, n_tp = mesh.shape["ep"], mesh.shape["tp"]
    row_spec = P(("dp", "ep", "tp"), None)

    def local_layer(x_loc, ids_loc, gate_loc, wg_loc, wu_loc, wd_loc):
        tok, d_model = x_loc.shape
        n_loc = wg_loc.shape[0]
        n_exp = n_loc * n_y
        capacity = CAP_FACTOR * tok // n_exp
        packed = n_loc * capacity * 5 // 8
        pos, table, most = route(ids_loc, n_exp, capacity, packed, n_y, n_tp)

        def by_rows():
            gate = gate_loc.reshape(1, tok)
            return packed_layer(pos, gate, table, x_loc, wg_loc, wu_loc, wd_loc, n_y, n_tp, packed, capacity)

        def by_slots():
            rows, pos = dispatch(x_loc, ids_loc, n_exp, capacity)
            y = experts(rows.reshape(n_exp, capacity, d_model), wg_loc, wu_loc, wd_loc, n_y, n_tp)
            return combine(pos, gate_loc, y.reshape(n_exp * capacity, d_model))

        return lax.cond(most[0, 0] <= packed, by_rows, by_slots)

    return jax.shard_map(local_layer, mesh=mesh, in_specs=(row_spec, row_spec, row_spec, P("ep", None, "tp"), P("ep", None, "tp"), P("ep", "tp", None)), out_specs=row_spec, check_vma=False)
```

```python
import functools

import jax
import jax.numpy as jnp
from jax import lax
from jax.experimental import pallas as pl
from jax.experimental.pallas import tpu as pltpu
from jax.sharding import PartitionSpec as P

CAP_FACTOR = 2
GROUP = 2
W_SLOTS = 4
MESH = pl.DeviceIdType.MESH
BF16 = jnp.bfloat16
F32 = jnp.float32


def dispatch_kernel(capacity, n_exp, ids_ref, x_ref, rows_ref, pos_ref):
    tok = ids_ref.shape[1]
    n_slots = rows_ref.shape[0]
    ids = ids_ref[...]
    one_hot = lax.broadcasted_iota(jnp.int32, (n_exp, tok), 0) == ids
    before = lax.broadcasted_iota(jnp.int32, (tok, tok), 0) < lax.broadcasted_iota(jnp.int32, (tok, tok), 1)
    preceding = jnp.dot(one_hot.astype(F32).astype(BF16), before.astype(F32).astype(BF16), preferred_element_type=F32)
    slot = jnp.sum(jnp.where(one_hot, preceding, 0.0), axis=0, keepdims=True).astype(jnp.int32)
    pos = jnp.where(slot < capacity, ids * capacity + slot, -1)
    pos_ref[...] = pos
    tile = 256

    @pl.loop(0, n_slots // tile)
    def _(i):
        want = lax.broadcasted_iota(jnp.int32, (tile, tok), 0) + i * tile
        pick = (want == pos).astype(F32).astype(BF16)
        start = pl.multiple_of(i * tile, tile)
        rows_ref[pl.ds(start, tile), :] = jnp.dot(pick, x_ref[...], preferred_element_type=F32).astype(BF16)


def dispatch(x_loc, ids_loc, n_exp, capacity):
    tok, d_model = x_loc.shape
    return pl.pallas_call(
        functools.partial(dispatch_kernel, capacity, n_exp),
        out_shape=(
            jax.ShapeDtypeStruct((n_exp * capacity, d_model), BF16),
            jax.ShapeDtypeStruct((1, tok), jnp.int32),
        ),
        name="dispatch",
    )(ids_loc.reshape(1, tok), x_loc)


def combine_kernel(pos_ref, y_ref, out_ref):
    n_slots = y_ref.shape[0]
    tok = out_ref.shape[0]
    tile = 256

    @pl.loop(0, tok // tile)
    def _(i):
        rows = pl.ds(pl.multiple_of(i * tile, tile), tile)
        pos = pos_ref[rows, :]
        pick = (lax.broadcasted_iota(jnp.int32, (tile, n_slots), 1) == pos).astype(F32).astype(BF16)
        out_ref[rows, :] = jnp.dot(pick, y_ref[...], preferred_element_type=F32).astype(BF16)


def combine(pos, y_slots):
    tok = pos.shape[1]
    return pl.pallas_call(
        combine_kernel,
        out_shape=jax.ShapeDtypeStruct((tok, y_slots.shape[1]), BF16),
        name="combine",
    )(pos.reshape(tok, 1), y_slots)


def expert_kernel(
    n_y, n_x, rows_hbm, wg_hbm, wu_hbm, wd_hbm, out_hbm,
    x_buf, pair_buf, opp_buf, nbr_buf, w_in, w_out,
    ys_send, ys_recv, ys_loc, a_send, a_recv, b_send, b_recv, d_send, d_recv,
    p_send, p_recv, e_send, e_recv, f_send, f_recv, h_send, h_recv, h_loc, w_sem,
):
    n_loc, _, _, cap, d_model = x_buf.shape
    hidden = w_out.shape[2]
    n_grp = n_loc // GROUP
    half = n_y // 2
    yy = lax.axis_index("ep")
    tt = lax.axis_index("tp")
    xx, cc = tt // 2, tt % 2
    xr, xl, xo = (xx + 1) % n_x, (xx + n_x - 1) % n_x, (xx + 2) % n_x
    right, left, mate = {"tp": xr * 2 + cc}, {"tp": xl * 2 + cc}, {"tp": xx * 2 + 1 - cc}
    peers = [(yy + d) % n_y for d in range(1, n_y)]
    mine = cc * n_x

    def remote(src, dst, send, recv, device):
        return pltpu.make_async_remote_copy(
            src_ref=src, dst_ref=dst, send_sem=send, recv_sem=recv, device_id=device, device_id_type=MESH
        )

    def grp(g):
        return pl.ds(g * GROUP, GROUP)

    def y_copy(g, k, peer):
        return remote(
            rows_hbm.at[pl.ds(peer * n_loc + g * GROUP, GROUP)], x_buf.at[grp(g), mine + xx, yy],
            ys_send.at[g, k], ys_recv.at[g, k], {"ep": peer},
        )

    def y_local(g):
        return pltpu.make_async_copy(
            rows_hbm.at[pl.ds(yy * n_loc + g * GROUP, GROUP)], x_buf.at[grp(g), mine + xx, yy], ys_loc.at[g]
        )

    def block_copy(g, blk, send, recv, device):
        view = x_buf.at[grp(g), mine + blk]
        return remote(view, view, send, recv, device)

    def a_copy(g, k):
        return block_copy(g, xx, a_send.at[g, k], a_recv.at[g, k], (right, left)[k])

    def b_copy(g, k):
        view = x_buf.at[grp(g), mine + (xl, xr)[k], pl.ds(k * half, half)]
        return remote(view, view, b_send.at[g, k], b_recv.at[g, k], (right, left)[k])

    def d_copy(g, k):
        return block_copy(g, (xx, xl, xr, xo)[k], d_send.at[g, k], d_recv.at[g, k], mate)

    def p_copy(g):
        other = (1 - cc) * n_x
        return remote(x_buf.at[grp(g), pl.ds(other, n_x)], pair_buf.at[grp(g)], p_send.at[g], p_recv.at[g], mate)

    def e_copy(g, k):
        view = x_buf.at[grp(g), mine + xo, pl.ds(k * half, half)]
        return remote(view, opp_buf.at[k, grp(g)], e_send.at[g, k], e_recv.at[g, k], (right, left)[k])

    def f_copy(g, k):
        view = x_buf.at[grp(g), mine + (xr, xl)[k]]
        return remote(view, nbr_buf.at[k, grp(g)], f_send.at[g, k], f_recv.at[g, k], (right, left)[k])

    def h_copy(g, k, peer):
        return remote(
            x_buf.at[grp(g), mine + xx, peer], out_hbm.at[pl.ds(yy * n_loc + g * GROUP, GROUP)],
            h_send.at[g, k], h_recv.at[g, k], {"ep": peer},
        )

    def h_local(g):
        return pltpu.make_async_copy(
            x_buf.at[grp(g), mine + xx, yy], out_hbm.at[pl.ds(yy * n_loc + g * GROUP, GROUP)], h_loc.at[g]
        )

    def w_copies(g):
        s = g % 2
        return (
            pltpu.make_async_copy(wg_hbm.at[grp(g)], w_in.at[s, :, :, pl.ds(0, hidden)], w_sem.at[s, 0]),
            pltpu.make_async_copy(wu_hbm.at[grp(g)], w_in.at[s, :, :, pl.ds(hidden, hidden)], w_sem.at[s, 1]),
            pltpu.make_async_copy(wd_hbm.at[grp(g)], w_out.at[s], w_sem.at[s, 2]),
        )

    for g in range(2):
        for c in w_copies(g):
            c.start()

    barrier = pltpu.get_barrier_semaphore()
    for device in [right, left, mate] + [{"ep": p} for p in peers]:
        pl.semaphore_signal(barrier, inc=1, device_id=device, device_id_type=MESH)
    pl.semaphore_wait(barrier, 3 + len(peers))

    @pl.loop(0, n_grp)
    def _(g):
        for k, peer in enumerate(peers):
            y_copy(g, k, peer).start()
        y_local(g).start()

    def stage_a(g):
        for k, peer in enumerate(peers):
            y_copy(g, k, peer).wait_recv()
        y_local(g).wait()
        for k in range(2):
            a_copy(g, k).start()
        d_copy(g, 0).start()

    def stage_b(g):
        for k in range(2):
            a_copy(g, k).wait_recv()
            b_copy(g, k).start()
        for k in range(2):
            d_copy(g, 1 + k).start()

    def stage_c(g):
        for k in range(2):
            b_copy(g, k).wait_recv()
        d_copy(g, 3).start()

    def stage_d(g):
        for k in range(4):
            d_copy(g, k).wait()
        for k in range(2):
            a_copy(g, k).wait_send()
            b_copy(g, k).wait_send()
        for c in w_copies(g):
            c.wait()
        s = g % 2
        blocks = 2
        per = 2 * n_x // blocks

        @pl.loop(0, GROUP * per)
        def _(j):
            el = j // per
            at = (g * GROUP + el, pl.ds((j % per) * blocks, blocks))
            tile = x_buf[at].reshape(blocks * n_y * cap, d_model)
            both = jnp.dot(tile, w_in[s, el], preferred_element_type=F32)
            pre = both[:, :hidden]
            act = (jax.nn.silu(pre) * both[:, hidden:]).astype(BF16)
            part = jnp.dot(act, w_out[s, el], preferred_element_type=F32)
            x_buf[at] = part.astype(BF16).reshape(blocks, n_y, cap, d_model)

        p_copy(g).start()

        @pl.when(g + 2 < n_grp)
        def _():
            for c in w_copies(g + 2):
                c.start()

    def stage_e(g):
        p_copy(g).wait_recv()

        @pl.loop(0, GROUP * n_y)
        def _(j):
            e, q = g * GROUP + j // n_y, j % n_y
            total = x_buf[e, mine + xo, q].astype(F32) + pair_buf[e, xo, q].astype(F32)
            x_buf[e, mine + xo, q] = total.astype(BF16)

        for k in range(2):
            e_copy(g, k).start()

    def stage_f(g):
        for k in range(2):
            e_copy(g, k).wait_recv()
            blk = (xr, xl)[k]

            @pl.loop(0, GROUP * half)
            def _(j):
                e, q = g * GROUP + j // half, j % half
                a = q + k * half
                total = x_buf[e, mine + blk, a].astype(F32) + pair_buf[e, blk, a].astype(F32)
                total = total + opp_buf[k, e, q].astype(F32)
                x_buf[e, mine + blk, a] = total.astype(BF16)
                b = q + (1 - k) * half
                rest = x_buf[e, mine + blk, b].astype(F32) + pair_buf[e, blk, b].astype(F32)
                x_buf[e, mine + blk, b] = rest.astype(BF16)

            f_copy(g, k).start()

    def stage_h(g):
        for k in range(2):
            f_copy(g, k).wait_recv()

        @pl.loop(0, GROUP * n_y)
        def _(j):
            e, q = g * GROUP + j // n_y, j % n_y
            total = x_buf[e, mine + xx, q].astype(F32) + pair_buf[e, xx, q].astype(F32)
            total = total + (nbr_buf[0, e, q].astype(F32) + nbr_buf[1, e, q].astype(F32))
            x_buf[e, mine + xx, q] = total.astype(BF16)

        for k, peer in enumerate(peers):
            h_copy(g, k, peer).start()
        h_local(g).start()

    stages = (stage_a, stage_b, stage_c, stage_d, stage_e, stage_f, stage_h)

    @pl.loop(0, n_grp + len(stages) - 1)
    def _(t):
        for lag, stage in enumerate(stages):
            g = t - lag

            @pl.when((g >= 0) & (g < n_grp))
            def _():
                stage(g)

    @pl.loop(0, n_grp)
    def _(g):
        p_copy(g).wait_send()
        for k in range(2):
            e_copy(g, k).wait_send()
            f_copy(g, k).wait_send()
        for k, peer in enumerate(peers):
            y_copy(g, k, peer).wait_send()
            h_copy(g, k, peer).wait()
        h_local(g).wait()


def experts(rows, wg, wu, wd, n_y, n_tp):
    n_exp, cap, d_model = rows.shape
    n_loc, _, hidden = wg.shape
    n_x = n_tp // 2
    half = n_y // 2
    n_grp = n_loc // GROUP
    dma = pltpu.SemaphoreType.DMA
    hbm = pl.BlockSpec(memory_space=pltpu.HBM)
    return pl.pallas_call(
        functools.partial(expert_kernel, n_y, n_x),
        out_shape=jax.ShapeDtypeStruct(rows.shape, BF16),
        in_specs=[hbm] * 4,
        out_specs=hbm,
        scratch_shapes=[
            pltpu.VMEM((n_loc, 2 * n_x, n_y, cap, d_model), BF16),
            pltpu.VMEM((n_loc, n_x, n_y, cap, d_model), BF16),
            pltpu.VMEM((2, n_loc, half, cap, d_model), BF16),
            pltpu.VMEM((2, n_loc, n_y, cap, d_model), BF16),
            pltpu.VMEM((2, GROUP, d_model, 2 * hidden), BF16),
            pltpu.VMEM((2, GROUP, hidden, d_model), BF16),
            dma((n_grp, n_y - 1)), dma((n_grp, n_y - 1)), dma((n_grp,)),
            dma((n_grp, 2)), dma((n_grp, 2)),
            dma((n_grp, 2)), dma((n_grp, 2)),
            dma((n_grp, 4)), dma((n_grp, 4)),
            dma((n_grp,)), dma((n_grp,)),
            dma((n_grp, 2)), dma((n_grp, 2)),
            dma((n_grp, 2)), dma((n_grp, 2)),
            dma((n_grp, n_y - 1)), dma((n_grp, n_y - 1)), dma((n_grp,)),
            dma((2, 3)),
        ],
        compiler_params=pltpu.CompilerParams(
            collective_id=0, has_side_effects=True, vmem_limit_bytes=67043328
        ),
        name="experts",
    )(rows, wg, wu, wd)


def packed_kernel(
    n_y, n_x, packed, cap, ids_ref, x_ref, wg_hbm, wu_hbm, wd_hbm, out_ref, most_ref,
    pack_buf, x_buf, slot_buf, pair_buf, opp_buf, nbr_buf, ret_buf, w_in, w_out, pos_col,
    lists, table, flags, l_send, l_recv, t_send, t_recv, m_send, m_recv, ys_send, ys_recv, a_send, a_recv, b_send, b_recv, s_send, s_recv,
    p_send, p_recv, e_send, e_recv, n_send, n_recv, f_send, f_recv, h_send, h_recv, w_sem,
):
    tok, d_model = x_ref.shape
    n_loc = slot_buf.shape[1]
    n_slots = n_loc * cap
    hidden = w_out.shape[2]
    half = packed // 2
    n_src = 2 * n_x
    n_grp = n_loc // GROUP
    n_w = n_y * n_grp
    yy = lax.axis_index("ep")
    tt = lax.axis_index("tp")
    xx, cc = tt // 2, tt % 2
    xr, xl, xo = (xx + 1) % n_x, (xx + n_x - 1) % n_x, (xx + 2) % n_x
    right, left, mate = {"tp": xr * 2 + cc}, {"tp": xl * 2 + cc}, {"tp": xx * 2 + 1 - cc}
    across = {"tp": xo * 2 + cc}
    sides = (right, left)
    ahead, behind = (xr, xl), (xl, xr)
    mine, other = cc * n_x, (1 - cc) * n_x
    width = table.shape[3]
    n_exp = n_loc * n_y

    def row_of(t):
        return (yy + t + cc * (n_y - 2 * t) + n_y) % n_y

    def row_to(t):
        return (yy - t - cc * (n_y - 2 * t) + 2 * n_y) % n_y

    def remote(src, dst, send, recv, device):
        return pltpu.make_async_remote_copy(
            src_ref=src, dst_ref=dst, send_sem=send, recv_sem=recv, device_id=device, device_id_type=MESH
        )

    def part(h):
        return pl.ds(h * half, half)

    def y_copy(t):
        return remote(pack_buf.at[t], x_buf.at[t, xx], ys_send.at[t], ys_recv.at[t], {"ep": row_to(t)})

    def list_copy(t):
        return remote(lists.at[t], table.at[t, xx], l_send.at[t], l_recv.at[t], {"ep": row_to(t)})

    def table_copy(t, k):
        view = table.at[t, xx]
        return remote(view, view, t_send.at[t, k], t_recv.at[t, k], (right, left, across)[k])

    def table_arrival(t, k):
        view = table.at[t, (xl, xr, xo)[k]]
        return remote(view, view, t_send.at[t, k], t_recv.at[t, k], (right, left, across)[k])

    def flag_copy():
        return remote(flags.at[0], flags.at[1], m_send, m_recv, mate)

    def a_copy(t, k, h):
        view = x_buf.at[t, xx, part(h)]
        return remote(view, view, a_send.at[t, k, h], a_recv.at[t, k, h], sides[k])

    def a_arrival(t, k, h):
        view = x_buf.at[t, behind[k], part(h)]
        return remote(view, view, a_send.at[t, k, h], a_recv.at[t, k, h], sides[k])

    def b_copy(t, k):
        view = x_buf.at[t, behind[k], part(k)]
        return remote(view, view, b_send.at[t, k], b_recv.at[t, k], sides[k])

    def b_arrival(t, k):
        view = x_buf.at[t, xo, part(k)]
        return remote(view, view, b_send.at[t, k], b_recv.at[t, k], sides[k])

    def s_copy(t, b):
        view = slot_buf.at[t % 2, :, mine + b]
        return remote(view, view, s_send.at[t, b], s_recv.at[t, b], mate)

    def s_arrival(t, b):
        view = slot_buf.at[t % 2, :, other + b]
        return remote(view, view, s_send.at[t, b], s_recv.at[t, b], mate)

    def p_copy(t, i):
        at = pl.ds(i * GROUP, GROUP)
        return remote(
            slot_buf.at[t % 2, at, pl.ds(other, n_x)], pair_buf.at[t % 2, at], p_send.at[t, i], p_recv.at[t, i], mate
        )

    def e_copy(t, k):
        return remote(x_buf.at[t, xo, part(k)], opp_buf.at[k, t], e_send.at[t, k], e_recv.at[t, k], sides[k])

    def n_copy(t, k):
        h = 1 - k
        return remote(
            x_buf.at[t, ahead[k], part(h)], nbr_buf.at[k, t, part(h)], n_send.at[t, k], n_recv.at[t, k], sides[k]
        )

    def f_copy(t, k):
        return remote(
            x_buf.at[t, ahead[k], part(k)], nbr_buf.at[k, t, part(k)], f_send.at[t, k], f_recv.at[t, k], sides[k]
        )

    def h_copy(t):
        return remote(x_buf.at[t, xx], ret_buf.at[t], h_send.at[t], h_recv.at[t], {"ep": row_of(t)})

    def w_copies(w):
        s = w % W_SLOTS
        at = pl.ds((w % n_grp) * GROUP, GROUP)
        return (
            pltpu.make_async_copy(wg_hbm.at[at], w_in.at[s, :, :, pl.ds(0, hidden)], w_sem.at[s, 0]),
            pltpu.make_async_copy(wu_hbm.at[at], w_in.at[s, :, :, pl.ds(hidden, hidden)], w_sem.at[s, 1]),
            pltpu.make_async_copy(wd_hbm.at[at], w_out.at[s], w_sem.at[s, 2]),
        )

    barrier = pltpu.get_barrier_semaphore()
    for device in [right, left, across, mate] + [{"ep": (yy + d) % n_y} for d in range(1, n_y)]:
        pl.semaphore_signal(barrier, inc=1, device_id=device, device_id_type=MESH)
    for w in range(W_SLOTS):
        for c in w_copies(w):
            c.start()

    ids = ids_ref[...]
    one_hot = lax.broadcasted_iota(jnp.int32, (n_exp, tok), 0) == ids
    earlier = lax.broadcasted_iota(jnp.int32, (tok, tok), 0) < lax.broadcasted_iota(jnp.int32, (tok, tok), 1)
    earlier = earlier.astype(F32).astype(BF16)
    preceding = jnp.dot(one_hot.astype(F32).astype(BF16), earlier, preferred_element_type=F32)
    slot = jnp.sum(jnp.where(one_hot, preceding, 0.0), axis=0, keepdims=True)
    kept = slot < cap
    rank = ids // n_loc
    pad = 8
    to_rank = (lax.broadcasted_iota(jnp.int32, (pad, tok), 0) == rank) & kept
    before = jnp.dot(to_rank.astype(F32).astype(BF16), earlier, preferred_element_type=F32)
    place = jnp.sum(jnp.where(to_rank, before, 0.0), axis=0, keepdims=True).astype(jnp.int32)
    counts = jnp.sum(to_rank.astype(F32), axis=1, keepdims=True)
    most = jnp.max(counts, axis=0, keepdims=True).astype(jnp.int32)
    pos = jnp.where(kept & (place < packed), rank * packed + place, -1)
    row_id = lax.broadcasted_iota(jnp.int32, (pad, tok), 0)
    parts = jnp.where(row_id == 0, (ids % n_loc).astype(F32), jnp.where(row_id == 1, slot, 1.0))
    parts = jnp.where(kept, parts, 0.0).astype(BF16)

    def wanted(t):
        pick = (lax.broadcasted_iota(jnp.int32, (packed, tok), 0) + row_to(t) * packed) == pos
        return pick.astype(F32).astype(BF16)

    def pack(t):
        return jnp.dot(wanted(t), x_ref[...], preferred_element_type=F32).astype(BF16)

    def list_of(t):
        got = lax.dot_general(parts, wanted(t), (((1,), (1,)), ((), ())), preferred_element_type=F32)
        return jnp.where(got[2:3] > 0.5, got[0:1] * cap + got[1:2], -1.0).astype(jnp.int32)

    def send_half(t, h):
        for k in range(2):
            a_copy(t, k, h if k == 0 else 1 - h).start()

    def send_table(t):
        for k in (2, 0, 1):
            table_copy(t, k).start()

    def send_own(t):
        list_copy(t).wait_recv()
        send_table(t)
        y_copy(t).wait_recv()
        send_half(t, 0)
        send_half(t, 1)

    def pass_on(t):
        for k in range(2):
            a_arrival(t, k, k).wait_recv()
            b_copy(t, k).start()

    def source_row(t, b):
        return table[t, b][:, :packed]

    def spread(t, blocks):
        @pl.loop(0, len(blocks))
        def _(j):
            b = blocks[0]
            for n, blk in enumerate(blocks[1:]):
                b = jnp.where(j == n + 1, blk, b)
            to = source_row(t, b)
            pick = (lax.broadcasted_iota(jnp.int32, (n_slots, packed), 0) == to).astype(F32).astype(BF16)
            slots = jnp.dot(pick, x_buf[t, b], preferred_element_type=F32).astype(BF16)
            slot_buf[t % 2, :, mine + b] = slots.reshape(n_loc, cap, d_model)
            s_copy(t, b).start()

    def share(t):
        for k in range(2):
            table_arrival(t, k).wait_recv()
            a_arrival(t, k, 1 - k).wait_recv()
        spread(t, (xl, xr))

    def multiply(t, lo, hi):
        @pl.loop(lo, hi)
        def _(i):
            w = t * n_grp + i
            s = w % W_SLOTS
            for c in w_copies(w):
                c.wait()
            both = []
            for el in range(GROUP):
                tile = slot_buf[t % 2, i * GROUP + el].reshape(n_src * cap, d_model)
                both.append(jnp.dot(tile, w_in[s, el], preferred_element_type=F32))
            for el in range(GROUP):
                act = (jax.nn.silu(both[el][:, :hidden]) * both[el][:, hidden:]).astype(BF16)
                out = jnp.dot(act, w_out[s, el], preferred_element_type=F32)
                slot_buf[t % 2, i * GROUP + el] = out.astype(BF16).reshape(n_src, cap, d_model)
            p_copy(t, i).start()

            @pl.when(w + W_SLOTS < n_w)
            def _():
                for c in w_copies(w + W_SLOTS):
                    c.start()

    def gather_back(t, blocks):
        @pl.loop(0, len(blocks))
        def _(j):
            b = blocks[0]
            for n, blk in enumerate(blocks[1:]):
                b = jnp.where(j == n + 1, blk, b)
            to = source_row(t, b).astype(F32)
            col = jnp.transpose(jnp.broadcast_to(to, (128, packed)))
            lane = lax.broadcasted_iota(jnp.int32, (packed, 128), 1).astype(F32)
            pick = jnp.concatenate(
                [(col == lane + float(128 * m)).astype(F32).astype(BF16) for m in range(n_slots // 128)], axis=1
            )
            total = slot_buf[t % 2, :, mine + b].astype(F32) + pair_buf[t % 2, :, b].astype(F32)
            slots = total.astype(BF16).reshape(n_slots, d_model)
            x_buf[t, b] = jnp.dot(pick, slots, preferred_element_type=F32).astype(BF16)

    def first_sums(t):
        @pl.loop(0, n_grp)
        def _(i):
            p_copy(t, i).wait_recv()

        gather_back(t, (xo,))
        for k in range(2):
            e_copy(t, k).start()
        gather_back(t, (xr, xl))

    def early_sums(t):
        for k in range(2):
            n_copy(t, k).start()

    def last_sums(t):
        for k in range(2):
            e_copy(t, k).wait_recv()
            at = (t, ahead[k], slice(k * half, (k + 1) * half))
            x_buf[at] = (x_buf[at].astype(F32) + opp_buf[k, t].astype(F32)).astype(BF16)
            f_copy(t, k).start()

    def give_back(t, local):
        for k in range(2):
            n_copy(t, k).wait_recv()
            f_copy(t, k).wait_recv()
        total = x_buf[t, xx].astype(F32) + (nbr_buf[0, t].astype(F32) + nbr_buf[1, t].astype(F32))
        if local:
            ret_buf[t] = total.astype(BF16)
        else:
            x_buf[t, xx] = total.astype(BF16)
            h_copy(t).start()

    def combine_into(t, first):
        tile = 256

        @pl.loop(0, tok // tile)
        def _(i):
            rows = pl.ds(pl.multiple_of(i * tile, tile), tile)
            want = pos_col[rows, :] - (row_to(t) * packed).astype(F32)
            lane = lax.broadcasted_iota(jnp.int32, (tile, 128), 1).astype(F32)
            pick = jnp.concatenate(
                [(want == lane + float(128 * m)).astype(F32) for m in range(-(-packed // 128))], axis=1
            )
            y = jnp.dot(pick[:, :packed].astype(BF16), ret_buf[t], preferred_element_type=F32)
            if not first:
                y = y + out_ref[rows, :].astype(F32)
            out_ref[rows, :] = y.astype(BF16)

    x_buf[0, xx] = pack(0)
    pl.semaphore_wait(barrier, 3 + n_y)
    send_half(0, 0)
    table[0, xx, :, 0:packed] = list_of(0)
    table[0, xx, :, packed:width] = jnp.broadcast_to(most, (1, width - packed))
    send_table(0)
    send_half(0, 1)

    @pl.loop(1, n_y)
    def _(t):
        lists[t, :, 0:packed] = list_of(t)
        lists[t, :, packed:width] = jnp.broadcast_to(most, (1, width - packed))
        list_copy(t).start()
        pack_buf[t] = pack(t)
        y_copy(t).start()

    spread(0, (xx,))
    pass_on(0)
    send_own(1)
    tile = 256
    for i in range(tok // tile):
        spot = pos[:, i * tile:(i + 1) * tile].astype(F32)
        pos_col[i * tile:(i + 1) * tile, :] = jnp.transpose(jnp.broadcast_to(spot, (128, tile)))
    share(0)

    @pl.loop(0, n_y)
    def _(t):
        table_arrival(t, 2).wait_recv()
        for k in range(2):
            b_arrival(t, k).wait_recv()
        spread(t, (xo,))

        @pl.when(t + 1 < n_y)
        def _():
            pass_on(t + 1)

        @pl.when(t + 2 < n_y)
        def _():
            send_own(t + 2)

        for b in range(n_x):
            s_arrival(t, b).wait_recv()
            s_copy(t, b).wait_send()
        multiply(t, 0, n_grp // 2)

        @pl.when(t + 1 < n_y)
        def _():
            spread(t + 1, (xx,))

        multiply(t, n_grp // 2, n_grp)

        @pl.when(t > 1)
        def _():
            last_sums(t - 1)

        @pl.when(t + 1 < n_y)
        def _():
            share(t + 1)

        for k in range(2):
            for h in range(2):
                a_copy(t, k, h).wait_send()
            b_copy(t, k).wait_send()
        first_sums(t)

        @pl.when(t > 0)
        def _():
            early_sums(t)

        gather_back(t, (xx,))

        @pl.loop(0, n_grp)
        def _(i):
            p_copy(t, i).wait_send()

        @pl.when(t > 2)
        def _():
            give_back(t - 2, False)

    top = jnp.max(table[:, :, 0, packed:width])
    flags[0] = jnp.full((1, 128), top, jnp.int32)
    flag_copy().start()
    last_sums(n_y - 1)
    early_sums(0)
    last_sums(0)
    for t in range(1, n_y + 1):
        if n_y - 2 <= t < n_y:
            give_back(t, False)
        if t > 1:
            h_copy(t - 1).wait_recv()
            combine_into(t - 1, t == 2)
    flag_copy().wait()
    most_ref[...] = jnp.maximum(flags[0], flags[1])
    for t in range(1, n_y):
        list_copy(t).wait_send()
        y_copy(t).wait_send()
        h_copy(t).wait_send()

    @pl.loop(0, n_y)
    def _(t):
        for k in range(3):
            table_copy(t, k).wait_send()
        for k in range(2):
            e_copy(t, k).wait_send()
            n_copy(t, k).wait_send()
            f_copy(t, k).wait_send()

    give_back(0, True)
    combine_into(0, False)


def packed_layer(ids_loc, x_loc, wg, wu, wd, n_y, n_tp, packed, cap):
    tok, d_model = x_loc.shape
    n_loc, _, hidden = wg.shape
    n_x = n_tp // 2
    n_grp = n_loc // GROUP
    half = packed // 2
    width = -(-(packed + 1) // 128) * 128
    dma = pltpu.SemaphoreType.DMA
    hbm = pl.BlockSpec(memory_space=pltpu.HBM)
    vmem = pl.BlockSpec(memory_space=pltpu.VMEM)
    return pl.pallas_call(
        functools.partial(packed_kernel, n_y, n_x, packed, cap),
        out_shape=(jax.ShapeDtypeStruct((tok, d_model), BF16), jax.ShapeDtypeStruct((1, 128), jnp.int32)),
        in_specs=[vmem] * 2 + [hbm] * 3,
        out_specs=(vmem, vmem),
        scratch_shapes=[
            pltpu.VMEM((n_y, packed, d_model), BF16),
            pltpu.VMEM((n_y, n_x, packed, d_model), BF16),
            pltpu.VMEM((2, n_loc, 2 * n_x, cap, d_model), BF16),
            pltpu.VMEM((2, n_loc, n_x, cap, d_model), BF16),
            pltpu.VMEM((2, n_y, half, d_model), BF16),
            pltpu.VMEM((2, n_y, packed, d_model), BF16),
            pltpu.VMEM((n_y, packed, d_model), BF16),
            pltpu.VMEM((W_SLOTS, GROUP, d_model, 2 * hidden), BF16),
            pltpu.VMEM((W_SLOTS, GROUP, hidden, d_model), BF16),
            pltpu.VMEM((tok, 128), F32),
            pltpu.VMEM((n_y, 1, width), jnp.int32),
            pltpu.VMEM((n_y, n_x, 1, width), jnp.int32),
            pltpu.VMEM((2, 1, 128), jnp.int32),
            dma((n_y,)), dma((n_y,)), dma((n_y, 3)), dma((n_y, 3)), dma, dma,
            dma((n_y,)), dma((n_y,)),
            dma((n_y, 2, 2)), dma((n_y, 2, 2)),
            dma((n_y, 2)), dma((n_y, 2)),
            dma((n_y, n_x)), dma((n_y, n_x)),
            dma((n_y, n_grp)), dma((n_y, n_grp)),
            dma((n_y, 2)), dma((n_y, 2)),
            dma((n_y, 2)), dma((n_y, 2)),
            dma((n_y, 2)), dma((n_y, 2)),
            dma((n_y,)), dma((n_y,)),
            dma((W_SLOTS, 3)),
        ],
        compiler_params=pltpu.CompilerParams(
            collective_id=2, has_side_effects=True, vmem_limit_bytes=67043328
        ),
        name="packed_layer",
    )(ids_loc.reshape(1, tok), x_loc, wg, wu, wd)


def solution(mesh):
    n_y, n_tp = mesh.shape["ep"], mesh.shape["tp"]
    row_spec = P(("dp", "ep", "tp"), None)

    def local_layer(x_loc, ids_loc, gate_loc, wg_loc, wu_loc, wd_loc):
        tok, d_model = x_loc.shape
        n_loc = wg_loc.shape[0]
        n_exp = n_loc * n_y
        capacity = CAP_FACTOR * tok // n_exp
        packed = n_loc * capacity * 5 // 8
        picked, most = packed_layer(ids_loc, x_loc, wg_loc, wu_loc, wd_loc, n_y, n_tp, packed, capacity)

        def by_slots(carry):
            rows, pos = dispatch(x_loc, ids_loc, n_exp, capacity)
            y = experts(rows.reshape(n_exp, capacity, d_model), wg_loc, wu_loc, wd_loc, n_y, n_tp)
            return combine(pos, y.reshape(n_exp * capacity, d_model)), jnp.int32(0)

        picked, _ = lax.while_loop(lambda carry: carry[1] > packed, by_slots, (picked, most[0, 0]))
        return (picked.astype(F32) * gate_loc).astype(BF16)

    return jax.shard_map(local_layer, mesh=mesh, in_specs=(row_spec, row_spec, row_spec, P("ep", None, "tp"), P("ep", None, "tp"), P("ep", "tp", None)), out_specs=row_spec, check_vma=False)
```

```python
import functools

import jax
import jax.numpy as jnp
from jax import lax
from jax.experimental import pallas as pl
from jax.experimental.pallas import tpu as pltpu
from jax.sharding import PartitionSpec as P

CAP_FACTOR = 2
GROUP = 2
W_SLOTS = 4
EXTRA = 64
VMEM_LIMIT = 59 * 2**20
MESH = pl.DeviceIdType.MESH
BF16 = jnp.bfloat16
F32 = jnp.float32


def halves(packed):
    first = -(-packed // 32) * 16
    return first, packed - first


def packed_kernel(
    n_y, n_x, packed, cap, base_ref, ids_ref, gate_ref, x_ref, wg_hbm, wu_hbm, wd_hbm, out_ref, most_ref,
    pack_buf, x_buf, slot_buf, pair_buf, opp_buf, nbr_buf, ret_buf, w_in, w_out, pos_col, gate_col,
    lists, table, flags, l_send, l_recv, t_send, t_recv, m_send, m_recv, ys_send, ys_recv, a_send, a_recv, b_send, b_recv, s_send, s_recv,
    p_send, p_recv, e_send, e_recv, n_send, n_recv, f_send, f_recv, h_send, h_recv, w_sem,
):
    tok, d_model = x_ref.shape
    n_loc = slot_buf.shape[1]
    n_slots = n_loc * cap
    hidden = w_out.shape[2]
    sizes = halves(packed)
    n_src = 2 * n_x
    n_grp = n_loc // GROUP
    n_w = n_y * n_grp
    yy = lax.axis_index("ep")
    tt = lax.axis_index("tp")
    xx, cc = tt // 2, tt % 2
    xr, xl, xo = (xx + n_x + 1 - 2 * cc) % n_x, (xx + n_x - 1 + 2 * cc) % n_x, (xx + 2) % n_x
    right, left, mate = {"tp": xr * 2 + cc}, {"tp": xl * 2 + cc}, {"tp": xx * 2 + 1 - cc}
    across = {"tp": xo * 2 + cc}
    sides = (right, left)
    ahead, behind = (xr, xl), (xl, xr)
    mine, other = cc * n_x, (1 - cc) * n_x
    width = table.shape[3]
    n_exp = n_loc * n_y

    def row_of(t):
        return (yy + t + cc * (n_y - 2 * t) + n_y) % n_y

    def row_to(t):
        return (yy - t - cc * (n_y - 2 * t) + 2 * n_y) % n_y

    def remote(src, dst, send, recv, device):
        return pltpu.make_async_remote_copy(
            src_ref=src, dst_ref=dst, send_sem=send, recv_sem=recv, device_id=device, device_id_type=MESH
        )

    def part(h):
        return pl.ds(h * sizes[0], sizes[h])

    def y_copy(t):
        return remote(pack_buf.at[t], x_buf.at[t, xx], ys_send.at[t], ys_recv.at[t], {"ep": row_to(t)})

    def list_copy(t):
        return remote(lists.at[t], table.at[t, xx], l_send.at[t], l_recv.at[t], {"ep": row_to(t)})

    def table_copy(t, k):
        view = table.at[t, xx]
        return remote(view, view, t_send.at[t, k], t_recv.at[t, k], (right, left, across)[k])

    def table_arrival(t, k):
        view = table.at[t, (xl, xr, xo)[k]]
        return remote(view, view, t_send.at[t, k], t_recv.at[t, k], (right, left, across)[k])

    def flag_copy():
        return remote(flags.at[0], flags.at[1], m_send, m_recv, mate)

    def a_copy(t, k, h):
        view = x_buf.at[t, xx, part(h)]
        return remote(view, view, a_send.at[t, k, h], a_recv.at[t, k, h], sides[k])

    def a_arrival(t, k, h):
        view = x_buf.at[t, behind[k], part(h)]
        return remote(view, view, a_send.at[t, k, h], a_recv.at[t, k, h], sides[k])

    def b_copy(t, k):
        view = x_buf.at[t, behind[k], part(k)]
        return remote(view, view, b_send.at[t, k], b_recv.at[t, k], sides[k])

    def b_arrival(t, k):
        view = x_buf.at[t, xo, part(k)]
        return remote(view, view, b_send.at[t, k], b_recv.at[t, k], sides[k])

    def s_copy(t, b):
        view = slot_buf.at[t % 2, :, mine + b]
        return remote(view, view, s_send.at[t, b], s_recv.at[t, b], mate)

    def s_arrival(t, b):
        view = slot_buf.at[t % 2, :, other + b]
        return remote(view, view, s_send.at[t, b], s_recv.at[t, b], mate)

    def p_copy(t, i):
        at = pl.ds(i * GROUP, GROUP)
        return remote(
            slot_buf.at[t % 2, at, pl.ds(other, n_x)], pair_buf.at[t % 2, at], p_send.at[t, i], p_recv.at[t, i], mate
        )

    def e_copy(t, k):
        dst = opp_buf.at[k, t, pl.ds(0, sizes[k])]
        return remote(x_buf.at[t, xo, part(k)], dst, e_send.at[t, k], e_recv.at[t, k], sides[k])

    def n_copy(t, k):
        h = 1 - k
        return remote(
            x_buf.at[t, ahead[k], part(h)], nbr_buf.at[k, t, part(h)], n_send.at[t, k], n_recv.at[t, k], sides[k]
        )

    def f_copy(t, k):
        return remote(
            x_buf.at[t, ahead[k], part(k)], nbr_buf.at[k, t, part(k)], f_send.at[t, k], f_recv.at[t, k], sides[k]
        )

    def h_copy(t):
        return remote(x_buf.at[t, xx], ret_buf.at[t], h_send.at[t], h_recv.at[t], {"ep": row_of(t)})

    def w_copies(w):
        s = w % W_SLOTS
        at = pl.ds((w % n_grp) * GROUP, GROUP)
        return (
            pltpu.make_async_copy(wg_hbm.at[at], w_in.at[s, :, :, pl.ds(0, hidden)], w_sem.at[s, 0]),
            pltpu.make_async_copy(wu_hbm.at[at], w_in.at[s, :, :, pl.ds(hidden, hidden)], w_sem.at[s, 1]),
            pltpu.make_async_copy(wd_hbm.at[at], w_out.at[s], w_sem.at[s, 2]),
        )

    barrier = pltpu.get_barrier_semaphore()
    for device in [right, left, across, mate] + [{"ep": (yy + d) % n_y} for d in range(1, n_y)]:
        pl.semaphore_signal(barrier, inc=1, device_id=device, device_id_type=MESH)
    for w in range(W_SLOTS):
        for c in w_copies(w):
            c.start()

    ids = ids_ref[...]
    lanes = 128
    order = (lax.broadcasted_iota(jnp.int32, (lanes, 2 * lanes), 0), lax.broadcasted_iota(jnp.int32, (lanes, 2 * lanes), 1))
    earlier = ((order[0] < order[1]) | (order[1] >= lanes)).astype(F32).astype(BF16)

    def count_left(marks):
        n = marks.shape[0]
        tiles = [marks[:, i * lanes:(i + 1) * lanes] for i in range(tok // lanes)]
        both = jnp.dot(jnp.concatenate(tiles, axis=0).astype(BF16), earlier, preferred_element_type=F32)
        total, left = jnp.zeros((n, lanes), F32), []
        for i in range(len(tiles)):
            left.append(both[i * n:(i + 1) * n, :lanes] + total)
            total = total + both[i * n:(i + 1) * n, lanes:]
        return jnp.concatenate(left, axis=1), total

    one_hot = lax.broadcasted_iota(jnp.int32, (n_exp, tok), 0) == ids
    preceding, _ = count_left(one_hot.astype(F32))
    slot = jnp.sum(jnp.where(one_hot, preceding, 0.0), axis=0, keepdims=True)
    kept = slot < cap
    rank = ids // n_loc
    pad = 8
    to_rank = (lax.broadcasted_iota(jnp.int32, (pad, tok), 0) == rank) & kept
    before, counts = count_left(to_rank.astype(F32))
    place = jnp.sum(jnp.where(to_rank, before, 0.0), axis=0, keepdims=True).astype(jnp.int32) - base_ref[0]
    most = jnp.max(counts, axis=0, keepdims=True).astype(jnp.int32)[:, 0:width - packed]
    pos = jnp.where(kept & (place >= 0) & (place < packed), rank * packed + place, -1)
    row_id = lax.broadcasted_iota(jnp.int32, (pad, tok), 0)
    parts = jnp.where(row_id == 0, (ids % n_loc).astype(F32), jnp.where(row_id == 1, slot, 1.0))
    parts = jnp.where(kept, parts, 0.0).astype(BF16)

    def wanted(t):
        pick = (lax.broadcasted_iota(jnp.int32, (packed, tok), 0) + row_to(t) * packed) == pos
        return pick.astype(F32).astype(BF16)

    def pack(t):
        return jnp.dot(wanted(t), x_ref[...], preferred_element_type=F32).astype(BF16)

    def list_of(t):
        got = lax.dot_general(parts, wanted(t), (((1,), (1,)), ((), ())), preferred_element_type=F32)
        return jnp.where(got[2:3] > 0.5, got[0:1] * cap + got[1:2], -1.0).astype(jnp.int32)

    def send_half(t, h):
        for k in range(2):
            a_copy(t, k, h if k == 0 else 1 - h).start()

    def send_table(t):
        for k in (2, 0, 1):
            table_copy(t, k).start()

    def send_own(t):
        list_copy(t).wait_recv()
        send_table(t)
        y_copy(t).wait_recv()
        send_half(t, 0)
        send_half(t, 1)

    def pass_on(t):
        for k in range(2):
            a_arrival(t, k, k).wait_recv()
            b_copy(t, k).start()

    def source_row(t, b):
        return table[t, b][:, :packed]

    def spread(t, blocks):
        @pl.loop(0, len(blocks))
        def _(j):
            b = blocks[0]
            for n, blk in enumerate(blocks[1:]):
                b = jnp.where(j == n + 1, blk, b)
            to = source_row(t, b)
            pick = (lax.broadcasted_iota(jnp.int32, (n_slots, packed), 0) == to).astype(F32).astype(BF16)
            slots = jnp.dot(pick, x_buf[t, b], preferred_element_type=F32).astype(BF16)
            slot_buf[t % 2, :, mine + b] = slots.reshape(n_loc, cap, d_model)
            s_copy(t, b).start()

    def share(t):
        for k in range(2):
            table_arrival(t, k).wait_recv()
            a_arrival(t, k, 1 - k).wait_recv()
        spread(t, (xl, xr))

    def multiply(t, lo, hi):
        @pl.loop(lo, hi)
        def _(i):
            w = t * n_grp + i
            s = w % W_SLOTS
            for c in w_copies(w):
                c.wait()
            both = []
            for el in range(GROUP):
                tile = slot_buf[t % 2, i * GROUP + el].reshape(n_src * cap, d_model)
                both.append(jnp.dot(tile, w_in[s, el], preferred_element_type=F32))
            for el in range(GROUP):
                act = (jax.nn.silu(both[el][:, :hidden]) * both[el][:, hidden:]).astype(BF16)
                out = jnp.dot(act, w_out[s, el], preferred_element_type=F32)
                slot_buf[t % 2, i * GROUP + el] = out.astype(BF16).reshape(n_src, cap, d_model)
            p_copy(t, i).start()

            @pl.when(w + W_SLOTS < n_w)
            def _():
                for c in w_copies(w + W_SLOTS):
                    c.start()

    def gather_back(t, blocks):
        @pl.loop(0, len(blocks))
        def _(j):
            b = blocks[0]
            for n, blk in enumerate(blocks[1:]):
                b = jnp.where(j == n + 1, blk, b)
            to = source_row(t, b).astype(F32)
            col = jnp.transpose(jnp.broadcast_to(to, (128, packed)))
            lane = lax.broadcasted_iota(jnp.int32, (packed, 128), 1).astype(F32)
            pick = jnp.concatenate(
                [(col == lane + float(128 * m)).astype(F32).astype(BF16) for m in range(n_slots // 128)], axis=1
            )
            total = slot_buf[t % 2, :, mine + b].astype(F32) + pair_buf[t % 2, :, b].astype(F32)
            slots = total.astype(BF16).reshape(n_slots, d_model)
            x_buf[t, b] = jnp.dot(pick, slots, preferred_element_type=F32).astype(BF16)

    def first_sums(t):
        @pl.loop(0, n_grp)
        def _(i):
            p_copy(t, i).wait_recv()

        gather_back(t, (xo,))
        for k in range(2):
            e_copy(t, k).start()
        gather_back(t, (xr, xl))

    def early_sums(t):
        for k in range(2):
            n_copy(t, k).start()

    def last_sums(t):
        for k in range(2):
            e_copy(t, k).wait_recv()
            at = (t, ahead[k], part(k))
            x_buf[at] = (x_buf[at].astype(F32) + opp_buf[k, t, pl.ds(0, sizes[k])].astype(F32)).astype(BF16)
            f_copy(t, k).start()

    def give_back(t, local):
        for k in range(2):
            n_copy(t, k).wait_recv()
            f_copy(t, k).wait_recv()
        total = x_buf[t, xx].astype(F32) + (nbr_buf[0, t].astype(F32) + nbr_buf[1, t].astype(F32))
        if local:
            ret_buf[t] = total.astype(BF16)
        else:
            x_buf[t, xx] = total.astype(BF16)
            h_copy(t).start()

    def combine_into(t, first):
        tile = 256

        @pl.loop(0, tok // tile)
        def _(i):
            rows = pl.ds(pl.multiple_of(i * tile, tile), tile)
            want = pos_col[rows, :] - (row_to(t) * packed).astype(F32)
            lane = lax.broadcasted_iota(jnp.int32, (tile, 128), 1).astype(F32)
            pick = jnp.concatenate(
                [(want == lane + float(128 * m)).astype(F32) for m in range(-(-packed // 128))], axis=1
            )
            y = jnp.dot(pick[:, :packed].astype(BF16), ret_buf[t], preferred_element_type=F32)
            gate = gate_col[rows, :]
            y = jnp.concatenate([y[:, m * 128:(m + 1) * 128] * gate for m in range(d_model // 128)], axis=1)
            if not first:
                y = y + out_ref[rows, :].astype(F32)
            out_ref[rows, :] = y.astype(BF16)

    x_buf[0, xx] = pack(0)
    pl.semaphore_wait(barrier, 3 + n_y)
    send_half(0, 0)
    table[0, xx, :, 0:packed] = list_of(0)
    table[0, xx, :, packed:width] = most
    send_table(0)
    send_half(0, 1)

    @pl.loop(1, n_y)
    def _(t):
        lists[t, :, 0:packed] = list_of(t)
        lists[t, :, packed:width] = most
        list_copy(t).start()
        pack_buf[t] = pack(t)
        y_copy(t).start()

    spread(0, (xx,))
    pass_on(0)
    send_own(1)
    tile = 256
    for i in range(tok // tile):
        spot = pos[:, i * tile:(i + 1) * tile].astype(F32)
        pos_col[i * tile:(i + 1) * tile, :] = jnp.transpose(jnp.broadcast_to(spot, (128, tile)))
        gate = gate_ref[:, i * tile:(i + 1) * tile]
        gate_col[i * tile:(i + 1) * tile, :] = jnp.transpose(jnp.broadcast_to(gate, (128, tile)))
    share(0)

    @pl.loop(0, n_y)
    def _(t):
        table_arrival(t, 2).wait_recv()
        for k in range(2):
            b_arrival(t, k).wait_recv()
        spread(t, (xo,))

        @pl.when(t + 1 < n_y)
        def _():
            pass_on(t + 1)

        @pl.when(t + 2 < n_y)
        def _():
            send_own(t + 2)

        for b in range(n_x):
            s_arrival(t, b).wait_recv()
            s_copy(t, b).wait_send()
        multiply(t, 0, n_grp // 2)

        @pl.when(t + 1 < n_y)
        def _():
            spread(t + 1, (xx,))

        multiply(t, n_grp // 2, n_grp)

        @pl.when(t > 1)
        def _():
            last_sums(t - 1)

        @pl.when(t + 1 < n_y)
        def _():
            share(t + 1)

        for k in range(2):
            for h in range(2):
                a_copy(t, k, h).wait_send()
            b_copy(t, k).wait_send()
        first_sums(t)

        @pl.when(t > 0)
        def _():
            early_sums(t)

        gather_back(t, (xx,))

        @pl.loop(0, n_grp)
        def _(i):
            p_copy(t, i).wait_send()

        @pl.when(t > 2)
        def _():
            give_back(t - 2, False)

    top = jnp.max(table[:, :, 0, packed:width])
    flags[0] = jnp.full((1, 128), top, jnp.int32)
    flag_copy().start()
    last_sums(n_y - 1)
    early_sums(0)
    last_sums(0)
    for t in range(1, n_y + 1):
        if n_y - 2 <= t < n_y:
            give_back(t, False)
        if t > 1:
            h_copy(t - 1).wait_recv()
            combine_into(t - 1, t == 2)
    flag_copy().wait()
    most_ref[...] = jnp.maximum(flags[0], flags[1])
    for t in range(1, n_y):
        list_copy(t).wait_send()
        y_copy(t).wait_send()
        h_copy(t).wait_send()

    @pl.loop(0, n_y)
    def _(t):
        for k in range(3):
            table_copy(t, k).wait_send()
        for k in range(2):
            e_copy(t, k).wait_send()
            n_copy(t, k).wait_send()
            f_copy(t, k).wait_send()

    give_back(0, True)
    combine_into(0, False)


def packed_layer(base, ids_loc, gate_loc, x_loc, wg, wu, wd, n_y, n_tp, packed, cap, collective_id):
    tok, d_model = x_loc.shape
    n_loc, _, hidden = wg.shape
    n_x = n_tp // 2
    n_grp = n_loc // GROUP
    half = halves(packed)[0]
    width = -(-(packed + 1) // 128) * 128
    dma = pltpu.SemaphoreType.DMA
    hbm = pl.BlockSpec(memory_space=pltpu.HBM)
    vmem = pl.BlockSpec(memory_space=pltpu.VMEM)
    return pl.pallas_call(
        functools.partial(packed_kernel, n_y, n_x, packed, cap),
        out_shape=(jax.ShapeDtypeStruct((tok, d_model), BF16), jax.ShapeDtypeStruct((1, 128), jnp.int32)),
        in_specs=[pl.BlockSpec(memory_space=pltpu.SMEM)] + [vmem] * 3 + [hbm] * 3,
        out_specs=(vmem, vmem),
        scratch_shapes=[
            pltpu.VMEM((n_y, packed, d_model), BF16),
            pltpu.VMEM((n_y, n_x, packed, d_model), BF16),
            pltpu.VMEM((2, n_loc, 2 * n_x, cap, d_model), BF16),
            pltpu.VMEM((2, n_loc, n_x, cap, d_model), BF16),
            pltpu.VMEM((2, n_y, half, d_model), BF16),
            pltpu.VMEM((2, n_y, packed, d_model), BF16),
            pltpu.VMEM((n_y, packed, d_model), BF16),
            pltpu.VMEM((W_SLOTS, GROUP, d_model, 2 * hidden), BF16),
            pltpu.VMEM((W_SLOTS, GROUP, hidden, d_model), BF16),
            pltpu.VMEM((tok, 128), F32),
            pltpu.VMEM((tok, 128), F32),
            pltpu.VMEM((n_y, 1, width), jnp.int32),
            pltpu.VMEM((n_y, n_x, 1, width), jnp.int32),
            pltpu.VMEM((2, 1, 128), jnp.int32),
            dma((n_y,)), dma((n_y,)), dma((n_y, 3)), dma((n_y, 3)), dma, dma,
            dma((n_y,)), dma((n_y,)),
            dma((n_y, 2, 2)), dma((n_y, 2, 2)),
            dma((n_y, 2)), dma((n_y, 2)),
            dma((n_y, n_x)), dma((n_y, n_x)),
            dma((n_y, n_grp)), dma((n_y, n_grp)),
            dma((n_y, 2)), dma((n_y, 2)),
            dma((n_y, 2)), dma((n_y, 2)),
            dma((n_y, 2)), dma((n_y, 2)),
            dma((n_y,)), dma((n_y,)),
            dma((W_SLOTS, 3)),
        ],
        compiler_params=pltpu.CompilerParams(
            collective_id=collective_id, has_side_effects=True, vmem_limit_bytes=VMEM_LIMIT
        ),
        name="packed_layer",
    )(base.reshape(1), ids_loc.reshape(1, tok), gate_loc.reshape(1, tok), x_loc, wg, wu, wd)


def solution(mesh):
    n_y, n_tp = mesh.shape["ep"], mesh.shape["tp"]
    row_spec = P(("dp", "ep", "tp"), None)

    def local_layer(x_loc, ids_loc, gate_loc, wg_loc, wu_loc, wd_loc):
        tok, d_model = x_loc.shape
        n_loc = wg_loc.shape[0]
        n_exp = n_loc * n_y
        capacity = CAP_FACTOR * tok // n_exp
        packed = n_loc * capacity * 19 // 32
        args = (ids_loc, gate_loc, x_loc, wg_loc, wu_loc, wd_loc, n_y, n_tp)
        out, most = packed_layer(jnp.int32(0), *args, packed, capacity, 0)

        def more(carry):
            total, base = carry
            extra, _ = packed_layer(base, *args, EXTRA, capacity, 1)
            return total + extra, base + EXTRA

        out, _ = lax.while_loop(lambda carry: carry[1] < most[0, 0], more, (out, jnp.int32(packed)))
        return out

    return jax.shard_map(local_layer, mesh=mesh, in_specs=(row_spec, row_spec, row_spec, P("ep", None, "tp"), P("ep", None, "tp"), P("ep", "tp", None)), out_specs=row_spec, check_vma=False)
```

```python
import functools

import jax
import jax.numpy as jnp
from jax import lax
from jax.experimental import pallas as pl
from jax.experimental.pallas import tpu as pltpu
from jax.sharding import PartitionSpec as P

CAP_FACTOR = 2
GROUP = 2
W_SLOTS = 4
EXTRA = 64
VMEM_LIMIT = 59 * 2**20
MESH = pl.DeviceIdType.MESH
BF16 = jnp.bfloat16
F32 = jnp.float32


def halves(packed):
    first = -(-packed // 32) * 16
    return first, packed - first


def packed_kernel(
    n_y, n_x, packed, cap, base_ref, ids_ref, gate_ref, x_hbm, wg_hbm, wu_hbm, wd_hbm, out_ref, most_ref,
    x_ref, x_sem, pack_buf, x_buf, slot_buf, pair_buf, opp_buf, nbr_buf, ret_buf, w_in, w_out, pos_col, gate_col,
    lists, table, flags, l_send, l_recv, t_send, t_recv, m_send, m_recv, ys_send, ys_recv, a_send, a_recv, b_send, b_recv, s_send, s_recv,
    p_send, p_recv, e_send, e_recv, n_send, n_recv, f_send, f_recv, h_send, h_recv, w_sem,
):
    tok, d_model = x_ref.shape
    n_loc = slot_buf.shape[1]
    n_slots = n_loc * cap
    hidden = w_out.shape[2]
    sizes = halves(packed)
    n_src = 2 * n_x
    n_grp = n_loc // GROUP
    n_w = n_y * n_grp
    yy = lax.axis_index("ep")
    tt = lax.axis_index("tp")
    xx, cc = tt // 2, tt % 2
    xr, xl, xo = (xx + n_x + 1 - 2 * cc) % n_x, (xx + n_x - 1 + 2 * cc) % n_x, (xx + 2) % n_x
    right, left, mate = {"tp": xr * 2 + cc}, {"tp": xl * 2 + cc}, {"tp": xx * 2 + 1 - cc}
    across = {"tp": xo * 2 + cc}
    sides = (right, left)
    ahead, behind = (xr, xl), (xl, xr)
    mine, other = cc * n_x, (1 - cc) * n_x
    width = table.shape[3]
    n_exp = n_loc * n_y

    def row_of(t):
        return (yy + t + cc * (n_y - 2 * t) + n_y) % n_y

    def row_to(t):
        return (yy - t - cc * (n_y - 2 * t) + 2 * n_y) % n_y

    def remote(src, dst, send, recv, device):
        return pltpu.make_async_remote_copy(
            src_ref=src, dst_ref=dst, send_sem=send, recv_sem=recv, device_id=device, device_id_type=MESH
        )

    def part(h):
        return pl.ds(h * sizes[0], sizes[h])

    def y_copy(t):
        return remote(pack_buf.at[t], x_buf.at[t, xx], ys_send.at[t], ys_recv.at[t], {"ep": row_to(t)})

    def list_copy(t):
        return remote(lists.at[t], table.at[t, xx], l_send.at[t], l_recv.at[t], {"ep": row_to(t)})

    def table_copy(t, k):
        view = table.at[t, xx]
        return remote(view, view, t_send.at[t, k], t_recv.at[t, k], (right, left, across)[k])

    def table_arrival(t, k):
        view = table.at[t, (xl, xr, xo)[k]]
        return remote(view, view, t_send.at[t, k], t_recv.at[t, k], (right, left, across)[k])

    def flag_copy():
        return remote(flags.at[0], flags.at[1], m_send, m_recv, mate)

    def a_copy(t, k, h):
        view = x_buf.at[t, xx, part(h)]
        return remote(view, view, a_send.at[t, k, h], a_recv.at[t, k, h], sides[k])

    def a_arrival(t, k, h):
        view = x_buf.at[t, behind[k], part(h)]
        return remote(view, view, a_send.at[t, k, h], a_recv.at[t, k, h], sides[k])

    def b_copy(t, k):
        view = x_buf.at[t, behind[k], part(k)]
        return remote(view, view, b_send.at[t, k], b_recv.at[t, k], sides[k])

    def b_arrival(t, k):
        view = x_buf.at[t, xo, part(k)]
        return remote(view, view, b_send.at[t, k], b_recv.at[t, k], sides[k])

    def s_copy(t, b):
        view = slot_buf.at[t % 2, :, mine + b]
        return remote(view, view, s_send.at[t, b], s_recv.at[t, b], mate)

    def s_arrival(t, b):
        view = slot_buf.at[t % 2, :, other + b]
        return remote(view, view, s_send.at[t, b], s_recv.at[t, b], mate)

    def p_copy(t, i):
        at = pl.ds(i * GROUP, GROUP)
        return remote(
            slot_buf.at[t % 2, at, pl.ds(other, n_x)], pair_buf.at[t % 2, at], p_send.at[t, i], p_recv.at[t, i], mate
        )

    def e_copy(t, k):
        dst = opp_buf.at[k, t, pl.ds(0, sizes[k])]
        return remote(x_buf.at[t, xo, part(k)], dst, e_send.at[t, k], e_recv.at[t, k], sides[k])

    def n_copy(t, k):
        h = 1 - k
        return remote(
            x_buf.at[t, ahead[k], part(h)], nbr_buf.at[k, t, part(h)], n_send.at[t, k], n_recv.at[t, k], sides[k]
        )

    def f_copy(t, k):
        return remote(
            x_buf.at[t, ahead[k], part(k)], nbr_buf.at[k, t, part(k)], f_send.at[t, k], f_recv.at[t, k], sides[k]
        )

    def h_copy(t):
        return remote(x_buf.at[t, xx], ret_buf.at[t], h_send.at[t], h_recv.at[t], {"ep": row_of(t)})

    def w_copies(w):
        s = w % W_SLOTS
        at = pl.ds((w % n_grp) * GROUP, GROUP)
        return (
            pltpu.make_async_copy(wg_hbm.at[at], w_in.at[s, :, :, pl.ds(0, hidden)], w_sem.at[s, 0]),
            pltpu.make_async_copy(wu_hbm.at[at], w_in.at[s, :, :, pl.ds(hidden, hidden)], w_sem.at[s, 1]),
            pltpu.make_async_copy(wd_hbm.at[at], w_out.at[s], w_sem.at[s, 2]),
        )

    x_copy = pltpu.make_async_copy(x_hbm, x_ref, x_sem)
    x_copy.start()
    barrier = pltpu.get_barrier_semaphore()
    for device in [right, left, across, mate] + [{"ep": (yy + d) % n_y} for d in range(1, n_y)]:
        pl.semaphore_signal(barrier, inc=1, device_id=device, device_id_type=MESH)
    for w in range(W_SLOTS):
        for c in w_copies(w):
            c.start()

    ids = ids_ref[...]
    lanes = 128
    order = (lax.broadcasted_iota(jnp.int32, (lanes, 2 * lanes), 0), lax.broadcasted_iota(jnp.int32, (lanes, 2 * lanes), 1))
    earlier = ((order[0] < order[1]) | (order[1] >= lanes)).astype(F32).astype(BF16)

    def count_left(marks):
        n = marks.shape[0]
        tiles = [marks[:, i * lanes:(i + 1) * lanes] for i in range(tok // lanes)]
        both = jnp.dot(jnp.concatenate(tiles, axis=0).astype(BF16), earlier, preferred_element_type=F32)
        total, left = jnp.zeros((n, lanes), F32), []
        for i in range(len(tiles)):
            left.append(both[i * n:(i + 1) * n, :lanes] + total)
            total = total + both[i * n:(i + 1) * n, lanes:]
        return jnp.concatenate(left, axis=1), total

    one_hot = lax.broadcasted_iota(jnp.int32, (n_exp, tok), 0) == ids
    preceding, _ = count_left(one_hot.astype(F32))
    slot = jnp.sum(jnp.where(one_hot, preceding, 0.0), axis=0, keepdims=True)
    kept = slot < cap
    rank = ids // n_loc
    pad = 8
    to_rank = (lax.broadcasted_iota(jnp.int32, (pad, tok), 0) == rank) & kept
    before, counts = count_left(to_rank.astype(F32))
    place = jnp.sum(jnp.where(to_rank, before, 0.0), axis=0, keepdims=True).astype(jnp.int32) - base_ref[0]
    most = jnp.max(counts, axis=0, keepdims=True).astype(jnp.int32)[:, 0:width - packed]
    pos = jnp.where(kept & (place >= 0) & (place < packed), rank * packed + place, -1)
    row_id = lax.broadcasted_iota(jnp.int32, (pad, tok), 0)
    parts = jnp.where(row_id == 0, (ids % n_loc).astype(F32), jnp.where(row_id == 1, slot, 1.0))
    parts = jnp.where(kept, parts, 0.0).astype(BF16)

    def wanted(t):
        pick = (lax.broadcasted_iota(jnp.int32, (packed, tok), 0) + row_to(t) * packed) == pos
        return pick.astype(F32).astype(BF16)

    def pack(t):
        return jnp.dot(wanted(t), x_ref[...], preferred_element_type=F32).astype(BF16)

    def list_of(t):
        got = lax.dot_general(parts, wanted(t), (((1,), (1,)), ((), ())), preferred_element_type=F32)
        return jnp.where(got[2:3] > 0.5, got[0:1] * cap + got[1:2], -1.0).astype(jnp.int32)

    def send_half(t, h):
        for k in range(2):
            a_copy(t, k, h if k == 0 else 1 - h).start()

    def send_table(t):
        for k in (2, 0, 1):
            table_copy(t, k).start()

    def send_own(t):
        list_copy(t).wait_recv()
        send_table(t)
        y_copy(t).wait_recv()
        send_half(t, 0)
        send_half(t, 1)

    def pass_on(t):
        for k in range(2):
            a_arrival(t, k, k).wait_recv()
            b_copy(t, k).start()

    def source_row(t, b):
        return table[t, b][:, :packed]

    def spread(t, blocks):
        @pl.loop(0, len(blocks))
        def _(j):
            b = blocks[0]
            for n, blk in enumerate(blocks[1:]):
                b = jnp.where(j == n + 1, blk, b)
            to = source_row(t, b)
            pick = (lax.broadcasted_iota(jnp.int32, (n_slots, packed), 0) == to).astype(F32).astype(BF16)
            slots = jnp.dot(pick, x_buf[t, b], preferred_element_type=F32).astype(BF16)
            slot_buf[t % 2, :, mine + b] = slots.reshape(n_loc, cap, d_model)
            s_copy(t, b).start()

    def share(t):
        for k in range(2):
            table_arrival(t, k).wait_recv()
            a_arrival(t, k, 1 - k).wait_recv()
        spread(t, (xl, xr))

    def multiply(t, lo, hi):
        @pl.loop(lo, hi)
        def _(i):
            w = t * n_grp + i
            s = w % W_SLOTS
            for c in w_copies(w):
                c.wait()
            both = []
            for el in range(GROUP):
                tile = slot_buf[t % 2, i * GROUP + el].reshape(n_src * cap, d_model)
                both.append(jnp.dot(tile, w_in[s, el], preferred_element_type=F32))
            for el in range(GROUP):
                act = (jax.nn.silu(both[el][:, :hidden]) * both[el][:, hidden:]).astype(BF16)
                out = jnp.dot(act, w_out[s, el], preferred_element_type=F32)
                slot_buf[t % 2, i * GROUP + el] = out.astype(BF16).reshape(n_src, cap, d_model)
            p_copy(t, i).start()

            @pl.when(w + W_SLOTS < n_w)
            def _():
                for c in w_copies(w + W_SLOTS):
                    c.start()

    def gather_back(t, blocks):
        @pl.loop(0, len(blocks))
        def _(j):
            b = blocks[0]
            for n, blk in enumerate(blocks[1:]):
                b = jnp.where(j == n + 1, blk, b)
            to = source_row(t, b).astype(F32)
            col = jnp.transpose(jnp.broadcast_to(to, (128, packed)))
            lane = lax.broadcasted_iota(jnp.int32, (packed, 128), 1).astype(F32)
            pick = jnp.concatenate(
                [(col == lane + float(128 * m)).astype(F32).astype(BF16) for m in range(n_slots // 128)], axis=1
            )
            total = slot_buf[t % 2, :, mine + b].astype(F32) + pair_buf[t % 2, :, b].astype(F32)
            slots = total.astype(BF16).reshape(n_slots, d_model)
            x_buf[t, b] = jnp.dot(pick, slots, preferred_element_type=F32).astype(BF16)

    def first_sums(t):
        @pl.loop(0, n_grp)
        def _(i):
            p_copy(t, i).wait_recv()

        gather_back(t, (xo,))
        for k in range(2):
            e_copy(t, k).start()
        gather_back(t, (xr, xl))

    def early_sums(t):
        for k in range(2):
            n_copy(t, k).start()

    def last_sums(t):
        for k in range(2):
            e_copy(t, k).wait_recv()
            at = (t, ahead[k], part(k))
            x_buf[at] = (x_buf[at].astype(F32) + opp_buf[k, t, pl.ds(0, sizes[k])].astype(F32)).astype(BF16)
            f_copy(t, k).start()

    def give_back(t, local):
        for k in range(2):
            n_copy(t, k).wait_recv()
            f_copy(t, k).wait_recv()
        total = x_buf[t, xx].astype(F32) + (nbr_buf[0, t].astype(F32) + nbr_buf[1, t].astype(F32))
        if local:
            ret_buf[t] = total.astype(BF16)
        else:
            x_buf[t, xx] = total.astype(BF16)
            h_copy(t).start()

    def combine_into(t, first):
        tile = 256

        @pl.loop(0, tok // tile)
        def _(i):
            rows = pl.ds(pl.multiple_of(i * tile, tile), tile)
            want = pos_col[rows, :] - (row_to(t) * packed).astype(F32)
            lane = lax.broadcasted_iota(jnp.int32, (tile, 128), 1).astype(F32)
            pick = jnp.concatenate(
                [(want == lane + float(128 * m)).astype(F32) for m in range(-(-packed // 128))], axis=1
            )
            y = jnp.dot(pick[:, :packed].astype(BF16), ret_buf[t], preferred_element_type=F32)
            gate = gate_col[rows, :]
            y = jnp.concatenate([y[:, m * 128:(m + 1) * 128] * gate for m in range(d_model // 128)], axis=1)
            if not first:
                y = y + out_ref[rows, :].astype(F32)
            out_ref[rows, :] = y.astype(BF16)

    x_copy.wait()
    x_buf[0, xx] = pack(0)
    pl.semaphore_wait(barrier, 3 + n_y)
    send_half(0, 0)
    table[0, xx, :, 0:packed] = list_of(0)
    table[0, xx, :, packed:width] = most
    send_table(0)
    send_half(0, 1)

    @pl.loop(1, n_y)
    def _(t):
        lists[t, :, 0:packed] = list_of(t)
        lists[t, :, packed:width] = most
        list_copy(t).start()
        pack_buf[t] = pack(t)
        y_copy(t).start()

    spread(0, (xx,))
    pass_on(0)
    send_own(1)
    tile = 256
    for i in range(tok // tile):
        spot = pos[:, i * tile:(i + 1) * tile].astype(F32)
        pos_col[i * tile:(i + 1) * tile, :] = jnp.transpose(jnp.broadcast_to(spot, (128, tile)))
        gate = gate_ref[:, i * tile:(i + 1) * tile]
        gate_col[i * tile:(i + 1) * tile, :] = jnp.transpose(jnp.broadcast_to(gate, (128, tile)))
    share(0)

    @pl.loop(0, n_y)
    def _(t):
        table_arrival(t, 2).wait_recv()
        for k in range(2):
            b_arrival(t, k).wait_recv()
        spread(t, (xo,))

        @pl.when(t + 1 < n_y)
        def _():
            pass_on(t + 1)

        @pl.when(t + 2 < n_y)
        def _():
            send_own(t + 2)

        for b in range(n_x):
            s_arrival(t, b).wait_recv()
            s_copy(t, b).wait_send()
        multiply(t, 0, n_grp // 2)

        @pl.when(t > 1)
        def _():
            last_sums(t - 1)

        @pl.when(t + 1 < n_y)
        def _():
            spread(t + 1, (xx,))

        multiply(t, n_grp // 2, n_grp)

        @pl.when(t + 1 < n_y)
        def _():
            share(t + 1)

        for k in range(2):
            for h in range(2):
                a_copy(t, k, h).wait_send()
            b_copy(t, k).wait_send()
        first_sums(t)

        @pl.when(t > 0)
        def _():
            early_sums(t)

        gather_back(t, (xx,))

        @pl.loop(0, n_grp)
        def _(i):
            p_copy(t, i).wait_send()

        @pl.when(t > 2)
        def _():
            give_back(t - 2, False)

    top = jnp.max(table[:, :, 0, packed:width])
    flags[0] = jnp.full((1, 128), top, jnp.int32)
    flag_copy().start()
    last_sums(n_y - 1)
    early_sums(0)
    last_sums(0)
    for t in range(1, n_y + 1):
        if n_y - 2 <= t < n_y:
            give_back(t, False)
        if t > 1:
            h_copy(t - 1).wait_recv()
            combine_into(t - 1, t == 2)
    flag_copy().wait()
    most_ref[...] = jnp.maximum(flags[0], flags[1])
    for t in range(1, n_y):
        list_copy(t).wait_send()
        y_copy(t).wait_send()
        h_copy(t).wait_send()

    @pl.loop(0, n_y)
    def _(t):
        for k in range(3):
            table_copy(t, k).wait_send()
        for k in range(2):
            e_copy(t, k).wait_send()
            n_copy(t, k).wait_send()
            f_copy(t, k).wait_send()

    give_back(0, True)
    combine_into(0, False)


def packed_layer(base, ids_loc, gate_loc, x_loc, wg, wu, wd, n_y, n_tp, packed, cap, collective_id):
    tok, d_model = x_loc.shape
    n_loc, _, hidden = wg.shape
    n_x = n_tp // 2
    n_grp = n_loc // GROUP
    half = halves(packed)[0]
    width = -(-(packed + 1) // 128) * 128
    dma = pltpu.SemaphoreType.DMA
    hbm = pl.BlockSpec(memory_space=pltpu.HBM)
    vmem = pl.BlockSpec(memory_space=pltpu.VMEM)
    return pl.pallas_call(
        functools.partial(packed_kernel, n_y, n_x, packed, cap),
        out_shape=(jax.ShapeDtypeStruct((tok, d_model), BF16), jax.ShapeDtypeStruct((1, 128), jnp.int32)),
        in_specs=[pl.BlockSpec(memory_space=pltpu.SMEM)] + [vmem] * 2 + [hbm] * 4,
        out_specs=(vmem, vmem),
        scratch_shapes=[
            pltpu.VMEM((tok, d_model), BF16),
            dma,
            pltpu.VMEM((n_y, packed, d_model), BF16),
            pltpu.VMEM((n_y, n_x, packed, d_model), BF16),
            pltpu.VMEM((2, n_loc, 2 * n_x, cap, d_model), BF16),
            pltpu.VMEM((2, n_loc, n_x, cap, d_model), BF16),
            pltpu.VMEM((2, n_y, half, d_model), BF16),
            pltpu.VMEM((2, n_y, packed, d_model), BF16),
            pltpu.VMEM((n_y, packed, d_model), BF16),
            pltpu.VMEM((W_SLOTS, GROUP, d_model, 2 * hidden), BF16),
            pltpu.VMEM((W_SLOTS, GROUP, hidden, d_model), BF16),
            pltpu.VMEM((tok, 128), F32),
            pltpu.VMEM((tok, 128), F32),
            pltpu.VMEM((n_y, 1, width), jnp.int32),
            pltpu.VMEM((n_y, n_x, 1, width), jnp.int32),
            pltpu.VMEM((2, 1, 128), jnp.int32),
            dma((n_y,)), dma((n_y,)), dma((n_y, 3)), dma((n_y, 3)), dma, dma,
            dma((n_y,)), dma((n_y,)),
            dma((n_y, 2, 2)), dma((n_y, 2, 2)),
            dma((n_y, 2)), dma((n_y, 2)),
            dma((n_y, n_x)), dma((n_y, n_x)),
            dma((n_y, n_grp)), dma((n_y, n_grp)),
            dma((n_y, 2)), dma((n_y, 2)),
            dma((n_y, 2)), dma((n_y, 2)),
            dma((n_y, 2)), dma((n_y, 2)),
            dma((n_y,)), dma((n_y,)),
            dma((W_SLOTS, 3)),
        ],
        compiler_params=pltpu.CompilerParams(
            collective_id=collective_id, has_side_effects=True, vmem_limit_bytes=VMEM_LIMIT
        ),
        name="packed_layer",
    )(base.reshape(1), ids_loc.reshape(1, tok), gate_loc.reshape(1, tok), x_loc, wg, wu, wd)


def solution(mesh):
    n_y, n_tp = mesh.shape["ep"], mesh.shape["tp"]
    row_spec = P(("dp", "ep", "tp"), None)

    def local_layer(x_loc, ids_loc, gate_loc, wg_loc, wu_loc, wd_loc):
        tok, d_model = x_loc.shape
        n_loc = wg_loc.shape[0]
        n_exp = n_loc * n_y
        capacity = CAP_FACTOR * tok // n_exp
        packed = n_loc * capacity * 19 // 32
        args = (ids_loc, gate_loc, x_loc, wg_loc, wu_loc, wd_loc, n_y, n_tp)
        out, most = packed_layer(jnp.int32(0), *args, packed, capacity, 0)

        def more(carry):
            total, base = carry
            extra, _ = packed_layer(base, *args, EXTRA, capacity, 1)
            return total + extra, base + EXTRA

        out, _ = lax.while_loop(lambda carry: carry[1] < most[0, 0], more, (out, jnp.int32(packed)))
        return out

    return jax.shard_map(local_layer, mesh=mesh, in_specs=(row_spec, row_spec, row_spec, P("ep", None, "tp"), P("ep", None, "tp"), P("ep", "tp", None)), out_specs=row_spec, check_vma=False)
```

```python
import functools

import jax
import jax.numpy as jnp
from jax import lax
from jax.experimental import pallas as pl
from jax.experimental.pallas import tpu as pltpu
from jax.sharding import PartitionSpec as P

CAP_FACTOR = 2
GROUP = 2
W_SLOTS = 4
EXTRA = 64
VMEM_LIMIT = 59 * 2**20
MESH = pl.DeviceIdType.MESH
BF16 = jnp.bfloat16
F32 = jnp.float32


def halves(packed):
    first = -(-packed // 32) * 16
    return first, packed - first


def packed_kernel(
    n_y, n_x, packed, cap, base_ref, ids_ref, gate_ref, x_hbm, wg_hbm, wu_hbm, wd_hbm, out_ref, most_ref,
    x_ref, x_sem, pack_buf, x_buf, slot_buf, pair_buf, opp_buf, nbr_buf, ret_buf, w_in, w_out, pos_col, gate_col,
    lists, table, flags, l_send, l_recv, t_send, t_recv, m_send, m_recv, ys_send, ys_recv, a_send, a_recv, b_send, b_recv, s_send, s_recv,
    p_send, p_recv, e_send, e_recv, n_send, n_recv, f_send, f_recv, h_send, h_recv, w_sem,
):
    tok, d_model = x_ref.shape
    n_loc = slot_buf.shape[1]
    n_slots = n_loc * cap
    hidden = w_out.shape[2]
    sizes = halves(packed)
    n_src = 2 * n_x
    n_grp = n_loc // GROUP
    n_w = n_y * n_grp
    yy = lax.axis_index("ep")
    tt = lax.axis_index("tp")
    xx, cc = tt // 2, tt % 2
    xr, xl, xo = (xx + n_x + 1 - 2 * cc) % n_x, (xx + n_x - 1 + 2 * cc) % n_x, (xx + 2) % n_x
    right, left, mate = {"tp": xr * 2 + cc}, {"tp": xl * 2 + cc}, {"tp": xx * 2 + 1 - cc}
    across = {"tp": xo * 2 + cc}
    sides = (right, left)
    ahead, behind = (xr, xl), (xl, xr)
    mine, other = cc * n_x, (1 - cc) * n_x
    width = table.shape[3]
    n_exp = n_loc * n_y

    def row_of(t):
        return (yy + t + cc * (n_y - 2 * t) + n_y) % n_y

    def row_to(t):
        return (yy - t - cc * (n_y - 2 * t) + 2 * n_y) % n_y

    def remote(src, dst, send, recv, device):
        return pltpu.make_async_remote_copy(
            src_ref=src, dst_ref=dst, send_sem=send, recv_sem=recv, device_id=device, device_id_type=MESH
        )

    def part(h):
        return pl.ds(h * sizes[0], sizes[h])

    def y_copy(t):
        return remote(pack_buf.at[t], x_buf.at[t, xx], ys_send.at[t], ys_recv.at[t], {"ep": row_to(t)})

    def list_copy(t):
        return remote(lists.at[t], table.at[t, xx], l_send.at[t], l_recv.at[t], {"ep": row_to(t)})

    def table_copy(t, k):
        view = table.at[t, xx]
        return remote(view, view, t_send.at[t, k], t_recv.at[t, k], (right, left, across)[k])

    def table_arrival(t, k):
        view = table.at[t, (xl, xr, xo)[k]]
        return remote(view, view, t_send.at[t, k], t_recv.at[t, k], (right, left, across)[k])

    def flag_copy():
        return remote(flags.at[0], flags.at[1], m_send, m_recv, mate)

    def a_copy(t, k, h):
        view = x_buf.at[t, xx, part(h)]
        return remote(view, view, a_send.at[t, k, h], a_recv.at[t, k, h], sides[k])

    def a_arrival(t, k, h):
        view = x_buf.at[t, behind[k], part(h)]
        return remote(view, view, a_send.at[t, k, h], a_recv.at[t, k, h], sides[k])

    def b_copy(t, k):
        view = x_buf.at[t, behind[k], part(k)]
        return remote(view, view, b_send.at[t, k], b_recv.at[t, k], sides[k])

    def b_arrival(t, k):
        view = x_buf.at[t, xo, part(k)]
        return remote(view, view, b_send.at[t, k], b_recv.at[t, k], sides[k])

    def s_copy(t, b):
        view = slot_buf.at[t % 2, :, mine + b]
        return remote(view, view, s_send.at[t, b], s_recv.at[t, b], mate)

    def s_arrival(t, b):
        view = slot_buf.at[t % 2, :, other + b]
        return remote(view, view, s_send.at[t, b], s_recv.at[t, b], mate)

    def p_copy(t, i):
        at = pl.ds(i * GROUP, GROUP)
        return remote(
            slot_buf.at[t % 2, at, pl.ds(other, n_x)], pair_buf.at[t % 2, at], p_send.at[t, i], p_recv.at[t, i], mate
        )

    def e_copy(t, k):
        dst = opp_buf.at[k, t, pl.ds(0, sizes[k])]
        return remote(x_buf.at[t, xo, part(k)], dst, e_send.at[t, k], e_recv.at[t, k], sides[k])

    def n_copy(t, k):
        h = 1 - k
        return remote(
            x_buf.at[t, ahead[k], part(h)], nbr_buf.at[k, t, part(h)], n_send.at[t, k], n_recv.at[t, k], sides[k]
        )

    def f_copy(t, k):
        return remote(
            x_buf.at[t, ahead[k], part(k)], nbr_buf.at[k, t, part(k)], f_send.at[t, k], f_recv.at[t, k], sides[k]
        )

    def h_copy(t):
        return remote(x_buf.at[t, xx], ret_buf.at[t], h_send.at[t], h_recv.at[t], {"ep": row_of(t)})

    def w_copies(w):
        s = w % W_SLOTS
        at = pl.ds((w % n_grp) * GROUP, GROUP)
        return (
            pltpu.make_async_copy(wg_hbm.at[at], w_in.at[s, :, :, pl.ds(0, hidden)], w_sem.at[s, 0]),
            pltpu.make_async_copy(wu_hbm.at[at], w_in.at[s, :, :, pl.ds(hidden, hidden)], w_sem.at[s, 1]),
            pltpu.make_async_copy(wd_hbm.at[at], w_out.at[s], w_sem.at[s, 2]),
        )

    x_copy = pltpu.make_async_copy(x_hbm, x_ref, x_sem)
    x_copy.start()
    barrier = pltpu.get_barrier_semaphore()
    for device in [right, left, across, mate] + [{"ep": (yy + d) % n_y} for d in range(1, n_y)]:
        pl.semaphore_signal(barrier, inc=1, device_id=device, device_id_type=MESH)
    for w in range(W_SLOTS):
        for c in w_copies(w):
            c.start()

    ids = ids_ref[...]
    lanes = 128
    order = (lax.broadcasted_iota(jnp.int32, (lanes, 2 * lanes), 0), lax.broadcasted_iota(jnp.int32, (lanes, 2 * lanes), 1))
    earlier = ((order[0] < order[1]) | (order[1] >= lanes)).astype(F32).astype(BF16)

    def count_left(marks):
        n = marks.shape[0]
        tiles = [marks[:, i * lanes:(i + 1) * lanes] for i in range(tok // lanes)]
        both = jnp.dot(jnp.concatenate(tiles, axis=0).astype(BF16), earlier, preferred_element_type=F32)
        total, left = jnp.zeros((n, lanes), F32), []
        for i in range(len(tiles)):
            left.append(both[i * n:(i + 1) * n, :lanes] + total)
            total = total + both[i * n:(i + 1) * n, lanes:]
        return jnp.concatenate(left, axis=1), total

    one_hot = lax.broadcasted_iota(jnp.int32, (n_exp, tok), 0) == ids
    preceding, _ = count_left(one_hot.astype(F32))
    slot = jnp.sum(jnp.where(one_hot, preceding, 0.0), axis=0, keepdims=True)
    kept = slot < cap
    rank = ids // n_loc
    pad = 8
    to_rank = (lax.broadcasted_iota(jnp.int32, (pad, tok), 0) == rank) & kept
    before, counts = count_left(to_rank.astype(F32))
    place = jnp.sum(jnp.where(to_rank, before, 0.0), axis=0, keepdims=True).astype(jnp.int32) - base_ref[0]
    most = jnp.max(counts, axis=0, keepdims=True).astype(jnp.int32)[:, 0:width - packed]
    pos = jnp.where(kept & (place >= 0) & (place < packed), rank * packed + place, -1)
    row_id = lax.broadcasted_iota(jnp.int32, (pad, tok), 0)
    parts = jnp.where(row_id == 0, (ids % n_loc).astype(F32), jnp.where(row_id == 1, slot, 1.0))
    parts = jnp.where(kept, parts, 0.0).astype(BF16)

    def wanted(t):
        pick = (lax.broadcasted_iota(jnp.int32, (packed, tok), 0) + row_to(t) * packed) == pos
        return pick.astype(F32).astype(BF16)

    def pack(t):
        return jnp.dot(wanted(t), x_ref[...], preferred_element_type=F32).astype(BF16)

    def list_of(t):
        got = lax.dot_general(parts, wanted(t), (((1,), (1,)), ((), ())), preferred_element_type=F32)
        return jnp.where(got[2:3] > 0.5, got[0:1] * cap + got[1:2], -1.0).astype(jnp.int32)

    def send_half(t, h):
        for k in range(2):
            a_copy(t, k, h if k == 0 else 1 - h).start()

    def send_table(t):
        for k in (2, 0, 1):
            table_copy(t, k).start()

    def send_own(t):
        list_copy(t).wait_recv()
        send_table(t)
        y_copy(t).wait_recv()
        send_half(t, 0)
        send_half(t, 1)

    def pass_on(t):
        for k in range(2):
            a_arrival(t, k, k).wait_recv()
            b_copy(t, k).start()

    def source_row(t, b):
        return table[t, b][:, :packed]

    def spread(t, blocks):
        @pl.loop(0, len(blocks))
        def _(j):
            b = blocks[0]
            for n, blk in enumerate(blocks[1:]):
                b = jnp.where(j == n + 1, blk, b)
            to = source_row(t, b)
            pick = (lax.broadcasted_iota(jnp.int32, (n_slots, packed), 0) == to).astype(F32).astype(BF16)
            slots = jnp.dot(pick, x_buf[t, b], preferred_element_type=F32).astype(BF16)
            slot_buf[t % 2, :, mine + b] = slots.reshape(n_loc, cap, d_model)
            s_copy(t, b).start()

    def share(t):
        for k in range(2):
            table_arrival(t, k).wait_recv()
            a_arrival(t, k, 1 - k).wait_recv()
        spread(t, (xl, xr))

    def multiply(t, lo, hi):
        @pl.loop(lo, hi)
        def _(i):
            w = t * n_grp + i
            s = w % W_SLOTS
            for c in w_copies(w):
                c.wait()
            both = []
            for el in range(GROUP):
                tile = slot_buf[t % 2, i * GROUP + el].reshape(n_src * cap, d_model)
                both.append(jnp.dot(tile, w_in[s, el], preferred_element_type=F32))
            for el in range(GROUP):
                act = (jax.nn.silu(both[el][:, :hidden]) * both[el][:, hidden:]).astype(BF16)
                out = jnp.dot(act, w_out[s, el], preferred_element_type=F32)
                slot_buf[t % 2, i * GROUP + el] = out.astype(BF16).reshape(n_src, cap, d_model)
            p_copy(t, i).start()

            @pl.when(w + W_SLOTS < n_w)
            def _():
                for c in w_copies(w + W_SLOTS):
                    c.start()

    def gather_back(t, blocks):
        @pl.loop(0, len(blocks))
        def _(j):
            b = blocks[0]
            for n, blk in enumerate(blocks[1:]):
                b = jnp.where(j == n + 1, blk, b)
            to = source_row(t, b).astype(F32)
            col = jnp.transpose(jnp.broadcast_to(to, (128, packed)))
            lane = lax.broadcasted_iota(jnp.int32, (packed, 128), 1).astype(F32)
            pick = jnp.concatenate(
                [(col == lane + float(128 * m)).astype(F32).astype(BF16) for m in range(n_slots // 128)], axis=1
            )
            total = slot_buf[t % 2, :, mine + b].astype(F32) + pair_buf[t % 2, :, b].astype(F32)
            slots = total.astype(BF16).reshape(n_slots, d_model)
            x_buf[t, b] = jnp.dot(pick, slots, preferred_element_type=F32).astype(BF16)

    def first_sums(t):
        @pl.loop(0, n_grp)
        def _(i):
            p_copy(t, i).wait_recv()

        gather_back(t, (xo,))
        for k in range(2):
            e_copy(t, k).start()
        gather_back(t, (xr, xl))

    def early_sums(t):
        for k in range(2):
            n_copy(t, k).start()

    def last_sum(t, k):
        e_copy(t, k).wait_recv()
        at = (t, ahead[k], part(k))
        x_buf[at] = (x_buf[at].astype(F32) + opp_buf[k, t, pl.ds(0, sizes[k])].astype(F32)).astype(BF16)
        f_copy(t, k).start()

    def last_sums(t):
        for k in range(2):
            last_sum(t, k)

    def give_back(t):
        for k in range(2):
            n_copy(t, k).wait_recv()
            f_copy(t, k).wait_recv()
        total = x_buf[t, xx].astype(F32) + (nbr_buf[0, t].astype(F32) + nbr_buf[1, t].astype(F32))
        x_buf[t, xx] = total.astype(BF16)
        h_copy(t).start()

    def keep_half(h):
        f_copy(0, h).wait_recv()
        n_copy(0, 1 - h).wait_recv()
        at = part(h)
        total = x_buf[0, xx, at].astype(F32) + (nbr_buf[0, 0, at].astype(F32) + nbr_buf[1, 0, at].astype(F32))
        ret_buf[0, at] = total.astype(BF16)

    def combine_into(t, first, low, size):
        tile = 256

        @pl.loop(0, tok // tile)
        def _(i):
            rows = pl.ds(pl.multiple_of(i * tile, tile), tile)
            want = pos_col[rows, :] - (row_to(t) * packed + low).astype(F32)
            lane = lax.broadcasted_iota(jnp.int32, (tile, 128), 1).astype(F32)
            pick = jnp.concatenate(
                [(want == lane + float(128 * m)).astype(F32) for m in range(-(-size // 128))], axis=1
            )
            y = jnp.dot(pick[:, :size].astype(BF16), ret_buf[t, pl.ds(low, size)], preferred_element_type=F32)
            gate = gate_col[rows, :]
            y = jnp.concatenate([y[:, m * 128:(m + 1) * 128] * gate for m in range(d_model // 128)], axis=1)
            if not first:
                y = y + out_ref[rows, :].astype(F32)
            out_ref[rows, :] = y.astype(BF16)

    x_copy.wait()
    x_buf[0, xx] = pack(0)
    pl.semaphore_wait(barrier, 3 + n_y)
    send_half(0, 0)
    table[0, xx, :, 0:packed] = list_of(0)
    table[0, xx, :, packed:width] = most
    send_table(0)
    send_half(0, 1)

    @pl.loop(1, n_y)
    def _(t):
        lists[t, :, 0:packed] = list_of(t)
        lists[t, :, packed:width] = most
        list_copy(t).start()
        pack_buf[t] = pack(t)
        y_copy(t).start()

    spread(0, (xx,))
    pass_on(0)
    send_own(1)
    tile = 256
    for i in range(tok // tile):
        spot = pos[:, i * tile:(i + 1) * tile].astype(F32)
        pos_col[i * tile:(i + 1) * tile, :] = jnp.transpose(jnp.broadcast_to(spot, (128, tile)))
        gate = gate_ref[:, i * tile:(i + 1) * tile]
        gate_col[i * tile:(i + 1) * tile, :] = jnp.transpose(jnp.broadcast_to(gate, (128, tile)))
    share(0)

    @pl.loop(0, n_y)
    def _(t):
        table_arrival(t, 2).wait_recv()
        for k in range(2):
            b_arrival(t, k).wait_recv()
        spread(t, (xo,))

        @pl.when(t + 1 < n_y)
        def _():
            pass_on(t + 1)

        @pl.when(t + 2 < n_y)
        def _():
            send_own(t + 2)

        for b in range(n_x):
            s_arrival(t, b).wait_recv()
            s_copy(t, b).wait_send()
        multiply(t, 0, n_grp // 2)

        @pl.when(t > 1)
        def _():
            last_sums(t - 1)

        @pl.when(t + 1 < n_y)
        def _():
            spread(t + 1, (xx,))

        multiply(t, n_grp // 2, n_grp)

        @pl.when(t + 1 < n_y)
        def _():
            share(t + 1)

        for k in range(2):
            for h in range(2):
                a_copy(t, k, h).wait_send()
            b_copy(t, k).wait_send()
        first_sums(t)

        @pl.when(t > 0)
        def _():
            early_sums(t)

        gather_back(t, (xx,))

        @pl.loop(0, n_grp)
        def _(i):
            p_copy(t, i).wait_send()

        @pl.when(t > 2)
        def _():
            give_back(t - 2)

    top = jnp.max(table[:, :, 0, packed:width])
    flags[0] = jnp.full((1, 128), top, jnp.int32)
    flag_copy().start()
    last_sums(n_y - 1)
    last_sum(0, 0)
    for k in (1, 0):
        n_copy(0, k).start()
    last_sum(0, 1)
    for t in range(1, n_y + 1):
        if n_y - 2 <= t < n_y:
            give_back(t)
        if t > 1:
            h_copy(t - 1).wait_recv()
            combine_into(t - 1, t == 2, 0, packed)
    flag_copy().wait()
    most_ref[...] = jnp.maximum(flags[0], flags[1])
    for t in range(1, n_y):
        list_copy(t).wait_send()
        y_copy(t).wait_send()
        h_copy(t).wait_send()

    @pl.loop(0, n_y)
    def _(t):
        for k in range(3):
            table_copy(t, k).wait_send()
        for k in range(2):
            e_copy(t, k).wait_send()
            n_copy(t, k).wait_send()
            f_copy(t, k).wait_send()

    for h in range(2):
        keep_half(h)
        combine_into(0, False, h * sizes[0], sizes[h])


def packed_layer(base, ids_loc, gate_loc, x_loc, wg, wu, wd, n_y, n_tp, packed, cap, collective_id):
    tok, d_model = x_loc.shape
    n_loc, _, hidden = wg.shape
    n_x = n_tp // 2
    n_grp = n_loc // GROUP
    half = halves(packed)[0]
    width = -(-(packed + 1) // 128) * 128
    dma = pltpu.SemaphoreType.DMA
    hbm = pl.BlockSpec(memory_space=pltpu.HBM)
    vmem = pl.BlockSpec(memory_space=pltpu.VMEM)
    return pl.pallas_call(
        functools.partial(packed_kernel, n_y, n_x, packed, cap),
        out_shape=(jax.ShapeDtypeStruct((tok, d_model), BF16), jax.ShapeDtypeStruct((1, 128), jnp.int32)),
        in_specs=[pl.BlockSpec(memory_space=pltpu.SMEM)] + [vmem] * 2 + [hbm] * 4,
        out_specs=(vmem, vmem),
        scratch_shapes=[
            pltpu.VMEM((tok, d_model), BF16),
            dma,
            pltpu.VMEM((n_y, packed, d_model), BF16),
            pltpu.VMEM((n_y, n_x, packed, d_model), BF16),
            pltpu.VMEM((2, n_loc, 2 * n_x, cap, d_model), BF16),
            pltpu.VMEM((2, n_loc, n_x, cap, d_model), BF16),
            pltpu.VMEM((2, n_y, half, d_model), BF16),
            pltpu.VMEM((2, n_y, packed, d_model), BF16),
            pltpu.VMEM((n_y, packed, d_model), BF16),
            pltpu.VMEM((W_SLOTS, GROUP, d_model, 2 * hidden), BF16),
            pltpu.VMEM((W_SLOTS, GROUP, hidden, d_model), BF16),
            pltpu.VMEM((tok, 128), F32),
            pltpu.VMEM((tok, 128), F32),
            pltpu.VMEM((n_y, 1, width), jnp.int32),
            pltpu.VMEM((n_y, n_x, 1, width), jnp.int32),
            pltpu.VMEM((2, 1, 128), jnp.int32),
            dma((n_y,)), dma((n_y,)), dma((n_y, 3)), dma((n_y, 3)), dma, dma,
            dma((n_y,)), dma((n_y,)),
            dma((n_y, 2, 2)), dma((n_y, 2, 2)),
            dma((n_y, 2)), dma((n_y, 2)),
            dma((n_y, n_x)), dma((n_y, n_x)),
            dma((n_y, n_grp)), dma((n_y, n_grp)),
            dma((n_y, 2)), dma((n_y, 2)),
            dma((n_y, 2)), dma((n_y, 2)),
            dma((n_y, 2)), dma((n_y, 2)),
            dma((n_y,)), dma((n_y,)),
            dma((W_SLOTS, 3)),
        ],
        compiler_params=pltpu.CompilerParams(
            collective_id=collective_id, has_side_effects=True, vmem_limit_bytes=VMEM_LIMIT
        ),
        name="packed_layer",
    )(base.reshape(1), ids_loc.reshape(1, tok), gate_loc.reshape(1, tok), x_loc, wg, wu, wd)


def solution(mesh):
    n_y, n_tp = mesh.shape["ep"], mesh.shape["tp"]
    row_spec = P(("dp", "ep", "tp"), None)

    def local_layer(x_loc, ids_loc, gate_loc, wg_loc, wu_loc, wd_loc):
        tok, d_model = x_loc.shape
        n_loc = wg_loc.shape[0]
        n_exp = n_loc * n_y
        capacity = CAP_FACTOR * tok // n_exp
        packed = n_loc * capacity * 19 // 32
        args = (ids_loc, gate_loc, x_loc, wg_loc, wu_loc, wd_loc, n_y, n_tp)
        out, most = packed_layer(jnp.int32(0), *args, packed, capacity, 0)

        def more(carry):
            total, base = carry
            extra, _ = packed_layer(base, *args, EXTRA, capacity, 1)
            return total + extra, base + EXTRA

        def passes(first):
            return lax.while_loop(lambda carry: carry[1] < most[0, 0], more, (first, jnp.int32(packed)))[0]

        out = lax.cond(most[0, 0] > packed, passes, lambda first: first, out)
        return out

    return jax.shard_map(local_layer, mesh=mesh, in_specs=(row_spec, row_spec, row_spec, P("ep", None, "tp"), P("ep", None, "tp"), P("ep", "tp", None)), out_specs=row_spec, check_vma=False)
```

```python
import functools

import jax
import jax.numpy as jnp
from jax import lax
from jax.experimental import pallas as pl
from jax.experimental.pallas import tpu as pltpu
from jax.sharding import PartitionSpec as P

CAP_FACTOR = 2
GROUP = 2
W_SLOTS = 4
EXTRA = 64
VMEM_LIMIT = 59 * 2**20
MESH = pl.DeviceIdType.MESH
BF16 = jnp.bfloat16
F32 = jnp.float32


def halves(packed):
    first = -(-packed // 32) * 16
    return first, packed - first


def packed_kernel(
    n_y, n_x, packed, cap, base_ref, ids_ref, gate_ref, x_hbm, wg_hbm, wu_hbm, wd_hbm, out_ref, most_ref,
    x_ref, x_sem, pack_buf, x_buf, slot_buf, pair_buf, opp_buf, nbr_buf, ret_buf, w_in, w_out, pos_col, gate_col,
    lists, table, flags, l_send, l_recv, t_send, t_recv, m_send, m_recv, ys_send, ys_recv, a_send, a_recv, b_send, b_recv, s_send, s_recv,
    p_send, p_recv, e_send, e_recv, n_send, n_recv, f_send, f_recv, h_send, h_recv, w_sem,
):
    tok, d_model = x_ref.shape
    n_loc = slot_buf.shape[1]
    n_slots = n_loc * cap
    hidden = w_out.shape[2]
    sizes = halves(packed)
    n_src = 2 * n_x
    n_grp = n_loc // GROUP
    n_w = n_y * n_grp
    yy = lax.axis_index("ep")
    tt = lax.axis_index("tp")
    xx, cc = tt // 2, tt % 2
    xr, xl, xo = (xx + n_x + 1 - 2 * cc) % n_x, (xx + n_x - 1 + 2 * cc) % n_x, (xx + 2) % n_x
    right, left, mate = {"tp": xr * 2 + cc}, {"tp": xl * 2 + cc}, {"tp": xx * 2 + 1 - cc}
    across = {"tp": xo * 2 + cc}
    sides = (right, left)
    ahead, behind = (xr, xl), (xl, xr)
    mine, other = cc * n_x, (1 - cc) * n_x
    width = table.shape[3]
    n_exp = n_loc * n_y

    def row_of(t):
        return (yy + t + cc * (n_y - 2 * t) + n_y) % n_y

    def row_to(t):
        return (yy - t - cc * (n_y - 2 * t) + 2 * n_y) % n_y

    def remote(src, dst, send, recv, device):
        return pltpu.make_async_remote_copy(
            src_ref=src, dst_ref=dst, send_sem=send, recv_sem=recv, device_id=device, device_id_type=MESH
        )

    def part(h):
        return pl.ds(h * sizes[0], sizes[h])

    def y_copy(t):
        return remote(pack_buf.at[t], x_buf.at[t, xx], ys_send.at[t], ys_recv.at[t], {"ep": row_to(t)})

    def list_copy(t):
        return remote(lists.at[t], table.at[t, xx], l_send.at[t], l_recv.at[t], {"ep": row_to(t)})

    def table_copy(t, k):
        view = table.at[t, xx]
        return remote(view, view, t_send.at[t, k], t_recv.at[t, k], (right, left, across)[k])

    def table_arrival(t, k):
        view = table.at[t, (xl, xr, xo)[k]]
        return remote(view, view, t_send.at[t, k], t_recv.at[t, k], (right, left, across)[k])

    def flag_copy():
        return remote(flags.at[0], flags.at[1], m_send, m_recv, mate)

    def a_copy(t, k, h):
        view = x_buf.at[t, xx, part(h)]
        return remote(view, view, a_send.at[t, k, h], a_recv.at[t, k, h], sides[k])

    def a_arrival(t, k, h):
        view = x_buf.at[t, behind[k], part(h)]
        return remote(view, view, a_send.at[t, k, h], a_recv.at[t, k, h], sides[k])

    def b_copy(t, k):
        view = x_buf.at[t, behind[k], part(k)]
        return remote(view, view, b_send.at[t, k], b_recv.at[t, k], sides[k])

    def b_arrival(t, k):
        view = x_buf.at[t, xo, part(k)]
        return remote(view, view, b_send.at[t, k], b_recv.at[t, k], sides[k])

    def s_copy(t, b):
        view = slot_buf.at[t % 2, :, mine + b]
        return remote(view, view, s_send.at[t, b], s_recv.at[t, b], mate)

    def s_arrival(t, b):
        view = slot_buf.at[t % 2, :, other + b]
        return remote(view, view, s_send.at[t, b], s_recv.at[t, b], mate)

    def p_copy(t, i):
        at = pl.ds(i * GROUP, GROUP)
        return remote(
            slot_buf.at[t % 2, at, pl.ds(other, n_x)], pair_buf.at[t % 2, at], p_send.at[t, i], p_recv.at[t, i], mate
        )

    def e_copy(t, k):
        dst = opp_buf.at[k, t, pl.ds(0, sizes[k])]
        return remote(x_buf.at[t, xo, part(k)], dst, e_send.at[t, k], e_recv.at[t, k], sides[k])

    def n_copy(t, k):
        h = 1 - k
        return remote(
            x_buf.at[t, ahead[k], part(h)], nbr_buf.at[k, t, part(h)], n_send.at[t, k], n_recv.at[t, k], sides[k]
        )

    def f_copy(t, k):
        return remote(
            x_buf.at[t, ahead[k], part(k)], nbr_buf.at[k, t, part(k)], f_send.at[t, k], f_recv.at[t, k], sides[k]
        )

    def h_copy(t):
        return remote(x_buf.at[t, xx], ret_buf.at[t], h_send.at[t], h_recv.at[t], {"ep": row_of(t)})

    def w_copies(w):
        s = w % W_SLOTS
        at = pl.ds((w % n_grp) * GROUP, GROUP)
        return (
            pltpu.make_async_copy(wg_hbm.at[at], w_in.at[s, :, :, pl.ds(0, hidden)], w_sem.at[s, 0]),
            pltpu.make_async_copy(wu_hbm.at[at], w_in.at[s, :, :, pl.ds(hidden, hidden)], w_sem.at[s, 1]),
            pltpu.make_async_copy(wd_hbm.at[at], w_out.at[s], w_sem.at[s, 2]),
        )

    x_copy = pltpu.make_async_copy(x_hbm, x_ref, x_sem)
    x_copy.start()
    barrier = pltpu.get_barrier_semaphore()
    for device in [right, left, across, mate] + [{"ep": (yy + d) % n_y} for d in range(1, n_y)]:
        pl.semaphore_signal(barrier, inc=1, device_id=device, device_id_type=MESH)
    for w in range(W_SLOTS):
        for c in w_copies(w):
            c.start()

    ids = ids_ref[...]
    lanes = 128
    order = (lax.broadcasted_iota(jnp.int32, (lanes, 2 * lanes), 0), lax.broadcasted_iota(jnp.int32, (lanes, 2 * lanes), 1))
    earlier = ((order[0] < order[1]) | (order[1] >= lanes)).astype(F32).astype(BF16)

    def count_left(marks):
        n = marks.shape[0]
        tiles = [marks[:, i * lanes:(i + 1) * lanes] for i in range(tok // lanes)]
        both = jnp.dot(jnp.concatenate(tiles, axis=0).astype(BF16), earlier, preferred_element_type=F32)
        total, left = jnp.zeros((n, lanes), F32), []
        for i in range(len(tiles)):
            left.append(both[i * n:(i + 1) * n, :lanes] + total)
            total = total + both[i * n:(i + 1) * n, lanes:]
        return jnp.concatenate(left, axis=1), total

    one_hot = lax.broadcasted_iota(jnp.int32, (n_exp, tok), 0) == ids
    preceding, _ = count_left(one_hot.astype(F32))
    slot = jnp.sum(jnp.where(one_hot, preceding, 0.0), axis=0, keepdims=True)
    kept = slot < cap
    rank = ids // n_loc
    pad = 8
    to_rank = (lax.broadcasted_iota(jnp.int32, (pad, tok), 0) == rank) & kept
    before, counts = count_left(to_rank.astype(F32))
    place = jnp.sum(jnp.where(to_rank, before, 0.0), axis=0, keepdims=True).astype(jnp.int32) - base_ref[0]
    most = jnp.max(counts, axis=0, keepdims=True).astype(jnp.int32)[:, 0:width - packed]
    pos = jnp.where(kept & (place >= 0) & (place < packed), rank * packed + place, -1)
    row_id = lax.broadcasted_iota(jnp.int32, (pad, tok), 0)
    parts = jnp.where(row_id == 0, (ids % n_loc).astype(F32), jnp.where(row_id == 1, slot, 1.0))
    parts = jnp.where(kept, parts, 0.0).astype(BF16)

    def wanted(t):
        pick = (lax.broadcasted_iota(jnp.int32, (packed, tok), 0) + row_to(t) * packed) == pos
        return pick.astype(F32).astype(BF16)

    def pack(t):
        return jnp.dot(wanted(t), x_ref[...], preferred_element_type=F32).astype(BF16)

    def list_of(t):
        got = lax.dot_general(parts, wanted(t), (((1,), (1,)), ((), ())), preferred_element_type=F32)
        return jnp.where(got[2:3] > 0.5, got[0:1] * cap + got[1:2], -1.0).astype(jnp.int32)

    def send_half(t, h):
        for k in range(2):
            a_copy(t, k, h if k == 0 else 1 - h).start()

    def send_table(t):
        for k in (2, 0, 1):
            table_copy(t, k).start()

    def send_own(t):
        list_copy(t).wait_recv()
        send_table(t)
        y_copy(t).wait_recv()
        send_half(t, 0)
        send_half(t, 1)

    def pass_on(t):
        for k in range(2):
            a_arrival(t, k, k).wait_recv()
            b_copy(t, k).start()

    def source_row(t, b):
        return table[t, b][:, :packed]

    def spread(t, blocks):
        @pl.loop(0, len(blocks))
        def _(j):
            b = blocks[0]
            for n, blk in enumerate(blocks[1:]):
                b = jnp.where(j == n + 1, blk, b)
            to = source_row(t, b)
            pick = (lax.broadcasted_iota(jnp.int32, (n_slots, packed), 0) == to).astype(F32).astype(BF16)
            slots = jnp.dot(pick, x_buf[t, b], preferred_element_type=F32).astype(BF16)
            slot_buf[t % 2, :, mine + b] = slots.reshape(n_loc, cap, d_model)
            s_copy(t, b).start()

    def share(t):
        for k in range(2):
            table_arrival(t, k).wait_recv()
            a_arrival(t, k, 1 - k).wait_recv()
        spread(t, (xl, xr))

    def multiply(t, lo, hi):
        @pl.loop(lo, hi)
        def _(i):
            w = t * n_grp + i
            s = w % W_SLOTS
            for c in w_copies(w):
                c.wait()
            both = []
            for el in range(GROUP):
                tile = slot_buf[t % 2, i * GROUP + el].reshape(n_src * cap, d_model)
                both.append(jnp.dot(tile, w_in[s, el], preferred_element_type=F32))
            for el in range(GROUP):
                act = (jax.nn.silu(both[el][:, :hidden]) * both[el][:, hidden:]).astype(BF16)
                out = jnp.dot(act, w_out[s, el], preferred_element_type=F32)
                slot_buf[t % 2, i * GROUP + el] = out.astype(BF16).reshape(n_src, cap, d_model)
            p_copy(t, i).start()

            @pl.when(w + W_SLOTS < n_w)
            def _():
                for c in w_copies(w + W_SLOTS):
                    c.start()

    def gather_back(t, blocks):
        @pl.loop(0, len(blocks))
        def _(j):
            b = blocks[0]
            for n, blk in enumerate(blocks[1:]):
                b = jnp.where(j == n + 1, blk, b)
            to = source_row(t, b).astype(F32)
            col = jnp.transpose(jnp.broadcast_to(to, (128, packed)))
            lane = lax.broadcasted_iota(jnp.int32, (packed, 128), 1).astype(F32)
            pick = jnp.concatenate(
                [(col == lane + float(128 * m)).astype(F32).astype(BF16) for m in range(n_slots // 128)], axis=1
            )
            total = slot_buf[t % 2, :, mine + b].astype(F32) + pair_buf[t % 2, :, b].astype(F32)
            slots = total.astype(BF16).reshape(n_slots, d_model)
            x_buf[t, b] = jnp.dot(pick, slots, preferred_element_type=F32).astype(BF16)

    def first_sums(t):
        @pl.loop(0, n_grp)
        def _(i):
            p_copy(t, i).wait_recv()

        gather_back(t, (xo,))
        for k in range(2):
            e_copy(t, k).start()
        gather_back(t, (xr, xl))

    def early_sums(t):
        for k in range(2):
            n_copy(t, k).start()

    def last_sum(t, k):
        e_copy(t, k).wait_recv()
        at = (t, ahead[k], part(k))
        x_buf[at] = (x_buf[at].astype(F32) + opp_buf[k, t, pl.ds(0, sizes[k])].astype(F32)).astype(BF16)
        f_copy(t, k).start()

    def last_sums(t):
        for k in range(2):
            last_sum(t, k)

    def give_back(t):
        for k in range(2):
            n_copy(t, k).wait_recv()
            f_copy(t, k).wait_recv()
        total = x_buf[t, xx].astype(F32) + (nbr_buf[0, t].astype(F32) + nbr_buf[1, t].astype(F32))
        x_buf[t, xx] = total.astype(BF16)
        h_copy(t).start()

    def keep_half(h):
        f_copy(0, h).wait_recv()
        n_copy(0, 1 - h).wait_recv()
        at = part(h)
        total = x_buf[0, xx, at].astype(F32) + (nbr_buf[0, 0, at].astype(F32) + nbr_buf[1, 0, at].astype(F32))
        ret_buf[0, at] = total.astype(BF16)

    def combine_into(t, low, size):
        tile = 256

        @pl.loop(0, tok // tile)
        def _(i):
            rows = pl.ds(pl.multiple_of(i * tile, tile), tile)
            want = pos_col[rows, :] - (row_to(t) * packed + low).astype(F32)
            lane = lax.broadcasted_iota(jnp.int32, (tile, 128), 1).astype(F32)
            pick = jnp.concatenate(
                [(want == lane + float(128 * m)).astype(F32) for m in range(-(-size // 128))], axis=1
            )
            y = jnp.dot(pick[:, :size].astype(BF16), ret_buf[t, pl.ds(low, size)], preferred_element_type=F32)
            gate = gate_col[rows, :]
            y = jnp.concatenate([y[:, m * 128:(m + 1) * 128] * gate for m in range(d_model // 128)], axis=1)
            out_ref[rows, :] = (y + out_ref[rows, :].astype(F32)).astype(BF16)

    x_copy.wait()
    x_buf[0, xx] = pack(0)
    pl.semaphore_wait(barrier, 3 + n_y)
    send_half(0, 0)
    table[0, xx, :, 0:packed] = list_of(0)
    table[0, xx, :, packed:width] = most
    send_table(0)
    send_half(0, 1)

    @pl.loop(1, n_y)
    def _(t):
        lists[t, :, 0:packed] = list_of(t)
        lists[t, :, packed:width] = most
        list_copy(t).start()
        pack_buf[t] = pack(t)
        y_copy(t).start()

    spread(0, (xx,))
    pass_on(0)
    send_own(1)
    tile = 256
    for i in range(tok // tile):
        spot = pos[:, i * tile:(i + 1) * tile].astype(F32)
        pos_col[i * tile:(i + 1) * tile, :] = jnp.transpose(jnp.broadcast_to(spot, (128, tile)))
        gate = gate_ref[:, i * tile:(i + 1) * tile]
        gate_col[i * tile:(i + 1) * tile, :] = jnp.transpose(jnp.broadcast_to(gate, (128, tile)))
    out_ref[...] = jnp.zeros_like(out_ref)
    share(0)

    @pl.loop(0, n_y)
    def _(t):
        table_arrival(t, 2).wait_recv()
        for k in range(2):
            b_arrival(t, k).wait_recv()
        spread(t, (xo,))

        @pl.when(t + 1 < n_y)
        def _():
            pass_on(t + 1)

        @pl.when(t + 2 < n_y)
        def _():
            send_own(t + 2)

        for b in range(n_x):
            s_arrival(t, b).wait_recv()
            s_copy(t, b).wait_send()
        multiply(t, 0, n_grp // 2)

        @pl.when(t > 1)
        def _():
            last_sums(t - 1)

        @pl.when(t + 1 < n_y)
        def _():
            spread(t + 1, (xx,))

        multiply(t, n_grp // 2, n_grp)

        @pl.when(t + 1 < n_y)
        def _():
            share(t + 1)

        for k in range(2):
            for h in range(2):
                a_copy(t, k, h).wait_send()
            b_copy(t, k).wait_send()
        first_sums(t)

        @pl.when(t > 0)
        def _():
            early_sums(t)

        gather_back(t, (xx,))

        @pl.loop(0, n_grp)
        def _(i):
            p_copy(t, i).wait_send()

        @pl.when(t > 2)
        def _():
            give_back(t - 2)

    top = jnp.max(table[:, :, 0, packed:width])
    flags[0] = jnp.full((1, 128), top, jnp.int32)
    flag_copy().start()
    last_sums(n_y - 1)
    last_sum(0, 0)
    for k in (1, 0):
        n_copy(0, k).start()
    last_sum(0, 1)
    for t in range(1, n_y):
        if t >= n_y - 2:
            give_back(t)
        if t > 1:
            h_copy(t - 1).wait_recv()
            combine_into(t - 1, 0, packed)
    keep_half(0)
    combine_into(0, 0, sizes[0])
    h_copy(n_y - 1).wait_recv()
    combine_into(n_y - 1, 0, packed)
    flag_copy().wait()
    most_ref[...] = jnp.maximum(flags[0], flags[1])
    for t in range(1, n_y):
        list_copy(t).wait_send()
        y_copy(t).wait_send()
        h_copy(t).wait_send()

    @pl.loop(0, n_y)
    def _(t):
        for k in range(3):
            table_copy(t, k).wait_send()
        for k in range(2):
            e_copy(t, k).wait_send()
            n_copy(t, k).wait_send()
            f_copy(t, k).wait_send()

    keep_half(1)
    combine_into(0, sizes[0], sizes[1])


def packed_layer(base, ids_loc, gate_loc, x_loc, wg, wu, wd, n_y, n_tp, packed, cap, collective_id):
    tok, d_model = x_loc.shape
    n_loc, _, hidden = wg.shape
    n_x = n_tp // 2
    n_grp = n_loc // GROUP
    half = halves(packed)[0]
    width = -(-(packed + 1) // 128) * 128
    dma = pltpu.SemaphoreType.DMA
    hbm = pl.BlockSpec(memory_space=pltpu.HBM)
    vmem = pl.BlockSpec(memory_space=pltpu.VMEM)
    return pl.pallas_call(
        functools.partial(packed_kernel, n_y, n_x, packed, cap),
        out_shape=(jax.ShapeDtypeStruct((tok, d_model), BF16), jax.ShapeDtypeStruct((1, 128), jnp.int32)),
        in_specs=[pl.BlockSpec(memory_space=pltpu.SMEM)] + [vmem] * 2 + [hbm] * 4,
        out_specs=(vmem, vmem),
        scratch_shapes=[
            pltpu.VMEM((tok, d_model), BF16),
            dma,
            pltpu.VMEM((n_y, packed, d_model), BF16),
            pltpu.VMEM((n_y, n_x, packed, d_model), BF16),
            pltpu.VMEM((2, n_loc, 2 * n_x, cap, d_model), BF16),
            pltpu.VMEM((2, n_loc, n_x, cap, d_model), BF16),
            pltpu.VMEM((2, n_y, half, d_model), BF16),
            pltpu.VMEM((2, n_y, packed, d_model), BF16),
            pltpu.VMEM((n_y, packed, d_model), BF16),
            pltpu.VMEM((W_SLOTS, GROUP, d_model, 2 * hidden), BF16),
            pltpu.VMEM((W_SLOTS, GROUP, hidden, d_model), BF16),
            pltpu.VMEM((tok, 128), F32),
            pltpu.VMEM((tok, 128), F32),
            pltpu.VMEM((n_y, 1, width), jnp.int32),
            pltpu.VMEM((n_y, n_x, 1, width), jnp.int32),
            pltpu.VMEM((2, 1, 128), jnp.int32),
            dma((n_y,)), dma((n_y,)), dma((n_y, 3)), dma((n_y, 3)), dma, dma,
            dma((n_y,)), dma((n_y,)),
            dma((n_y, 2, 2)), dma((n_y, 2, 2)),
            dma((n_y, 2)), dma((n_y, 2)),
            dma((n_y, n_x)), dma((n_y, n_x)),
            dma((n_y, n_grp)), dma((n_y, n_grp)),
            dma((n_y, 2)), dma((n_y, 2)),
            dma((n_y, 2)), dma((n_y, 2)),
            dma((n_y, 2)), dma((n_y, 2)),
            dma((n_y,)), dma((n_y,)),
            dma((W_SLOTS, 3)),
        ],
        compiler_params=pltpu.CompilerParams(
            collective_id=collective_id, has_side_effects=True, vmem_limit_bytes=VMEM_LIMIT
        ),
        name="packed_layer",
    )(base.reshape(1), ids_loc.reshape(1, tok), gate_loc.reshape(1, tok), x_loc, wg, wu, wd)


def solution(mesh):
    n_y, n_tp = mesh.shape["ep"], mesh.shape["tp"]
    row_spec = P(("dp", "ep", "tp"), None)

    def local_layer(x_loc, ids_loc, gate_loc, wg_loc, wu_loc, wd_loc):
        tok, d_model = x_loc.shape
        n_loc = wg_loc.shape[0]
        n_exp = n_loc * n_y
        capacity = CAP_FACTOR * tok // n_exp
        packed = n_loc * capacity * 19 // 32
        args = (ids_loc, gate_loc, x_loc, wg_loc, wu_loc, wd_loc, n_y, n_tp)
        out, most = packed_layer(jnp.int32(0), *args, packed, capacity, 0)

        def more(carry):
            total, base = carry
            extra, _ = packed_layer(base, *args, EXTRA, capacity, 1)
            return total + extra, base + EXTRA

        def passes(first):
            return lax.while_loop(lambda carry: carry[1] < most[0, 0], more, (first, jnp.int32(packed)))[0]

        out = lax.cond(most[0, 0] > packed, passes, lambda first: first, out)
        return out

    return jax.shard_map(local_layer, mesh=mesh, in_specs=(row_spec, row_spec, row_spec, P("ep", None, "tp"), P("ep", None, "tp"), P("ep", "tp", None)), out_specs=row_spec, check_vma=False)
```
